256 devices in a mesh: ha: 16 (over z, core), wa: 8 (over y, x_lo), ba: 2 (over x_hi).
Axes of the slice: x: 4 (x_hi: 2, x_lo: 2; x = x_hi * 2 + x_lo), y: 4, z: 8, core: 2. Of those that a mesh axis runs over, the one named last changes fastest.
Arguments:
- tokens: bfloat16 [2, 256, 256, 384], P('ba', 'ha', 'wa'), may hold values from -6 to 6
- cotangent: bfloat16 [2, 256, 256, 384], P('ba', 'ha', 'wa'), may hold values from -6 to 6
- w_qkv: bfloat16 [384, 1152], replicated, may hold values from -0.20412415 to 0.20412415
- w_proj: bfloat16 [384, 384], replicated, may hold values from -0.3125 to 0.3125
- table_logits: float32 [12, 225], replicated, may hold values from -6 to 6
- logit_scale: float32 [12], replicated, may hold values from 1 to 5.5
- gain: float32 [384], replicated, may hold values from 0.5 to 1.5
Outputs:
- d_tokens: bfloat16 [2, 256, 256, 384], P('ba', 'ha', 'wa')
- d_wqkv: float32 [384, 1152], P(None, 'ba')
- d_wproj: float32 [384, 384], P(None, 'ba')
- d_table: float32 [12, 225], replicated
- d_scale: float32 [12], replicated
- d_gain: float32 [384], replicated
The draws below stay inside these ranges and needn't reach their ends.
All inputs are finite; a program needn't handle non-finite values.
Results may differ from the reference program's by a relative error of at most 0.01.
The reference program's roundings to bfloat16 on the way count: a program that leaves them out, or rounds other values in their place, can miss the bound.
Values may be sent and summed in bfloat16 or wider, within the bound.
A program may use at most 64 MiB of HBM per device.

```python
import math
import jax
import jax.numpy as jnp
from jax import lax

HEADS = 12
C = 384
WIN = 8
TABLE = 225
HEIGHT = 256
WIDTH = 256
BATCH = 2


def draw_w_qkv(key, part):
    spread = C ** (-0.5)
    base = jax.random.normal(key, (C, 3 * C), jnp.float32) * spread
    base = jnp.clip(base, -4.0 * spread, 4.0 * spread)
    return base.astype(jnp.bfloat16)


def shard_levels(key, shape, cuts, low, largest):
    factor_of, own = 1.0, jax.random.fold_in(key, 6)
    for dim, shards_of in cuts:
        heights = jnp.exp(jax.random.uniform(jax.random.fold_in(own, dim), (shards_of,), jnp.float32, low / len(cuts), largest / len(cuts)))
        factor_of = factor_of * jnp.repeat(heights, shape[dim] // shards_of).reshape([-1 if axis == dim else 1 for axis in range(len(shape))])
    return factor_of


def normal_values(own_key, shape, deviation, most, shards=(), kind=jnp.bfloat16):
    values = jax.random.normal(own_key, shape, jnp.float32) * deviation
    if len(shards) > 0:
        values = shard_levels(own_key, shape, shards, -0.22, 0.18) * values
    return jnp.clip(values, min=-most, max=most).astype(kind)


def setup_inputs(seed: int = 0) -> dict:
    splits = jax.random.split(jax.random.key(seed), 8)
    return {
        "tokens": normal_values(splits[0], (BATCH, HEIGHT, WIDTH, C), 1.0, 6.0, ((0, 2), (1, 16), (2, 8))),
        "cotangent": normal_values(splits[1], (BATCH, HEIGHT, WIDTH, C), 1.0, 6.0, ((0, 2), (1, 16), (2, 8))),
        "w_qkv": draw_w_qkv(jax.random.fold_in(splits[7], 71), 0),
        "w_proj": normal_values(splits[3], (C, C), C ** -0.5, 0.3125),
        "table_logits": normal_values(splits[4], (HEADS, TABLE), 1.5, 6.0, (), jnp.float32),
        "logit_scale": jnp.clip(jax.random.uniform(splits[5], (HEADS,), jnp.float32, 1.0, 5.5), 1.0, 5.5),
        "gain": jnp.clip(1.0 + 0.1 * jax.random.normal(splits[6], (C,), jnp.float32), 0.5, 1.5),
    }


EPS_NORM = 1e-05
MASK_FILL = -100.0
SCALE_CAP = math.log(100.0)
BIAS_RANGE = 16.0
HIGHEST = lax.Precision.HIGHEST

def coarse_product(form, left, right):
    return jnp.einsum(form, left.astype(jnp.float32), right.astype(jnp.float32), precision=HIGHEST)

def fine_product(form, left, right):
    return jnp.einsum(form, left, right, precision=HIGHEST)

def to_windows(block, window):
    images, height, width, depth = block.shape
    tiles = block.reshape(images, height // window, window, width // window, window, depth)
    tiles = tiles.transpose(0, 1, 3, 2, 4, 5)
    return tiles.reshape(images, height // window * (width // window), window * window, depth)

def from_windows(tiles, images, height, width, window):
    depth = tiles.shape[-1]
    grid = tiles.reshape(images, height // window, width // window, window, window, depth)
    return grid.transpose(0, 1, 3, 2, 4, 5).reshape(images, height, width, depth)

def position_onehot(window):
    places = jnp.arange(window * window, dtype=jnp.int32)
    row_of = places // window
    col_of = places % window
    offset = (row_of[:, None] - row_of[None, :] + window - 1) * (2 * window - 1) + (col_of[:, None] - col_of[None, :] + window - 1)
    entries = jnp.arange((2 * window - 1) ** 2, dtype=jnp.int32)
    return (offset.reshape(-1)[:, None] == entries[None, :]).astype(jnp.float32)

def region_of(coords, extent, window):
    return (coords >= extent - window).astype(jnp.int32) + (coords >= extent - window // 2).astype(jnp.int32)

def region_mask(row_start, col_start, rows, cols, height, width, window):
    row_label = region_of(row_start + jnp.arange(rows, dtype=jnp.int32), height, window)
    col_label = region_of(col_start + jnp.arange(cols, dtype=jnp.int32), width, window)
    labels = row_label[:, None] * 3 + col_label[None, :]
    labels = labels.reshape(rows // window, window, cols // window, window).transpose(0, 2, 1, 3)
    labels = labels.reshape(-1, window * window)
    return jnp.where(labels[:, :, None] != labels[:, None, :], MASK_FILL, 0.0).astype(jnp.float32)

def grads_region(block, grad_block, row_start, col_start, height, width, window, params):
    w_qkv, w_proj, table_logits, logit_scale, gain = params
    images, rows, cols, depth = block.shape
    heads = logit_scale.shape[0]
    head_dim = depth // heads
    tiles = to_windows(block, window)
    grad_tiles = to_windows(grad_block, window)
    count = tiles.shape[1]
    length = window * window
    flat = tiles.reshape(-1, depth)
    qkv = jnp.dot(flat, w_qkv, preferred_element_type=jnp.float32).astype(jnp.bfloat16)
    qkv = qkv.reshape(images, count, length, 3, heads, head_dim)
    query = qkv[:, :, :, 0].astype(jnp.float32)
    keys = qkv[:, :, :, 1].astype(jnp.float32)
    values = qkv[:, :, :, 2]
    query_inv = lax.rsqrt(lax.optimization_barrier(jnp.sum(query * query, -1, keepdims=True)) + 1.0)
    key_inv = lax.rsqrt(lax.optimization_barrier(jnp.sum(keys * keys, -1, keepdims=True)) + 1.0)
    unit_query = query * query_inv
    unit_key = keys * key_inv
    scale = jnp.exp(jnp.minimum(logit_scale, SCALE_CAP))
    onehot = position_onehot(window)
    sigma = jax.nn.sigmoid(table_logits)
    rel_bias = jnp.dot(sigma * BIAS_RANGE, onehot.T, precision=HIGHEST).reshape(heads, length, length)
    mask = region_mask(row_start, col_start, rows, cols, height, width, window)
    cosine = fine_product('bnqhd,bnkhd->bnhqk', unit_query, unit_key)
    scores = scale[:, None, None] * cosine + rel_bias[None, None] + mask[None, :, None]
    top = lax.optimization_barrier(jnp.max(scores, -1, keepdims=True))
    expo = jnp.exp(scores - top)
    probs = expo / lax.optimization_barrier(jnp.sum(expo, -1, keepdims=True))
    probs_low = probs.astype(jnp.bfloat16)
    attended = coarse_product('bnhqk,bnkhd->bnqhd', probs_low, values).astype(jnp.bfloat16).reshape(-1, depth)
    proj = jnp.dot(attended, w_proj, preferred_element_type=jnp.float32)
    centre = proj - lax.optimization_barrier(jnp.mean(proj, -1, keepdims=True))
    inv_std = lax.rsqrt(lax.optimization_barrier(jnp.mean(centre * centre, -1, keepdims=True)) + EPS_NORM)
    normed = centre * inv_std
    upstream = grad_tiles.reshape(-1, depth).astype(jnp.float32)
    d_gain = lax.optimization_barrier(jnp.sum(upstream * normed, 0))
    scaled = upstream * gain
    d_proj = inv_std * (scaled - lax.optimization_barrier(jnp.mean(scaled, -1, keepdims=True)) - normed * lax.optimization_barrier(jnp.mean(scaled * normed, -1, keepdims=True)))
    d_proj = d_proj.astype(jnp.bfloat16)
    d_wproj = jnp.dot(attended.T, d_proj, preferred_element_type=jnp.float32)
    d_att = jnp.dot(d_proj, w_proj.T, preferred_element_type=jnp.float32).astype(jnp.bfloat16)
    d_att = d_att.reshape(images, count, length, heads, head_dim)
    d_probs = coarse_product('bnqhd,bnkhd->bnhqk', d_att, values)
    d_values = coarse_product('bnhqk,bnqhd->bnkhd', probs_low, d_att)
    d_scores = probs * (d_probs - lax.optimization_barrier(jnp.sum(d_probs * probs, -1, keepdims=True)))
    d_bias = lax.optimization_barrier(jnp.sum(d_scores, (0, 1))).reshape(heads, length * length)
    d_table = jnp.dot(d_bias, onehot, precision=HIGHEST) * (BIAS_RANGE * sigma * (1.0 - sigma))
    live = (logit_scale < SCALE_CAP).astype(jnp.float32)
    d_scale = lax.optimization_barrier(jnp.sum(d_scores * cosine, (0, 1, 3, 4))) * scale * live
    d_cos = d_scores * scale[:, None, None]
    d_unit_q = fine_product('bnhqk,bnkhd->bnqhd', d_cos, unit_key)
    d_unit_k = fine_product('bnhqk,bnqhd->bnkhd', d_cos, unit_query)
    d_query = query_inv * (d_unit_q - unit_query * lax.optimization_barrier(jnp.sum(unit_query * d_unit_q, -1, keepdims=True)))
    d_key = key_inv * (d_unit_k - unit_key * lax.optimization_barrier(jnp.sum(unit_key * d_unit_k, -1, keepdims=True)))
    d_qkv = jnp.stack([d_query, d_key, d_values], 3).astype(jnp.bfloat16).reshape(-1, 3 * depth)
    d_wqkv = jnp.dot(flat.T, d_qkv, preferred_element_type=jnp.float32)
    d_flat = jnp.dot(d_qkv, w_qkv.T, preferred_element_type=jnp.float32).astype(jnp.bfloat16)
    d_block = from_windows(d_flat.reshape(images, count, length, depth), images, rows, cols, window)
    return (d_block, (d_wqkv, d_wproj, d_table, d_scale, d_gain))

def reference(tokens, cotangent, w_qkv, w_proj, table_logits, logit_scale, gain):
    shift = WIN // 2
    images, height, width, depth = tokens.shape
    moved = jnp.roll(tokens, (-shift, -shift), axis=(1, 2))
    moved_grad = jnp.roll(cotangent, (-shift, -shift), axis=(1, 2))
    params = (w_qkv, w_proj, table_logits, logit_scale, gain)
    bands = height // WIN
    anchor = jnp.zeros((), jnp.int32)

    def one_band(totals, index):
        image = (index // bands).astype(jnp.int32)
        start = (index % bands * WIN).astype(jnp.int32)
        block = lax.dynamic_slice(moved, (image, start, anchor, anchor), (1, WIN, width, depth))
        grad_block = lax.dynamic_slice(moved_grad, (image, start, anchor, anchor), (1, WIN, width, depth))
        d_block, parts = grads_region(block, grad_block, start, anchor, height, width, WIN, params)
        return (jax.tree.map(jnp.add, totals, parts), d_block[0])
    initial = (jnp.zeros((depth, 3 * depth), jnp.float32), jnp.zeros((depth, depth), jnp.float32), jnp.zeros(table_logits.shape, jnp.float32), jnp.zeros(logit_scale.shape, jnp.float32), jnp.zeros(gain.shape, jnp.float32))
    totals, pieces = lax.scan(one_band, initial, jnp.arange(images * bands, dtype=jnp.int32))
    d_moved = pieces.reshape(images, height, width, depth)
    back = jnp.roll(d_moved, (shift, shift), axis=(1, 2))
    d_tokens = (cotangent.astype(jnp.float32) + back.astype(jnp.float32)).astype(jnp.bfloat16)
    return (d_tokens, totals[0], totals[1], totals[2], totals[3], totals[4])
```

```python
import functools
import math

import jax
import jax.numpy as jnp
from jax import lax
from jax.experimental import pallas as pl
from jax.experimental.pallas import tpu as pltpu
from jax.sharding import PartitionSpec as P

MESH = pl.DeviceIdType.MESH
F32 = jnp.float32
BF16 = jnp.bfloat16
HIGHEST = lax.Precision.HIGHEST

EPS_NORM = 1e-05
MASK_FILL = -100.0
OTHER_WINDOW = -1e30
SCALE_CAP = math.log(100.0)
BIAS_RANGE = 16.0

ROWS, COLS, C = 16, 32, 384
TOKENS = ROWS * COLS
HEADS = 12
GROUPS = 3
PER = 4
PAIRS = 4
TABLE = 225
CHUNKS = 3
BARRIER = 34

NT = (((1,), (1,)), ((), ()))
TN = (((0,), (0,)), ((), ()))
NN = (((1,), (0,)), ((), ()))


def dot(a, b, dims=NN):
    return lax.dot_general(a, b, dims, preferred_element_type=F32)


def fine(a, b, dims=NN):
    return lax.dot_general(a, b, dims, precision=HIGHEST, preferred_element_type=F32)


def iota(shape, dim):
    return lax.broadcasted_iota(jnp.int32, shape, dim)


def split(x):
    high = x.astype(BF16)
    low = (x - high.astype(F32)).astype(BF16)
    return jnp.concatenate([high, low], axis=1)


def offset_onehot():
    entry = iota((TABLE, 256), 0)
    row = lax.shift_right_logical(entry * 4370, 16)
    col = entry - 15 * row
    lane = (row - 7) * 16 + (col - 7)
    lane = jnp.where(lane < 0, lane + 256, lane)
    return (lane == iota((TABLE, 256), 1)).astype(F32)


def remote(src, dst, send, recv, device):
    return pltpu.make_async_remote_copy(
        src_ref=src, dst_ref=dst, send_sem=send, recv_sem=recv, device_id=device, device_id_type=MESH
    )


def kernel(
    tok, cot, wqkv, wproj, table, lscale, gain,
    dtok_o, f_s, total_o,
    pk_send, rows_recv, pk_recv, cr_recv,
    x_s, c_s, qkv_s, qinv_s, kinv_s, qrow_s, bias_s, mask_s, p_s, raw_s, att_s, datt_s, dproj_s, dqkv_s, dbias_s, dm_s,
    rows_send2, pk_send2, rows_recv2, pk_recv2, cr_recv2,
    keep_k, g_s, core_recv, s1_s, xy_recv, z_buf,
    sm_s, smc_recv, smx_buf, smz_buf, smf_buf,
    hsem_s, hsem_r, csem_s, csem_r, xsem_s, xsem_r, zsem_s, zsem_r, fsem_s, fsem_r,
):
    ha, wa, ba = lax.axis_index("ha"), lax.axis_index("wa"), lax.axis_index("ba")
    core = ha % 2
    deep = ha // 2
    other = ha + 1 - 2 * core
    up, down = (ha + 15) % 16, (ha + 1) % 16
    left, right = (wa + 7) % 8, (wa + 1) % 8
    mine = ba * 8 + wa
    row_mine = core * 8 + wa

    plane = []
    for d in range(1, 16):
        at = (mine + d) % 16
        plane.append((at // 8, at % 8))
    depth = [(deep + d) % 8 * 2 + core for d in range(1, 8)]
    level = []
    for d in range(1, 16):
        at = (row_mine + d) % 16
        level.append((deep * 2 + at // 8, at % 8))

    barrier = pltpu.get_barrier_semaphore()
    greeted = [(other, wa, ba)]
    greeted += [(ha, w, b) for b, w in plane]
    greeted += [(h, wa, ba) for h in depth]
    greeted += [(other, (wa + d) % 8, ba) for d in range(1, 8)]
    greeted += [(up, wa, ba), (down, wa, ba), (up, left, ba), (down, right, ba)]
    for device in greeted:
        pl.semaphore_signal(barrier, inc=1, device_id=device, device_id_type=MESH)

    sub8 = iota((8, C), 0) < 4

    for n, ref in enumerate((tok, cot)):
        for quad in range(4):
            x = ref[0, 4 * quad : 4 * quad + 4, 0:16, :].astype(F32).reshape(4, 2, 8, C)[:, 0]
            tiles = [jnp.where(sub8, x[2 * i], pltpu.roll(x[2 * i + 1], 4, 0)) for i in range(2)]
            pk_send[n, 16 * quad : 16 * quad + 16, :] = jnp.concatenate(tiles, 0).astype(BF16)

    onehot = offset_onehot()
    sigma = jax.nn.sigmoid(table[...])
    lanes = fine(sigma * BIAS_RANGE, onehot)
    for h in range(HEADS):
        line = jnp.broadcast_to(lanes[h : h + 1, :], (128, 256))
        bias_s[h] = pltpu.roll(line, 0, 1, stride=1, stride_axis=0)[:, :128]
    key, query = iota((128, 128), 0), iota((128, 128), 1)

    def bit(x, n):
        return lax.shift_right_logical(x, n) & 1

    apart = bit(key, 3) != bit(query, 3)
    low_rows = bit(key, 6) != bit(query, 6)
    low_cols = bit(key, 2) != bit(query, 2)
    second = bit(key, 3) == 1
    for pair in range(PAIRS):
        differ = jnp.zeros((128, 128), jnp.int32)
        if pair // 2 == 1:
            differ = jnp.where(low_rows, (ha == 15).astype(jnp.int32), differ)
        if pair % 2 == 1:
            differ = jnp.maximum(differ, jnp.where(low_cols & second, (wa == 7).astype(jnp.int32), 0))
        value = jnp.where(differ > 0, MASK_FILL, 0.0).astype(F32)
        mask_s[pair] = jnp.where(apart, OTHER_WINDOW, value)

    pl.semaphore_wait(barrier, BARRIER)
    halo = []
    for n, ref in enumerate((tok, cot)):
        halo.append(remote(ref.at[0, pl.ds(0, 4)], rows_recv.at[n], hsem_s.at[3 * n], hsem_r.at[3 * n], (up, wa, ba)))
        halo.append(remote(pk_send.at[n], pk_recv.at[n], hsem_s.at[3 * n + 1], hsem_r.at[3 * n + 1], (ha, left, ba)))
        halo.append(
            remote(pk_send.at[n, pl.ds(0, 16)], cr_recv.at[n], hsem_s.at[3 * n + 2], hsem_r.at[3 * n + 2], (up, left, ba))
        )
    for copy in halo:
        copy.start()
    for copy in halo:
        copy.wait()

    for n, (ref, out) in enumerate(((tok, x_s), (cot, c_s))):
        for quad in range(4):
            if quad < 3:
                rows = ref[0, 4 * quad + 4 : 4 * quad + 8]
                pack = pk_recv[n, 16 * quad + 16 : 16 * quad + 32, :]
            else:
                rows, pack = rows_recv[n], cr_recv[n]
            x = pltpu.roll(rows.astype(F32).reshape(16, 8, C), 4, 1).reshape(4, 4, 8, C)
            pack = pack.astype(F32).reshape(2, 8, C)
            for pair in range(2):
                parts = []
                for i in range(4):
                    for j in (2 * pair, 2 * pair + 1):
                        if j < 3:
                            after = x[i, j + 1]
                        else:
                            after = pack[i // 2] if i % 2 else pltpu.roll(pack[i // 2], 4, 0)
                        parts.append(jnp.where(sub8, x[i, j], after))
                at = (quad // 2 * 2 + pair) * 128 + quad % 2 * 64
                out[at : at + 64, :] = jnp.concatenate(parts, 0).astype(BF16)

    for part in range(3):
        for half in range(2):
            at = slice(256 * half, 256 * half + 256)
            y = dot(x_s[at, :], wqkv[:, C * part : C * part + C]).astype(BF16)
            for g in range(GROUPS):
                qkv_s[3 * part + g, at, :] = y[:, 128 * g : 128 * g + 128]

    head_lanes = [(lax.shift_right_logical(iota((1, 128), 1), 5) == h) for h in range(PER)]
    head_mask = [m.astype(F32).astype(BF16) for m in head_lanes]
    same = (lax.shift_right_logical(iota((256, 128), 0) & 127, 5) == lax.shift_right_logical(iota((256, 128), 1), 5))
    same = same.astype(F32).astype(BF16)
    pick = (lax.shift_right_logical(iota((8, 256), 1) & 127, 5) == iota((8, 256), 0)).astype(F32).astype(BF16)
    scales = jnp.exp(jnp.minimum(lscale[...], SCALE_CAP))

    def stacked(x):
        return jnp.concatenate([x * m for m in head_mask], axis=0)

    def across(x, h):
        return jnp.broadcast_to(x[:, 32 * h : 32 * h + 1], (128, 128))

    for g in range(GROUPS):
        scale_rows = jnp.concatenate(
            [jnp.broadcast_to(scales[:, PER * g + h : PER * g + h + 1], (1, 128)) for h in range(PER)], axis=0
        )

        def forward(pair, carry, g=g, scale_rows=scale_rows):
            at = pl.ds(pl.multiple_of(pair * 128, 128), 128)
            q, k, v = qkv_s[g, at, :], qkv_s[3 + g, at, :], qkv_s[6 + g, at, :]
            qf, kf = q.astype(F32), k.astype(F32)
            q2, k2 = split(qf * qf), split(kf * kf)
            qinv_s[g, at, :] = lax.rsqrt(dot(q2, same) + 1.0)
            kinv = lax.rsqrt(dot(k2, same) + 1.0)
            kinv_s[g, at, :] = kinv
            qrow = lax.rsqrt(dot(pick, q2, NT) + 1.0)[0:PER] * scale_rows
            qrow_s[g, pair, 0:PER, :] = qrow
            raw = dot(stacked(k), q, NT)
            low = []
            for h in range(PER):
                z = raw[128 * h : 128 * h + 128] * across(kinv, h) * qrow[h : h + 1]
                raw_s[g, pair, 128 * h : 128 * h + 128, :] = z
                z = z + bias_s[PER * g + h] + mask_s[pair]
                e = jnp.exp(z - jnp.max(z, axis=0, keepdims=True))
                p = e * (1.0 / jnp.sum(e, axis=0, keepdims=True))
                p_s[g, pair, 128 * h : 128 * h + 128, :] = p
                low.append(p.astype(BF16))
            att_s[g, at, :] = dot(jnp.concatenate(low, axis=0), stacked(v), TN).astype(BF16)
            return carry

        lax.fori_loop(0, PAIRS, forward, 0)

    dgain = jnp.zeros((1, C), F32)
    for pair in range(PAIRS):
        at = slice(128 * pair, 128 * pair + 128)
        att = jnp.concatenate([att_s[g, at, :] for g in range(GROUPS)], axis=1)
        proj = dot(att, wproj[...])
        centre = proj - jnp.mean(proj, -1, keepdims=True)
        inv_std = lax.rsqrt(jnp.mean(centre * centre, -1, keepdims=True) + EPS_NORM)
        normed = centre * inv_std
        upstream = c_s[at, :].astype(F32)
        dgain = dgain + jnp.sum(upstream * normed, 0, keepdims=True)
        scaled = upstream * gain[...].reshape(1, C)
        dproj = inv_std * (
            scaled - jnp.mean(scaled, -1, keepdims=True) - normed * jnp.mean(scaled * normed, -1, keepdims=True)
        )
        dproj = dproj.astype(BF16)
        dproj_s[at, :] = dproj
        datt = dot(dproj, wproj[...], NT).astype(BF16)
        for g in range(GROUPS):
            datt_s[g, at, :] = datt[:, 128 * g : 128 * g + 128]
    for g in range(GROUPS):
        sm_s[25 + g : 26 + g, :] = dgain[:, 128 * g : 128 * g + 128]
    sm_s[28:32, :] = jnp.zeros((4, 128), F32)

    att = [att_s[g] for g in range(GROUPS)]
    rows = [dot(dproj_s[...], a, TN).astype(BF16).reshape(2, 12, 16, 128) for a in att]
    for g in range(GROUPS):
        for half in range(2):
            g_s[0, 1, half, :, :, 128 * g : 128 * g + 128] = rows[g][half, 0:8]
            g_s[1, 1, half, 4:8, :, 128 * g : 128 * g + 128] = rows[g][half, 8:12]

    def core_copy(c):
        return remote(g_s.at[c, 1 - core], core_recv.at[c], csem_s.at[c], csem_r.at[c], (other, wa, ba))

    def plane_copies(c):
        return [
            remote(
                s1_s.at[c, b, w], xy_recv.at[c, d], xsem_s.at[c, d], xsem_r.at[c, d], (ha, w, b)
            )
            for d, (b, w) in enumerate(plane)
        ]

    def depth_copies(c):
        return [
            remote(z_buf.at[c, deep], z_buf.at[c, deep], zsem_s.at[c, d], zsem_r.at[c, d], (h, wa, ba))
            for d, h in enumerate(depth)
        ]

    def level_copies(c):
        return [
            remote(f_s.at[c, row_mine], f_s.at[c, row_mine], fsem_s.at[c, d], fsem_r.at[c, d], (h, w, ba))
            for d, (h, w) in enumerate(level)
        ]

    def wait_depth(c):
        for d in range(1, 8):
            at = (deep + 8 - d) % 8
            copy = remote(
                z_buf.at[c, deep], z_buf.at[c, at], zsem_s.at[c, d - 1], zsem_r.at[c, d - 1], (depth[d - 1], wa, ba)
            )
            copy.wait_send()
            copy.wait_recv()

    def wait_level(c):
        for d in range(1, 16):
            at = (row_mine + 16 - d) % 16
            h, w = level[d - 1]
            copy = remote(f_s.at[c, row_mine], f_s.at[c, at], fsem_s.at[c, d - 1], fsem_r.at[c, d - 1], (h, w, ba))
            copy.wait_send()
            copy.wait_recv()

    def start_all(copies):
        for copy in copies:
            copy.start()

    def to_plane(c):
        core_copy(c).wait()
        for b in range(2):
            s1_s[c, b] = (g_s[c, core, b].astype(F32) + core_recv[c, b].astype(F32)).astype(BF16)
        start_all(plane_copies(c))

    def to_depth(c):
        for copy in plane_copies(c):
            copy.wait()
        total = s1_s[c, ba, wa].astype(F32)
        for d in range(15):
            total = total + xy_recv[c, d].astype(F32)
        z_buf[c, deep] = total.astype(BF16)
        start_all(depth_copies(c))

    def to_level(c):
        wait_depth(c)
        total = z_buf[c, 0].astype(F32)
        for d in range(1, 8):
            total = total + z_buf[c, d].astype(F32)
        f_s[c, row_mine] = total.astype(BF16)
        start_all(level_copies(c))

    for g in range(GROUPS):

        def backward(pair, dscale, g=g):
            at = pl.ds(pl.multiple_of(pair * 128, 128), 128)
            q, k, v = qkv_s[g, at, :], qkv_s[3 + g, at, :], qkv_s[6 + g, at, :]
            datt = datt_s[g, at, :]
            qinv, kinv = qinv_s[g, at, :], kinv_s[g, at, :]
            raw = dot(stacked(v), datt, NT)
            low, grads, sums = [], [], []
            for h in range(PER):
                p = p_s[g, pair, 128 * h : 128 * h + 128, :]
                dp = raw[128 * h : 128 * h + 128]
                ds = p * (dp - jnp.sum(dp * p, axis=0, keepdims=True))
                dbias_s[PER * g + h] = jnp.where(pair == 0, 0.0, dbias_s[PER * g + h]) + ds
                sums.append(jnp.sum(ds * raw_s[g, pair, 128 * h : 128 * h + 128, :], axis=0, keepdims=True))
                grads.append((ds * across(kinv, h) * qrow_s[g, pair, h : h + 1, :]).astype(BF16))
                low.append(p.astype(BF16))
            dv = dot(jnp.concatenate(low, axis=1), stacked(datt))
            a = dot(jnp.concatenate(grads, axis=0), stacked(k), TN)
            b = dot(jnp.concatenate(grads, axis=1), stacked(q))
            qf, kf = q.astype(F32), k.astype(F32)
            uq, uk = qf * qinv, kf * kinv
            dq = a - uq * dot(split(uq * a), same)
            dk = b - uk * dot(split(uk * b), same)
            dqkv_s[g, at, 0:128] = dq.astype(BF16)
            dqkv_s[g, at, 128:256] = dk.astype(BF16)
            dqkv_s[g, at, 256:384] = dv.astype(BF16)
            return dscale + jnp.concatenate(sums, axis=0)

        dscale = lax.fori_loop(0, PAIRS, backward, jnp.zeros((PER, 128), F32))
        here = iota((PER, 128), 0) + PER * g == iota((PER, 128), 1)
        spread = jnp.where(here, jnp.sum(dscale, axis=1, keepdims=True), 0.0)
        spread = jnp.sum(spread, axis=0, keepdims=True)
        scale_row = spread if g == 0 else scale_row + spread
        for part in range(3):
            dw = dot(dqkv_s[g, :, 128 * part : 128 * part + 128], x_s[...], TN).astype(BF16).reshape(8, 16, C)
            if part == 0:
                g_s[g, 0, 0] = dw
            elif part == 2:
                g_s[g, 0, 1] = dw
            elif g == 0:
                keep_k[...] = dw
            elif g == 1:
                g_s[1, 1, 0, 0:4] = dw[0:4]
                g_s[1, 1, 1, 0:4] = dw[4:8]
            else:
                g_s[2, 1, 0] = keep_k[...]
                g_s[2, 1, 1] = dw
        core_copy(g).start()
        if g > 0:
            to_plane(g - 1)

    sm_s[24:25, :] = scale_row

    lane8, sub256 = iota((8, 128), 1), iota((8, 256), 0)
    for h in range(HEADS):
        ahead = dbias_s[h, 0:8, :]
        behind = jnp.zeros((8, 128), F32)
        for n in range(1, 16):
            turned = pltpu.roll(dbias_s[h, 8 * n : 8 * n + 8, :], 128 - 8 * n, 1)
            inside = lane8 < 128 - 8 * n
            ahead = ahead + jnp.where(inside, turned, 0.0)
            behind = behind + jnp.where(inside, 0.0, turned)
        both = jnp.concatenate([ahead, behind], axis=1)
        for n in range(3):
            both = jnp.where(bit(sub256, n) == 1, pltpu.roll(both, 256 - 2**n, 1), both)
        both = jnp.sum(both, axis=0, keepdims=True)
        sm_s[h : h + 1, :] = both[:, 0:128]
        sm_s[12 + h : 13 + h, :] = both[:, 128:256]
    small_core = remote(
        sm_s.at[pl.ds(pl.multiple_of(16 * (1 - core), 16), 16)], smc_recv, csem_s.at[3], csem_r.at[3], (other, wa, ba)
    )
    small_core.start()

    to_plane(2)

    for pair in range(PAIRS):
        at = slice(128 * pair, 128 * pair + 128)
        total = jnp.zeros((128, C), F32)
        for g in range(GROUPS):
            w = jnp.concatenate([wqkv[:, C * n + 128 * g : C * n + 128 * g + 128] for n in range(3)], axis=1)
            total = total + dot(dqkv_s[g, at, :], w, NT)
        dm_s[at, :] = total.astype(BF16)

    def image_rows(quad):
        parts = []
        for i in range(4):
            for pair in range(2):
                at = (quad // 2 * 2 + pair) * 128 + quad % 2 * 64 + 16 * i
                parts.append(dm_s[at : at + 16, :])
        return jnp.concatenate(parts, axis=0).reshape(4, 32, C)

    for quad in range(4):
        x = image_rows(quad)
        if quad == 3:
            rows_send2[...] = x
        x = x.astype(F32).reshape(4, 4, 8, C)
        tiles = [jnp.where(sub8, pltpu.roll(x[2 * i, 3], 4, 0), x[2 * i + 1, 3]) for i in range(2)]
        pk_send2[16 * quad : 16 * quad + 16, :] = jnp.concatenate(tiles, 0).astype(BF16)
    halo = [
        remote(rows_send2, rows_recv2, hsem_s.at[6], hsem_r.at[6], (down, wa, ba)),
        remote(pk_send2, pk_recv2, hsem_s.at[7], hsem_r.at[7], (ha, right, ba)),
        remote(pk_send2.at[pl.ds(48, 16)], cr_recv2, hsem_s.at[8], hsem_r.at[8], (down, right, ba)),
    ]
    start_all(halo)

    small_core.wait()
    mine16 = sm_s[pl.ds(pl.multiple_of(16 * core, 16), 16), :]
    smx_buf[mine] = mine16 + smc_recv[...]
    small_plane = [
        remote(smx_buf.at[mine], smx_buf.at[mine], xsem_s.at[3, d], xsem_r.at[3, d], (ha, w, b))
        for d, (b, w) in enumerate(plane)
    ]
    start_all(small_plane)

    for c in range(CHUNKS):
        to_depth(c)

    for d in range(1, 16):
        at = (mine + 16 - d) % 16
        b, w = plane[d - 1]
        copy = remote(smx_buf.at[mine], smx_buf.at[at], xsem_s.at[3, d - 1], xsem_r.at[3, d - 1], (ha, w, b))
        copy.wait_send()
        copy.wait_recv()
    total = smx_buf[0]
    for d in range(1, 16):
        total = total + smx_buf[d]
    smz_buf[deep] = total
    small_depth = [
        remote(smz_buf.at[deep], smz_buf.at[deep], zsem_s.at[3, d], zsem_r.at[3, d], (h, wa, ba))
        for d, h in enumerate(depth)
    ]
    start_all(small_depth)

    for copy in halo:
        copy.wait()
    for quad in range(4):
        if quad == 0:
            rows, pack = rows_recv2[...], cr_recv2[...]
        else:
            rows, pack = image_rows(quad - 1), pk_recv2[16 * quad - 16 : 16 * quad, :]
        x = pltpu.roll(rows.astype(F32).reshape(16, 8, C), 4, 1).reshape(4, 4, 8, C)
        pack = pack.astype(F32).reshape(2, 8, C)
        for i in range(4):
            parts = []
            for j in range(4):
                if j > 0:
                    before = x[i, j - 1]
                else:
                    before = pltpu.roll(pack[i // 2], 4, 0) if i % 2 else pack[i // 2]
                parts.append(jnp.where(sub8, before, x[i, j]))
            back = jnp.concatenate(parts, 0)
            row = 4 * quad + i
            dtok_o[0, row] = (cot[0, row].astype(F32) + back).astype(BF16)

    for c in range(CHUNKS):
        to_level(c)

    for d in range(1, 8):
        at = (deep + 8 - d) % 8
        copy = remote(
            smz_buf.at[deep], smz_buf.at[at], zsem_s.at[3, d - 1], zsem_r.at[3, d - 1], (depth[d - 1], wa, ba)
        )
        copy.wait_send()
        copy.wait_recv()
    total = smz_buf[0]
    for d in range(1, 8):
        total = total + smz_buf[d]
    smf_buf[core] = total
    small_last = remote(smf_buf.at[core], smf_buf.at[core], csem_s.at[4], csem_r.at[4], (other, wa, ba))
    small_last.start()

    for c in range(CHUNKS):
        wait_level(c)

    copy = remote(smf_buf.at[core], smf_buf.at[1 - core], csem_s.at[4], csem_r.at[4], (other, wa, ba))
    copy.wait_send()
    copy.wait_recv()
    total_o[0:16, :] = smf_buf[0]
    total_o[16:32, :] = smf_buf[1]


def finish(pieces, total, moved, table, lscale, dtok_o, dwqkv_o, dwproj_o, dtable_o, dscale_o, dgain_o):
    ba = lax.axis_index("ba")
    dtok_o[...] = moved[...]

    def rows(base, count):
        return pl.ds(pl.multiple_of(base, 64), count)

    def join(c, core, first, count):
        return pieces[c, 8 * core + first : 8 * core + first + count].reshape(16 * count, C).astype(F32)

    for c in range(CHUNKS):
        dwqkv_o[rows(128 * c + 192 * ba, 128), :] = join(c, 0, 0, 8)
    dwproj_o[0:128, :] = join(0, 1, 0, 8)
    dwqkv_o[rows(512 - 512 * ba, 64), :] = join(1, 1, 0, 4)
    dwproj_o[128:192, :] = join(1, 1, 4, 4)
    dwqkv_o[rows(384 - 320 * ba, 128), :] = join(2, 1, 0, 8)

    by_lane = jnp.concatenate([total[0:12], total[12:24]], axis=1)
    sigma = jax.nn.sigmoid(table[...])
    dtable_o[...] = fine(by_lane, offset_onehot(), NT) * (BIAS_RANGE * sigma * (1.0 - sigma))
    live = (lscale[...] < SCALE_CAP).astype(F32)
    dscale_o[...] = total[24:25, 0:HEADS] * live
    for g in range(GROUPS):
        dgain_o[pl.ds(128 * g, 128)] = total[25 + g]


def step(tokens, cotangent, w_qkv, w_proj, table_logits, logit_scale, gain):
    vmem = pl.BlockSpec(memory_space=pltpu.VMEM)
    middle = [
        jax.ShapeDtypeStruct((1, ROWS, COLS, C), BF16),
        jax.ShapeDtypeStruct((CHUNKS, 16, 16, C), BF16),
        jax.ShapeDtypeStruct((32, 128), F32),
    ]
    outs = [
        jax.ShapeDtypeStruct((1, ROWS, COLS, C), BF16),
        jax.ShapeDtypeStruct((576, C), F32),
        jax.ShapeDtypeStruct((192, C), F32),
        jax.ShapeDtypeStruct((HEADS, TABLE), F32),
        jax.ShapeDtypeStruct((1, HEADS), F32),
        jax.ShapeDtypeStruct((C,), F32),
    ]
    scratch = [
        pltpu.VMEM((2, 64, C), BF16),
        pltpu.VMEM((2, 4, COLS, C), BF16),
        pltpu.VMEM((2, 64, C), BF16),
        pltpu.VMEM((2, 16, C), BF16),
        pltpu.VMEM((TOKENS, C), BF16),
        pltpu.VMEM((TOKENS, C), BF16),
        pltpu.VMEM((9, TOKENS, 128), BF16),
        pltpu.VMEM((GROUPS, TOKENS, 128), F32),
        pltpu.VMEM((GROUPS, TOKENS, 128), F32),
        pltpu.VMEM((GROUPS, PAIRS, 8, 128), F32),
        pltpu.VMEM((HEADS, 128, 128), F32),
        pltpu.VMEM((PAIRS, 128, 128), F32),
        pltpu.VMEM((GROUPS, PAIRS, TOKENS, 128), F32),
        pltpu.VMEM((GROUPS, PAIRS, TOKENS, 128), F32),
        pltpu.VMEM((GROUPS, TOKENS, 128), BF16),
        pltpu.VMEM((GROUPS, TOKENS, 128), BF16),
        pltpu.VMEM((TOKENS, C), BF16),
        pltpu.VMEM((GROUPS, TOKENS, C), BF16),
        pltpu.VMEM((HEADS, 128, 128), F32),
        pltpu.VMEM((TOKENS, C), BF16),
        pltpu.VMEM((4, COLS, C), BF16),
        pltpu.VMEM((64, C), BF16),
        pltpu.VMEM((4, COLS, C), BF16),
        pltpu.VMEM((64, C), BF16),
        pltpu.VMEM((16, C), BF16),
        pltpu.VMEM((8, 16, C), BF16),
        pltpu.VMEM((CHUNKS, 2, 2, 8, 16, C), BF16),
        pltpu.VMEM((CHUNKS, 2, 8, 16, C), BF16),
        pltpu.VMEM((CHUNKS, 2, 8, 16, C), BF16),
        pltpu.VMEM((CHUNKS, 15, 16, C), BF16),
        pltpu.VMEM((CHUNKS, 8, 16, C), BF16),
        pltpu.VMEM((32, 128), F32),
        pltpu.VMEM((16, 128), F32),
        pltpu.VMEM((16, 16, 128), F32),
        pltpu.VMEM((8, 16, 128), F32),
        pltpu.VMEM((2, 16, 128), F32),
        pltpu.SemaphoreType.DMA((9,)),
        pltpu.SemaphoreType.DMA((9,)),
        pltpu.SemaphoreType.DMA((5,)),
        pltpu.SemaphoreType.DMA((5,)),
        pltpu.SemaphoreType.DMA((4, 15)),
        pltpu.SemaphoreType.DMA((4, 15)),
        pltpu.SemaphoreType.DMA((4, 7)),
        pltpu.SemaphoreType.DMA((4, 7)),
        pltpu.SemaphoreType.DMA((3, 15)),
        pltpu.SemaphoreType.DMA((3, 15)),
    ]
    lscale = logit_scale.reshape(1, HEADS)
    moved, pieces, total = pl.pallas_call(
        kernel,
        name="window_backward",
        out_shape=middle,
        in_specs=[vmem] * 7,
        out_specs=[vmem] * 3,
        scratch_shapes=scratch,
        compiler_params=pltpu.CompilerParams(collective_id=0, has_side_effects=True),
    )(tokens, cotangent, w_qkv, w_proj, table_logits, lscale, gain)
    d_tokens, d_wqkv, d_wproj, d_table, d_scale, d_gain = pl.pallas_call(
        finish, name="finish", out_shape=outs, in_specs=[vmem] * 5, out_specs=[vmem] * 6
    )(pieces, total, moved, table_logits, lscale)
    return d_tokens, d_wqkv.T, d_wproj.T, d_table, d_scale.reshape(HEADS), d_gain


def solution(mesh):
    image = P("ba", "ha", "wa", None)
    return jax.shard_map(
        step,
        mesh=mesh,
        in_specs=(image, image, P(), P(), P(), P(), P()),
        out_specs=(image, P(None, "ba"), P(None, "ba"), P(), P(), P()),
        check_vma=False,
    )
```

```python
import functools
import math

import jax
import jax.numpy as jnp
from jax import lax
from jax.experimental import pallas as pl
from jax.experimental.pallas import tpu as pltpu
from jax.sharding import PartitionSpec as P

MESH = pl.DeviceIdType.MESH
F32 = jnp.float32
BF16 = jnp.bfloat16
HIGHEST = lax.Precision.HIGHEST

EPS_NORM = 1e-05
MASK_FILL = -100.0
OTHER_WINDOW = -1e30
SCALE_CAP = math.log(100.0)
BIAS_RANGE = 16.0

ROWS, COLS, C = 16, 32, 384
TOKENS = ROWS * COLS
HEADS = 12
GROUPS = 3
PER = 4
PAIRS = 4
TABLE = 225
CHUNKS = 3
BARRIER = 34

NT = (((1,), (1,)), ((), ()))
TN = (((0,), (0,)), ((), ()))
NN = (((1,), (0,)), ((), ()))


def dot(a, b, dims=NN):
    return lax.dot_general(a, b, dims, preferred_element_type=F32)


def fine(a, b, dims=NN):
    return lax.dot_general(a, b, dims, precision=HIGHEST, preferred_element_type=F32)


def iota(shape, dim):
    return lax.broadcasted_iota(jnp.int32, shape, dim)


def split(x):
    high = x.astype(BF16)
    low = (x - high.astype(F32)).astype(BF16)
    return jnp.concatenate([high, low], axis=1)


def offset_onehot():
    entry = iota((TABLE, 256), 0)
    row = lax.shift_right_logical(entry * 4370, 16)
    col = entry - 15 * row
    lane = (row - 7) * 16 + (col - 7)
    lane = jnp.where(lane < 0, lane + 256, lane)
    return (lane == iota((TABLE, 256), 1)).astype(F32)


def remote(src, dst, send, recv, device):
    return pltpu.make_async_remote_copy(
        src_ref=src, dst_ref=dst, send_sem=send, recv_sem=recv, device_id=device, device_id_type=MESH
    )


def kernel(
    tok_h, cot_h, wqkv_h, wproj_h, table_h, lscale, gain,
    dtok_o, f_s, total_o,
    tok, cot, wqkv, wproj, table,
    pk_send, rows_recv, pk_recv, cr_recv,
    x_s, c_s, qkv_s, qinv_s, kinv_s, qrow_s, bias_s, mask_s, p_s, raw_s, att_s, datt_s, dproj_s, dqkv_s, dbias_s, dm_s,
    rows_send2, pk_send2, rows_recv2, pk_recv2, cr_recv2,
    keep_k, g_s, core_recv, s1_s, xy_recv, z_buf,
    sm_s, smc_recv, smx_buf, smz_buf, smf_buf,
    lsem, hsem_s, hsem_r, csem_s, csem_r, xsem_s, xsem_r, zsem_s, zsem_r, fsem_s, fsem_r,
):
    loads = [
        pltpu.make_async_copy(src, dst, lsem.at[n])
        for n, (src, dst) in enumerate(
            ((tok_h, tok), (cot_h, cot), (table_h, table), (wqkv_h, wqkv), (wproj_h, wproj))
        )
    ]
    for load in loads:
        load.start()

    ha, wa, ba = lax.axis_index("ha"), lax.axis_index("wa"), lax.axis_index("ba")
    core = ha % 2
    deep = ha // 2
    other = ha + 1 - 2 * core
    up, down = (ha + 15) % 16, (ha + 1) % 16
    left, right = (wa + 7) % 8, (wa + 1) % 8
    mine = ba * 8 + wa
    row_mine = core * 8 + wa

    plane = []
    for d in range(1, 16):
        at = (mine + d) % 16
        plane.append((at // 8, at % 8))
    depth = [(deep + d) % 8 * 2 + core for d in range(1, 8)]
    level = []
    for d in range(1, 16):
        at = (row_mine + d) % 16
        level.append((deep * 2 + at // 8, at % 8))

    barrier = pltpu.get_barrier_semaphore()
    greeted = [(other, wa, ba)]
    greeted += [(ha, w, b) for b, w in plane]
    greeted += [(h, wa, ba) for h in depth]
    greeted += [(other, (wa + d) % 8, ba) for d in range(1, 8)]
    greeted += [(up, wa, ba), (down, wa, ba), (up, left, ba), (down, right, ba)]
    for device in greeted:
        pl.semaphore_signal(barrier, inc=1, device_id=device, device_id_type=MESH)

    sub8 = iota((8, C), 0) < 4


    loads[0].wait()
    loads[1].wait()
    for n, ref in enumerate((tok, cot)):
        for quad in range(4):
            x = ref[0, 4 * quad : 4 * quad + 4, 0:16, :].astype(F32).reshape(4, 2, 8, C)[:, 0]
            tiles = [jnp.where(sub8, x[2 * i], pltpu.roll(x[2 * i + 1], 4, 0)) for i in range(2)]
            pk_send[n, 16 * quad : 16 * quad + 16, :] = jnp.concatenate(tiles, 0).astype(BF16)


    loads[2].wait()
    onehot = offset_onehot()
    sigma = jax.nn.sigmoid(table[...])
    lanes = fine(sigma * BIAS_RANGE, onehot)
    for h in range(HEADS):
        line = jnp.broadcast_to(lanes[h : h + 1, :], (128, 256))
        bias_s[h] = pltpu.roll(line, 0, 1, stride=1, stride_axis=0)[:, :128]
    key, query = iota((128, 128), 0), iota((128, 128), 1)

    def bit(x, n):
        return lax.shift_right_logical(x, n) & 1

    apart = bit(key, 3) != bit(query, 3)
    low_rows = bit(key, 6) != bit(query, 6)
    low_cols = bit(key, 2) != bit(query, 2)
    second = bit(key, 3) == 1
    for pair in range(PAIRS):
        differ = jnp.zeros((128, 128), jnp.int32)
        if pair // 2 == 1:
            differ = jnp.where(low_rows, (ha == 15).astype(jnp.int32), differ)
        if pair % 2 == 1:
            differ = jnp.maximum(differ, jnp.where(low_cols & second, (wa == 7).astype(jnp.int32), 0))
        value = jnp.where(differ > 0, MASK_FILL, 0.0).astype(F32)
        mask_s[pair] = jnp.where(apart, OTHER_WINDOW, value)


    pl.semaphore_wait(barrier, BARRIER)
    for n, ref in enumerate((tok, cot)):
        remote(ref.at[0, pl.ds(0, 4)], rows_recv.at[n], hsem_s.at[0], hsem_r.at[0], (up, wa, ba)).start()
        remote(pk_send.at[n], pk_recv.at[n], hsem_s.at[1], hsem_r.at[1], (ha, left, ba)).start()
        remote(pk_send.at[n, pl.ds(0, 16)], cr_recv.at[n], hsem_s.at[2], hsem_r.at[2], (up, left, ba)).start()

    def shifted(quad, pair):
        for n, (ref, out) in enumerate(((tok, x_s), (cot, c_s))):
            if quad < 3:
                rows = ref[0, 4 * quad + 4 : 4 * quad + 8]
            else:
                rows = rows_recv[n]
            x = pltpu.roll(rows.astype(F32).reshape(16, 8, C), 4, 1).reshape(4, 4, 8, C)
            if pair == 1:
                pack = pk_recv[n, 16 * quad + 16 : 16 * quad + 32, :] if quad < 3 else cr_recv[n]
                pack = pack.astype(F32).reshape(2, 8, C)
            parts = []
            for i in range(4):
                for j in (2 * pair, 2 * pair + 1):
                    if j < 3:
                        after = x[i, j + 1]
                    else:
                        after = pack[i // 2] if i % 2 else pltpu.roll(pack[i // 2], 4, 0)
                    parts.append(jnp.where(sub8, x[i, j], after))
            at = (quad // 2 * 2 + pair) * 128 + quad % 2 * 64
            out[at : at + 64, :] = jnp.concatenate(parts, 0).astype(BF16)

    def projected(first, count):
        at = slice(128 * first, 128 * (first + count))
        x = x_s[at, :]
        for part in range(3):
            y = dot(x, wqkv[:, C * part : C * part + C]).astype(BF16)
            for g in range(GROUPS):
                one = y[:, 128 * g : 128 * g + 128]
                qkv_s[3 * part + g, at, :] = one
                if part == 2:
                    continue
                wide = one.astype(F32)
                square = split(wide * wide)
                inverse = lax.rsqrt(dot(square, same) + 1.0)
                if part == 1:
                    kinv_s[g, at, :] = inverse
                    continue
                qinv_s[g, at, :] = inverse
                across_rows = lax.rsqrt(dot(pick, square, NT) + 1.0)
                for n in range(count):
                    qrow_s[g, first + n, 0:PER, :] = across_rows[0:PER, 128 * n : 128 * n + 128] * scale_rows[g]

    head_lanes = [(lax.shift_right_logical(iota((1, 128), 1), 5) == h) for h in range(PER)]
    head_mask = [m.astype(F32).astype(BF16) for m in head_lanes]
    same = (lax.shift_right_logical(iota((256, 128), 0) & 127, 5) == lax.shift_right_logical(iota((256, 128), 1), 5))
    same = same.astype(F32).astype(BF16)
    pick = (lax.shift_right_logical(iota((8, 256), 1) & 127, 5) == iota((8, 256), 0)).astype(F32).astype(BF16)
    scales = jnp.exp(jnp.minimum(lscale[...], SCALE_CAP))
    scale_rows = [
        jnp.concatenate(
            [jnp.broadcast_to(scales[:, PER * g + h : PER * g + h + 1], (1, 128)) for h in range(PER)], axis=0
        )
        for g in range(GROUPS)
    ]

    def stacked(x):
        return jnp.concatenate([x * m for m in head_mask], axis=0)

    def across(x, h):
        return jnp.broadcast_to(x[:, 32 * h : 32 * h + 1], (128, 128))

    def forward(g, pair):
        at = slice(128 * pair, 128 * pair + 128)
        q, k, v = qkv_s[g, at, :], qkv_s[3 + g, at, :], qkv_s[6 + g, at, :]
        kinv = kinv_s[g, at, :]
        raw = dot(stacked(k), q, NT)
        low = []
        for h in range(PER):
            z = raw[128 * h : 128 * h + 128] * across(kinv, h) * qrow_s[g, pair, h : h + 1, :]
            raw_s[g, pair, 128 * h : 128 * h + 128, :] = z
            z = z + bias_s[PER * g + h] + mask_s[pair]
            e = jnp.exp(z - jnp.max(z, axis=0, keepdims=True))
            p = e * (1.0 / jnp.sum(e, axis=0, keepdims=True))
            p_s[g, pair, 128 * h : 128 * h + 128, :] = p
            low.append(p.astype(BF16))
        att_s[g, at, :] = dot(jnp.concatenate(low, axis=0), stacked(v), TN).astype(BF16)


    for quad in range(2):
        shifted(quad, 0)
    loads[3].wait()
    projected(0, 1)
    for g in range(GROUPS):
        forward(g, 0)


    def taken(ref, send, recv):
        pltpu.make_async_copy(ref, ref, send).wait()
        pltpu.make_async_copy(ref, ref, recv).wait()

    for n, ref in enumerate((rows_recv, pk_recv, cr_recv)):
        taken(ref, hsem_s.at[n], hsem_r.at[n])

    for quad in range(4):
        shifted(quad, 1)
        if quad > 1:
            shifted(quad, 0)

    projected(1, 3)

    for g in range(GROUPS):
        for pair in range(1, PAIRS):
            forward(g, pair)
    loads[4].wait()


    dgain = jnp.zeros((1, C), F32)
    for pair in range(PAIRS):
        at = slice(128 * pair, 128 * pair + 128)
        att = jnp.concatenate([att_s[g, at, :] for g in range(GROUPS)], axis=1)
        proj = dot(att, wproj[...])
        centre = proj - jnp.mean(proj, -1, keepdims=True)
        inv_std = lax.rsqrt(jnp.mean(centre * centre, -1, keepdims=True) + EPS_NORM)
        normed = centre * inv_std
        upstream = c_s[at, :].astype(F32)
        dgain = dgain + jnp.sum(upstream * normed, 0, keepdims=True)
        scaled = upstream * gain[...].reshape(1, C)
        dproj = inv_std * (
            scaled - jnp.mean(scaled, -1, keepdims=True) - normed * jnp.mean(scaled * normed, -1, keepdims=True)
        )
        dproj = dproj.astype(BF16)
        dproj_s[at, :] = dproj
        datt = dot(dproj, wproj[...], NT).astype(BF16)
        for g in range(GROUPS):
            datt_s[g, at, :] = datt[:, 128 * g : 128 * g + 128]
    for g in range(GROUPS):
        sm_s[25 + g : 26 + g, :] = dgain[:, 128 * g : 128 * g + 128]
    sm_s[28:32, :] = jnp.zeros((4, 128), F32)


    att = [att_s[g] for g in range(GROUPS)]
    rows = [dot(dproj_s[...], a, TN).astype(BF16).reshape(2, 12, 16, 128) for a in att]
    for g in range(GROUPS):
        for half in range(2):
            g_s[0, 1, half, :, :, 128 * g : 128 * g + 128] = rows[g][half, 0:8]
            g_s[1, 1, half, 4:8, :, 128 * g : 128 * g + 128] = rows[g][half, 8:12]

    def core_copy(c):
        return remote(g_s.at[c, 1 - core], core_recv.at[c], csem_s.at[c], csem_r.at[c], (other, wa, ba))

    def to_plane(c):
        core_copy(c).wait()
        for b in range(2):
            s1_s[c, b] = (g_s[c, core, b].astype(F32) + core_recv[c, b].astype(F32)).astype(BF16)
        for d, (b, w) in enumerate(plane):
            remote(s1_s.at[c, b, w], xy_recv.at[c, d], xsem_s.at[c], xsem_r.at[c], (ha, w, b)).start()

    def to_depth(c):
        taken(xy_recv.at[c], xsem_s.at[c], xsem_r.at[c])
        total = s1_s[c, ba, wa].astype(F32)
        for d in range(15):
            total = total + xy_recv[c, d].astype(F32)
        z_buf[c, deep] = total.astype(BF16)
        for h in depth:
            remote(z_buf.at[c, deep], z_buf.at[c, deep], zsem_s.at[c], zsem_r.at[c], (h, wa, ba)).start()

    def to_level(c):
        taken(z_buf.at[c, pl.ds(0, 7)], zsem_s.at[c], zsem_r.at[c])
        total = z_buf[c, 0].astype(F32)
        for d in range(1, 8):
            total = total + z_buf[c, d].astype(F32)
        f_s[c, row_mine] = total.astype(BF16)
        for h, w in level:
            remote(f_s.at[c, row_mine], f_s.at[c, row_mine], fsem_s.at[c], fsem_r.at[c], (h, w, ba)).start()

    def wait_level(c):
        taken(f_s.at[c, pl.ds(0, 15)], fsem_s.at[c], fsem_r.at[c])


    for g in range(GROUPS):

        dscale = jnp.zeros((PER, 128), F32)
        for pair in range(PAIRS):
            at = slice(128 * pair, 128 * pair + 128)
            q, k, v = qkv_s[g, at, :], qkv_s[3 + g, at, :], qkv_s[6 + g, at, :]
            datt = datt_s[g, at, :]
            qinv, kinv = qinv_s[g, at, :], kinv_s[g, at, :]
            raw = dot(stacked(v), datt, NT)
            low, grads, sums = [], [], []
            for h in range(PER):
                p = p_s[g, pair, 128 * h : 128 * h + 128, :]
                dp = raw[128 * h : 128 * h + 128]
                ds = p * (dp - jnp.sum(dp * p, axis=0, keepdims=True))
                if pair == 0:
                    dbias_s[PER * g + h] = ds
                else:
                    dbias_s[PER * g + h] += ds
                sums.append(jnp.sum(ds * raw_s[g, pair, 128 * h : 128 * h + 128, :], axis=0, keepdims=True))
                grads.append((ds * across(kinv, h) * qrow_s[g, pair, h : h + 1, :]).astype(BF16))
                low.append(p.astype(BF16))
            dv = dot(jnp.concatenate(low, axis=1), stacked(datt))
            a = dot(jnp.concatenate(grads, axis=0), stacked(k), TN)
            b = dot(jnp.concatenate(grads, axis=1), stacked(q))
            qf, kf = q.astype(F32), k.astype(F32)
            uq, uk = qf * qinv, kf * kinv
            dq = a - uq * dot(split(uq * a), same)
            dk = b - uk * dot(split(uk * b), same)
            dqkv_s[g, at, 0:128] = dq.astype(BF16)
            dqkv_s[g, at, 128:256] = dk.astype(BF16)
            dqkv_s[g, at, 256:384] = dv.astype(BF16)
            dscale = dscale + jnp.concatenate(sums, axis=0)
            if g > 0 and pair == 1:
                to_plane(g - 1)

        here = iota((PER, 128), 0) + PER * g == iota((PER, 128), 1)
        spread = jnp.where(here, jnp.sum(dscale, axis=1, keepdims=True), 0.0)
        spread = jnp.sum(spread, axis=0, keepdims=True)
        scale_row = spread if g == 0 else scale_row + spread
        for part in range(3):
            dw = dot(dqkv_s[g, :, 128 * part : 128 * part + 128], x_s[...], TN).astype(BF16).reshape(8, 16, C)
            if part == 0:
                g_s[g, 0, 0] = dw
            elif part == 2:
                g_s[g, 0, 1] = dw
            elif g == 0:
                keep_k[...] = dw
            elif g == 1:
                g_s[1, 1, 0, 0:4] = dw[0:4]
                g_s[1, 1, 1, 0:4] = dw[4:8]
            else:
                g_s[2, 1, 0] = keep_k[...]
                g_s[2, 1, 1] = dw
        core_copy(g).start()


    sm_s[24:25, :] = scale_row

    lane8, sub256 = iota((8, 128), 1), iota((8, 256), 0)
    for h in range(HEADS):
        ahead = dbias_s[h, 0:8, :]
        behind = jnp.zeros((8, 128), F32)
        for n in range(1, 16):
            turned = pltpu.roll(dbias_s[h, 8 * n : 8 * n + 8, :], 128 - 8 * n, 1)
            inside = lane8 < 128 - 8 * n
            ahead = ahead + jnp.where(inside, turned, 0.0)
            behind = behind + jnp.where(inside, 0.0, turned)
        both = jnp.concatenate([ahead, behind], axis=1)
        for n in range(3):
            both = jnp.where(bit(sub256, n) == 1, pltpu.roll(both, 256 - 2**n, 1), both)
        both = jnp.sum(both, axis=0, keepdims=True)
        sm_s[h : h + 1, :] = both[:, 0:128]
        sm_s[12 + h : 13 + h, :] = both[:, 128:256]
    small_core = remote(
        sm_s.at[pl.ds(pl.multiple_of(16 * (1 - core), 16), 16)], smc_recv, csem_s.at[3], csem_r.at[3], (other, wa, ba)
    )
    small_core.start()


    to_plane(2)


    small_core.wait()
    smx_buf[mine] = sm_s[pl.ds(pl.multiple_of(16 * core, 16), 16), :] + smc_recv[...]
    for b, w in plane:
        remote(smx_buf.at[mine], smx_buf.at[mine], xsem_s.at[3], xsem_r.at[3], (ha, w, b)).start()


    for pair in range(PAIRS):
        at = slice(128 * pair, 128 * pair + 128)
        total = jnp.zeros((128, C), F32)
        for g in range(GROUPS):
            w = jnp.concatenate([wqkv[:, C * n + 128 * g : C * n + 128 * g + 128] for n in range(3)], axis=1)
            total = total + dot(dqkv_s[g, at, :], w, NT)
        dm_s[at, :] = total.astype(BF16)

    def image_rows(quad):
        parts = []
        for i in range(4):
            for pair in range(2):
                at = (quad // 2 * 2 + pair) * 128 + quad % 2 * 64 + 16 * i
                parts.append(dm_s[at : at + 16, :])
        return jnp.concatenate(parts, axis=0).reshape(4, 32, C)

    for quad in range(4):
        x = image_rows(quad)
        if quad == 3:
            rows_send2[...] = x
        x = x.astype(F32).reshape(4, 4, 8, C)
        tiles = [jnp.where(sub8, pltpu.roll(x[2 * i, 3], 4, 0), x[2 * i + 1, 3]) for i in range(2)]
        pk_send2[16 * quad : 16 * quad + 16, :] = jnp.concatenate(tiles, 0).astype(BF16)
    halo = [
        remote(rows_send2, rows_recv2, hsem_s.at[3], hsem_r.at[3], (down, wa, ba)),
        remote(pk_send2, pk_recv2, hsem_s.at[4], hsem_r.at[4], (ha, right, ba)),
        remote(pk_send2.at[pl.ds(48, 16)], cr_recv2, hsem_s.at[5], hsem_r.at[5], (down, right, ba)),
    ]
    for copy in halo:
        copy.start()


    for c in range(CHUNKS):
        to_depth(c)


    taken(smx_buf.at[pl.ds(0, 15)], xsem_s.at[3], xsem_r.at[3])
    total = smx_buf[0]
    for d in range(1, 16):
        total = total + smx_buf[d]
    smz_buf[deep] = total
    for h in depth:
        remote(smz_buf.at[deep], smz_buf.at[deep], zsem_s.at[3], zsem_r.at[3], (h, wa, ba)).start()


    for copy in halo:
        copy.wait()
    for quad in range(4):
        if quad == 0:
            rows, pack = rows_recv2[...], cr_recv2[...]
        else:
            rows, pack = image_rows(quad - 1), pk_recv2[16 * quad - 16 : 16 * quad, :]
        x = pltpu.roll(rows.astype(F32).reshape(16, 8, C), 4, 1).reshape(4, 4, 8, C)
        pack = pack.astype(F32).reshape(2, 8, C)
        for i in range(4):
            parts = []
            for j in range(4):
                if j > 0:
                    before = x[i, j - 1]
                else:
                    before = pltpu.roll(pack[i // 2], 4, 0) if i % 2 else pack[i // 2]
                parts.append(jnp.where(sub8, before, x[i, j]))
            back = jnp.concatenate(parts, 0)
            row = 4 * quad + i
            dtok_o[0, row] = (cot[0, row].astype(F32) + back).astype(BF16)


    for c in range(CHUNKS):
        to_level(c)


    taken(smz_buf.at[pl.ds(0, 7)], zsem_s.at[3], zsem_r.at[3])
    total = smz_buf[0]
    for d in range(1, 8):
        total = total + smz_buf[d]
    smf_buf[core] = total
    remote(smf_buf.at[core], smf_buf.at[core], csem_s.at[4], csem_r.at[4], (other, wa, ba)).start()


    for c in range(CHUNKS):
        wait_level(c)


    taken(smf_buf.at[0], csem_s.at[4], csem_r.at[4])
    total_o[0:16, :] = smf_buf[0]
    total_o[16:32, :] = smf_buf[1]


def finish(pieces, total, moved, table, lscale, dtok_o, dwqkv_o, dwproj_o, dtable_o, dscale_o, dgain_o):
    ba = lax.axis_index("ba")
    dtok_o[...] = moved[...]

    def rows(base, count):
        return pl.ds(pl.multiple_of(base, 64), count)

    def join(c, core, first, count):
        return pieces[c, 8 * core + first : 8 * core + first + count].reshape(16 * count, C).astype(F32)

    for c in range(CHUNKS):
        dwqkv_o[rows(128 * c + 192 * ba, 128), :] = join(c, 0, 0, 8)
    dwproj_o[0:128, :] = join(0, 1, 0, 8)
    dwqkv_o[rows(512 - 512 * ba, 64), :] = join(1, 1, 0, 4)
    dwproj_o[128:192, :] = join(1, 1, 4, 4)
    dwqkv_o[rows(384 - 320 * ba, 128), :] = join(2, 1, 0, 8)

    by_lane = jnp.concatenate([total[0:12], total[12:24]], axis=1)
    sigma = jax.nn.sigmoid(table[...])
    dtable_o[...] = fine(by_lane, offset_onehot(), NT) * (BIAS_RANGE * sigma * (1.0 - sigma))
    live = (lscale[...] < SCALE_CAP).astype(F32)
    dscale_o[...] = total[24:25, 0:HEADS] * live
    for g in range(GROUPS):
        dgain_o[pl.ds(128 * g, 128)] = total[25 + g]


def step(tokens, cotangent, w_qkv, w_proj, table_logits, logit_scale, gain):
    vmem = pl.BlockSpec(memory_space=pltpu.VMEM)
    middle = [
        jax.ShapeDtypeStruct((1, ROWS, COLS, C), BF16),
        jax.ShapeDtypeStruct((CHUNKS, 16, 16, C), BF16),
        jax.ShapeDtypeStruct((32, 128), F32),
    ]
    outs = [
        jax.ShapeDtypeStruct((1, ROWS, COLS, C), BF16),
        jax.ShapeDtypeStruct((576, C), F32),
        jax.ShapeDtypeStruct((192, C), F32),
        jax.ShapeDtypeStruct((HEADS, TABLE), F32),
        jax.ShapeDtypeStruct((1, HEADS), F32),
        jax.ShapeDtypeStruct((C,), F32),
    ]
    scratch = [
        pltpu.VMEM((1, ROWS, COLS, C), BF16),
        pltpu.VMEM((1, ROWS, COLS, C), BF16),
        pltpu.VMEM((C, 3 * C), BF16),
        pltpu.VMEM((C, C), BF16),
        pltpu.VMEM((HEADS, TABLE), F32),
        pltpu.VMEM((2, 64, C), BF16),
        pltpu.VMEM((2, 4, COLS, C), BF16),
        pltpu.VMEM((2, 64, C), BF16),
        pltpu.VMEM((2, 16, C), BF16),
        pltpu.VMEM((TOKENS, C), BF16),
        pltpu.VMEM((TOKENS, C), BF16),
        pltpu.VMEM((9, TOKENS, 128), BF16),
        pltpu.VMEM((GROUPS, TOKENS, 128), F32),
        pltpu.VMEM((GROUPS, TOKENS, 128), F32),
        pltpu.VMEM((GROUPS, PAIRS, 8, 128), F32),
        pltpu.VMEM((HEADS, 128, 128), F32),
        pltpu.VMEM((PAIRS, 128, 128), F32),
        pltpu.VMEM((GROUPS, PAIRS, TOKENS, 128), F32),
        pltpu.VMEM((GROUPS, PAIRS, TOKENS, 128), F32),
        pltpu.VMEM((GROUPS, TOKENS, 128), BF16),
        pltpu.VMEM((GROUPS, TOKENS, 128), BF16),
        pltpu.VMEM((TOKENS, C), BF16),
        pltpu.VMEM((GROUPS, TOKENS, C), BF16),
        pltpu.VMEM((HEADS, 128, 128), F32),
        pltpu.VMEM((TOKENS, C), BF16),
        pltpu.VMEM((4, COLS, C), BF16),
        pltpu.VMEM((64, C), BF16),
        pltpu.VMEM((4, COLS, C), BF16),
        pltpu.VMEM((64, C), BF16),
        pltpu.VMEM((16, C), BF16),
        pltpu.VMEM((8, 16, C), BF16),
        pltpu.VMEM((CHUNKS, 2, 2, 8, 16, C), BF16),
        pltpu.VMEM((CHUNKS, 2, 8, 16, C), BF16),
        pltpu.VMEM((CHUNKS, 2, 8, 16, C), BF16),
        pltpu.VMEM((CHUNKS, 15, 16, C), BF16),
        pltpu.VMEM((CHUNKS, 8, 16, C), BF16),
        pltpu.VMEM((32, 128), F32),
        pltpu.VMEM((16, 128), F32),
        pltpu.VMEM((16, 16, 128), F32),
        pltpu.VMEM((8, 16, 128), F32),
        pltpu.VMEM((2, 16, 128), F32),
        pltpu.SemaphoreType.DMA((5,)),
        pltpu.SemaphoreType.DMA((6,)),
        pltpu.SemaphoreType.DMA((6,)),
        pltpu.SemaphoreType.DMA((5,)),
        pltpu.SemaphoreType.DMA((5,)),
        pltpu.SemaphoreType.DMA((4,)),
        pltpu.SemaphoreType.DMA((4,)),
        pltpu.SemaphoreType.DMA((4,)),
        pltpu.SemaphoreType.DMA((4,)),
        pltpu.SemaphoreType.DMA((3,)),
        pltpu.SemaphoreType.DMA((3,)),
    ]
    lscale = logit_scale.reshape(1, HEADS)
    moved, pieces, total = pl.pallas_call(
        kernel,
        name="window_backward",
        out_shape=middle,
        in_specs=[pl.BlockSpec(memory_space=pl.ANY)] * 5 + [vmem] * 2,
        out_specs=[vmem] * 3,
        scratch_shapes=scratch,
        compiler_params=pltpu.CompilerParams(collective_id=0, has_side_effects=True),
    )(tokens, cotangent, w_qkv, w_proj, table_logits, lscale, gain)
    d_tokens, d_wqkv, d_wproj, d_table, d_scale, d_gain = pl.pallas_call(
        finish, name="finish", out_shape=outs, in_specs=[vmem] * 5, out_specs=[vmem] * 6
    )(pieces, total, moved, table_logits, lscale)
    return d_tokens, d_wqkv.T, d_wproj.T, d_table, d_scale.reshape(HEADS), d_gain


def solution(mesh):
    image = P("ba", "ha", "wa", None)
    return jax.shard_map(
        step,
        mesh=mesh,
        in_specs=(image, image, P(), P(), P(), P(), P()),
        out_specs=(image, P(None, "ba"), P(None, "ba"), P(), P(), P()),
        check_vma=False,
    )
```

```python
import functools
import math

import jax
import jax.numpy as jnp
from jax import lax
from jax.experimental import pallas as pl
from jax.experimental.pallas import tpu as pltpu
from jax.sharding import PartitionSpec as P

MESH = pl.DeviceIdType.MESH
F32 = jnp.float32
BF16 = jnp.bfloat16
HIGHEST = lax.Precision.HIGHEST

EPS_NORM = 1e-05
MASK_FILL = -100.0
OTHER_WINDOW = -1e30
SCALE_CAP = math.log(100.0)
BIAS_RANGE = 16.0

ROWS, COLS, C = 16, 32, 384
TOKENS = ROWS * COLS
HEADS = 12
GROUPS = 3
PER = 4
PAIRS = 4
TABLE = 225
CHUNKS = 3
BARRIER = 7

NT = (((1,), (1,)), ((), ()))
TN = (((0,), (0,)), ((), ()))
NN = (((1,), (0,)), ((), ()))


def dot(a, b, dims=NN):
    return lax.dot_general(a, b, dims, preferred_element_type=F32)


def fine(a, b, dims=NN):
    return lax.dot_general(a, b, dims, precision=HIGHEST, preferred_element_type=F32)


def iota(shape, dim):
    return lax.broadcasted_iota(jnp.int32, shape, dim)


def split(x):
    high = x.astype(BF16)
    low = (x - high.astype(F32)).astype(BF16)
    return jnp.concatenate([high, low], axis=1)


def offset_onehot():
    entry = iota((TABLE, 256), 0)
    row = lax.shift_right_logical(entry * 4370, 16)
    col = entry - 15 * row
    lane = (row - 7) * 16 + (col - 7)
    lane = jnp.where(lane < 0, lane + 256, lane)
    return (lane == iota((TABLE, 256), 1)).astype(F32)


def remote(src, dst, send, recv, device):
    return pltpu.make_async_remote_copy(
        src_ref=src, dst_ref=dst, send_sem=send, recv_sem=recv, device_id=device, device_id_type=MESH
    )


def kernel(
    tok_h, cot_h, wqkv_h, wproj_h, table_h, lscale_h, gain_h,
    dtok_o, f_s, total_o, factor_o,
    tok, cot, wqkv, wproj, table, lscale, gain,
    pk_send, rows_recv, pk_recv, cr_recv,
    x_s, c_s, qkv_s, qinv_s, kinv_s, qrow_s, bias_s, mask_s, p_s, raw_s, att_s, datt_s, dproj_s, dqkv_s, dbias_s, dm_s,
    rows_send2, pk_send2, rows_recv2, pk_recv2, cr_recv2,
    keep_k, g_s, core_recv, s1_s, xy_recv, z_buf,
    sm_s, smc_recv, smx_buf, smz_buf, smf_buf,
    told, lsem, hsem_s, hsem_r, csem_s, csem_r, xsem_s, xsem_r, zsem_s, zsem_r, fsem_s, fsem_r,
):
    loads = [
        pltpu.make_async_copy(src, dst, lsem.at[n])
        for n, (src, dst) in enumerate(
            (
                (tok_h, tok), (cot_h, cot), (table_h, table), (wqkv_h, wqkv), (wproj_h, wproj),
                (lscale_h, lscale), (gain_h, gain),
            )
        )
    ]
    for load in loads:
        load.start()

    ha, wa, ba = lax.axis_index("ha"), lax.axis_index("wa"), lax.axis_index("ba")
    core = ha % 2
    deep = ha // 2
    other = ha + 1 - 2 * core
    up, down = (ha + 15) % 16, (ha + 1) % 16
    left, right = (wa + 7) % 8, (wa + 1) % 8
    mine = ba * 8 + wa
    row_mine = core * 8 + wa

    plane = []
    for d in range(1, 16):
        at = (mine + d) % 16
        plane.append((at // 8, at % 8))
    depth = [(deep + d) % 8 * 2 + core for d in range(1, 8)]
    level = []
    for d in range(1, 16):
        at = (row_mine + d) % 16
        level.append((deep * 2 + at // 8, at % 8))

    barrier = pltpu.get_barrier_semaphore()
    greeted = [(ha, left, ba), (ha, right, ba), (ha, wa, 1 - ba)]
    greeted += [(up, wa, ba), (down, wa, ba), (up, left, ba), (down, right, ba)]
    for device in greeted:
        pl.semaphore_signal(barrier, inc=1, device_id=device, device_id_type=MESH)

    sub8 = iota((8, C), 0) < 4


    loads[0].wait()
    loads[1].wait()
    for n, ref in enumerate((tok, cot)):
        for quad in range(4):
            x = ref[0, 4 * quad : 4 * quad + 4, 0:16, :].astype(F32).reshape(4, 2, 8, C)[:, 0]
            tiles = [jnp.where(sub8, x[2 * i], pltpu.roll(x[2 * i + 1], 4, 0)) for i in range(2)]
            pk_send[n, 16 * quad : 16 * quad + 16, :] = jnp.concatenate(tiles, 0).astype(BF16)


    loads[2].wait()
    loads[5].wait()
    loads[6].wait()
    onehot = offset_onehot()
    sigma = jax.nn.sigmoid(table[...])
    lanes = fine(sigma * BIAS_RANGE, onehot)
    factor_o[0:HEADS, 0:TABLE] = BIAS_RANGE * sigma * (1.0 - sigma)
    factor_o[HEADS : HEADS + 1, 0:HEADS] = (lscale[...] < SCALE_CAP).astype(F32)
    for h in range(HEADS):
        line = jnp.broadcast_to(lanes[h : h + 1, :], (128, 256))
        bias_s[h] = pltpu.roll(line, 0, 1, stride=1, stride_axis=0)[:, :128]
    key, query = iota((128, 128), 0), iota((128, 128), 1)

    def bit(x, n):
        return lax.shift_right_logical(x, n) & 1

    apart = bit(key, 3) != bit(query, 3)
    low_rows = bit(key, 6) != bit(query, 6)
    low_cols = bit(key, 2) != bit(query, 2)
    second = bit(key, 3) == 1
    for pair in range(PAIRS):
        differ = jnp.zeros((128, 128), jnp.int32)
        if pair // 2 == 1:
            differ = jnp.where(low_rows, (ha == 15).astype(jnp.int32), differ)
        if pair % 2 == 1:
            differ = jnp.maximum(differ, jnp.where(low_cols & second, (wa == 7).astype(jnp.int32), 0))
        value = jnp.where(differ > 0, MASK_FILL, 0.0).astype(F32)
        mask_s[pair] = jnp.where(apart, OTHER_WINDOW, value)


    pl.semaphore_wait(barrier, BARRIER)
    for n, ref in enumerate((tok, cot)):
        for m, (src, dst, device) in enumerate(
            (
                (ref.at[0, pl.ds(0, 4)], rows_recv.at[n], (up, wa, ba)),
                (pk_send.at[n], pk_recv.at[n], (ha, left, ba)),
                (pk_send.at[n, pl.ds(0, 16)], cr_recv.at[n], (up, left, ba)),
            )
        ):
            remote(src, dst, hsem_s.at[3 * n + m], hsem_r.at[3 * n + m], device).start()

    def shifted(n, quad, pair):
        for ref, out in (((tok, x_s), (cot, c_s))[n],):
            if quad < 3:
                rows = ref[0, 4 * quad + 4 : 4 * quad + 8]
            else:
                rows = rows_recv[n]
            x = pltpu.roll(rows.astype(F32).reshape(16, 8, C), 4, 1).reshape(4, 4, 8, C)
            if pair == 1:
                pack = pk_recv[n, 16 * quad + 16 : 16 * quad + 32, :] if quad < 3 else cr_recv[n]
                pack = pack.astype(F32).reshape(2, 8, C)
            parts = []
            for i in range(4):
                for j in (2 * pair, 2 * pair + 1):
                    if j < 3:
                        after = x[i, j + 1]
                    else:
                        after = pack[i // 2] if i % 2 else pltpu.roll(pack[i // 2], 4, 0)
                    parts.append(jnp.where(sub8, x[i, j], after))
            at = (quad // 2 * 2 + pair) * 128 + quad % 2 * 64
            out[at : at + 64, :] = jnp.concatenate(parts, 0).astype(BF16)

    def projected(first, count):
        at = slice(128 * first, 128 * (first + count))
        x = x_s[at, :]
        for part in range(3):
            y = dot(x, wqkv[:, C * part : C * part + C]).astype(BF16)
            for g in range(GROUPS):
                one = y[:, 128 * g : 128 * g + 128]
                qkv_s[3 * part + g, at, :] = one
                if part == 2:
                    continue
                wide = one.astype(F32)
                square = split(wide * wide)
                inverse = lax.rsqrt(dot(square, same) + 1.0)
                if part == 1:
                    kinv_s[g, at, :] = inverse
                    continue
                qinv_s[g, at, :] = inverse
                across_rows = lax.rsqrt(dot(pick, square, NT) + 1.0)
                for n in range(count):
                    qrow_s[g, first + n, 0:PER, :] = across_rows[0:PER, 128 * n : 128 * n + 128] * scale_rows[g]

    head_lanes = [(lax.shift_right_logical(iota((1, 128), 1), 5) == h) for h in range(PER)]
    head_mask = [m.astype(F32).astype(BF16) for m in head_lanes]
    same = (lax.shift_right_logical(iota((256, 128), 0) & 127, 5) == lax.shift_right_logical(iota((256, 128), 1), 5))
    same = same.astype(F32).astype(BF16)
    pick = (lax.shift_right_logical(iota((8, 256), 1) & 127, 5) == iota((8, 256), 0)).astype(F32).astype(BF16)
    scales = jnp.exp(jnp.minimum(lscale[...], SCALE_CAP))
    scale_rows = [
        jnp.concatenate(
            [jnp.broadcast_to(scales[:, PER * g + h : PER * g + h + 1], (1, 128)) for h in range(PER)], axis=0
        )
        for g in range(GROUPS)
    ]

    def stacked(x):
        return jnp.concatenate([x * m for m in head_mask], axis=0)

    def across(x, h):
        return jnp.broadcast_to(x[:, 32 * h : 32 * h + 1], (128, 128))

    def forward(g, pair):
        at = slice(128 * pair, 128 * pair + 128)
        q, k, v = qkv_s[g, at, :], qkv_s[3 + g, at, :], qkv_s[6 + g, at, :]
        kinv = kinv_s[g, at, :]
        raw = dot(stacked(k), q, NT)
        low = []
        for h in range(PER):
            z = raw[128 * h : 128 * h + 128] * across(kinv, h) * qrow_s[g, pair, h : h + 1, :]
            raw_s[g, pair, 128 * h : 128 * h + 128, :] = z
            z = z + bias_s[PER * g + h] + mask_s[pair]
            e = jnp.exp(z - jnp.max(z, axis=0, keepdims=True))
            p = e * (1.0 / jnp.sum(e, axis=0, keepdims=True))
            p_s[g, pair, 128 * h : 128 * h + 128, :] = p
            low.append(p.astype(BF16))
        att_s[g, at, :] = dot(jnp.concatenate(low, axis=0), stacked(v), TN).astype(BF16)

    def tell(n, devices):
        for device in devices:
            pl.semaphore_signal(told.at[n], inc=1, device_id=device, device_id_type=MESH)

    tell(0, [(ha, left, ba), (ha, right, ba), (up, wa, ba), (down, wa, ba)])


    for quad in range(2):
        shifted(0, quad, 0)
    loads[3].wait()
    projected(0, 1)
    for g in range(GROUPS):
        forward(g, 0)


    def taken(ref, send, recv):
        pltpu.make_async_copy(ref, ref, send).wait()
        pltpu.make_async_copy(ref, ref, recv).wait()

    for m, ref in enumerate((rows_recv, pk_recv, cr_recv)):
        taken(ref.at[0], hsem_s.at[m], hsem_r.at[m])
    pl.semaphore_wait(told.at[0], 4)
    tell(1, [(ha, (wa + 2) % 8, ba), (ha, (wa + 6) % 8, ba), ((ha + 2) % 16, wa, ba), ((ha + 14) % 16, wa, ba)])

    for quad in range(4):
        shifted(0, quad, 1)
        if quad > 1:
            shifted(0, quad, 0)

    projected(1, 3)

    for g in range(GROUPS):
        for pair in range(1, PAIRS):
            forward(g, pair)
    loads[4].wait()

    for m, ref in enumerate((rows_recv, pk_recv, cr_recv)):
        taken(ref.at[1], hsem_s.at[3 + m], hsem_r.at[3 + m])
    pl.semaphore_wait(told.at[1], 4)
    tell(2, [(ha, wa, 1 - ba), (other, wa, ba), ((ha + 4) % 16, wa, ba), ((ha + 12) % 16, wa, ba)])
    for quad in range(4):
        for pair in range(2):
            shifted(1, quad, pair)


    dgain = jnp.zeros((1, C), F32)
    for pair in range(PAIRS):
        at = slice(128 * pair, 128 * pair + 128)
        att = jnp.concatenate([att_s[g, at, :] for g in range(GROUPS)], axis=1)
        proj = dot(att, wproj[...])
        centre = proj - jnp.mean(proj, -1, keepdims=True)
        inv_std = lax.rsqrt(jnp.mean(centre * centre, -1, keepdims=True) + EPS_NORM)
        normed = centre * inv_std
        upstream = c_s[at, :].astype(F32)
        dgain = dgain + jnp.sum(upstream * normed, 0, keepdims=True)
        scaled = upstream * gain[...].reshape(1, C)
        dproj = inv_std * (
            scaled - jnp.mean(scaled, -1, keepdims=True) - normed * jnp.mean(scaled * normed, -1, keepdims=True)
        )
        dproj = dproj.astype(BF16)
        dproj_s[at, :] = dproj
        datt = dot(dproj, wproj[...], NT).astype(BF16)
        for g in range(GROUPS):
            datt_s[g, at, :] = datt[:, 128 * g : 128 * g + 128]
    for g in range(GROUPS):
        sm_s[25 + g : 26 + g, :] = dgain[:, 128 * g : 128 * g + 128]
    sm_s[28:32, :] = jnp.zeros((4, 128), F32)


    att = [att_s[g] for g in range(GROUPS)]
    rows = [dot(dproj_s[...], a, TN).astype(BF16).reshape(2, 12, 16, 128) for a in att]
    for g in range(GROUPS):
        for half in range(2):
            g_s[0, 1, half, :, :, 128 * g : 128 * g + 128] = rows[g][half, 0:8]
            g_s[1, 1, half, 4:8, :, 128 * g : 128 * g + 128] = rows[g][half, 8:12]

    def core_copy(c):
        return remote(g_s.at[c, 1 - core], core_recv.at[c], csem_s.at[c], csem_r.at[c], (other, wa, ba))

    def to_plane(c):
        core_copy(c).wait()
        for b in range(2):
            s1_s[c, b] = (g_s[c, core, b].astype(F32) + core_recv[c, b].astype(F32)).astype(BF16)
        for d, (b, w) in enumerate(plane):
            remote(s1_s.at[c, b, w], xy_recv.at[c, d], xsem_s.at[c], xsem_r.at[c], (ha, w, b)).start()

    def to_depth(c):
        taken(xy_recv.at[c], xsem_s.at[c], xsem_r.at[c])
        total = s1_s[c, ba, wa].astype(F32)
        for d in range(15):
            total = total + xy_recv[c, d].astype(F32)
        z_buf[c, deep] = total.astype(BF16)
        for h in depth:
            remote(z_buf.at[c, deep], z_buf.at[c, deep], zsem_s.at[c], zsem_r.at[c], (h, wa, ba)).start()

    def to_level(c):
        taken(z_buf.at[c, pl.ds(0, 7)], zsem_s.at[c], zsem_r.at[c])
        total = z_buf[c, 0].astype(F32)
        for d in range(1, 8):
            total = total + z_buf[c, d].astype(F32)
        f_s[c, row_mine] = total.astype(BF16)
        for h, w in level:
            remote(f_s.at[c, row_mine], f_s.at[c, row_mine], fsem_s.at[c], fsem_r.at[c], (h, w, ba)).start()

    def wait_level(c):
        taken(f_s.at[c, pl.ds(0, 15)], fsem_s.at[c], fsem_r.at[c])


    for g in range(GROUPS):

        dscale = jnp.zeros((PER, 128), F32)
        for pair in range(PAIRS):
            at = slice(128 * pair, 128 * pair + 128)
            q, k, v = qkv_s[g, at, :], qkv_s[3 + g, at, :], qkv_s[6 + g, at, :]
            datt = datt_s[g, at, :]
            qinv, kinv = qinv_s[g, at, :], kinv_s[g, at, :]
            raw = dot(stacked(v), datt, NT)
            low, grads, sums = [], [], []
            for h in range(PER):
                p = p_s[g, pair, 128 * h : 128 * h + 128, :]
                dp = raw[128 * h : 128 * h + 128]
                ds = p * (dp - jnp.sum(dp * p, axis=0, keepdims=True))
                if pair == 0:
                    dbias_s[PER * g + h] = ds
                else:
                    dbias_s[PER * g + h] += ds
                sums.append(jnp.sum(ds * raw_s[g, pair, 128 * h : 128 * h + 128, :], axis=0, keepdims=True))
                grads.append((ds * across(kinv, h) * qrow_s[g, pair, h : h + 1, :]).astype(BF16))
                low.append(p.astype(BF16))
            dv = dot(jnp.concatenate(low, axis=1), stacked(datt))
            a = dot(jnp.concatenate(grads, axis=0), stacked(k), TN)
            b = dot(jnp.concatenate(grads, axis=1), stacked(q))
            qf, kf = q.astype(F32), k.astype(F32)
            uq, uk = qf * qinv, kf * kinv
            dq = a - uq * dot(split(uq * a), same)
            dk = b - uk * dot(split(uk * b), same)
            dqkv_s[g, at, 0:128] = dq.astype(BF16)
            dqkv_s[g, at, 128:256] = dk.astype(BF16)
            dqkv_s[g, at, 256:384] = dv.astype(BF16)
            dscale = dscale + jnp.concatenate(sums, axis=0)
            if g > 0 and pair == 1:
                if g == 1:
                    pl.semaphore_wait(told.at[2], 4)
                to_plane(g - 1)

        here = iota((PER, 128), 0) + PER * g == iota((PER, 128), 1)
        spread = jnp.where(here, jnp.sum(dscale, axis=1, keepdims=True), 0.0)
        spread = jnp.sum(spread, axis=0, keepdims=True)
        scale_row = spread if g == 0 else scale_row + spread
        for part in range(3):
            dw = dot(dqkv_s[g, :, 128 * part : 128 * part + 128], x_s[...], TN).astype(BF16).reshape(8, 16, C)
            if part == 0:
                g_s[g, 0, 0] = dw
            elif part == 2:
                g_s[g, 0, 1] = dw
            elif g == 0:
                keep_k[...] = dw
            elif g == 1:
                g_s[1, 1, 0, 0:4] = dw[0:4]
                g_s[1, 1, 1, 0:4] = dw[4:8]
            else:
                g_s[2, 1, 0] = keep_k[...]
                g_s[2, 1, 1] = dw
        core_copy(g).start()


    sm_s[24:25, :] = scale_row

    lane8, sub256 = iota((8, 128), 1), iota((8, 256), 0)
    for h in range(HEADS):
        ahead = dbias_s[h, 0:8, :]
        behind = jnp.zeros((8, 128), F32)
        for n in range(1, 16):
            turned = pltpu.roll(dbias_s[h, 8 * n : 8 * n + 8, :], 128 - 8 * n, 1)
            inside = lane8 < 128 - 8 * n
            ahead = ahead + jnp.where(inside, turned, 0.0)
            behind = behind + jnp.where(inside, 0.0, turned)
        both = jnp.concatenate([ahead, behind], axis=1)
        for n in range(3):
            both = jnp.where(bit(sub256, n) == 1, pltpu.roll(both, 256 - 2**n, 1), both)
        both = jnp.sum(both, axis=0, keepdims=True)
        sm_s[h : h + 1, :] = both[:, 0:128]
        sm_s[12 + h : 13 + h, :] = both[:, 128:256]
    small_core = remote(
        sm_s.at[pl.ds(pl.multiple_of(16 * (1 - core), 16), 16)], smc_recv, csem_s.at[3], csem_r.at[3], (other, wa, ba)
    )
    small_core.start()


    to_plane(2)


    small_core.wait()
    smx_buf[mine] = sm_s[pl.ds(pl.multiple_of(16 * core, 16), 16), :] + smc_recv[...]
    for b, w in plane:
        remote(smx_buf.at[mine], smx_buf.at[mine], xsem_s.at[3], xsem_r.at[3], (ha, w, b)).start()


    for pair in range(PAIRS):
        at = slice(128 * pair, 128 * pair + 128)
        total = jnp.zeros((128, C), F32)
        for g in range(GROUPS):
            w = jnp.concatenate([wqkv[:, C * n + 128 * g : C * n + 128 * g + 128] for n in range(3)], axis=1)
            total = total + dot(dqkv_s[g, at, :], w, NT)
        dm_s[at, :] = total.astype(BF16)

    def image_rows(quad):
        parts = []
        for i in range(4):
            for pair in range(2):
                at = (quad // 2 * 2 + pair) * 128 + quad % 2 * 64 + 16 * i
                parts.append(dm_s[at : at + 16, :])
        return jnp.concatenate(parts, axis=0).reshape(4, 32, C)

    for quad in range(4):
        x = image_rows(quad)
        if quad == 3:
            rows_send2[...] = x
        x = x.astype(F32).reshape(4, 4, 8, C)
        tiles = [jnp.where(sub8, pltpu.roll(x[2 * i, 3], 4, 0), x[2 * i + 1, 3]) for i in range(2)]
        pk_send2[16 * quad : 16 * quad + 16, :] = jnp.concatenate(tiles, 0).astype(BF16)
    halo = [
        remote(rows_send2, rows_recv2, hsem_s.at[6], hsem_r.at[6], (down, wa, ba)),
        remote(pk_send2, pk_recv2, hsem_s.at[7], hsem_r.at[7], (ha, right, ba)),
        remote(pk_send2.at[pl.ds(48, 16)], cr_recv2, hsem_s.at[8], hsem_r.at[8], (down, right, ba)),
    ]
    for copy in halo:
        copy.start()


    for c in range(CHUNKS):
        to_depth(c)


    taken(smx_buf.at[pl.ds(0, 15)], xsem_s.at[3], xsem_r.at[3])
    total = smx_buf[0]
    for d in range(1, 16):
        total = total + smx_buf[d]
    smz_buf[deep] = total
    for h in depth:
        remote(smz_buf.at[deep], smz_buf.at[deep], zsem_s.at[3], zsem_r.at[3], (h, wa, ba)).start()


    for copy in halo:
        copy.wait()
    for quad in range(4):
        if quad == 0:
            rows, pack = rows_recv2[...], cr_recv2[...]
        else:
            rows, pack = image_rows(quad - 1), pk_recv2[16 * quad - 16 : 16 * quad, :]
        x = pltpu.roll(rows.astype(F32).reshape(16, 8, C), 4, 1).reshape(4, 4, 8, C)
        pack = pack.astype(F32).reshape(2, 8, C)
        for i in range(4):
            parts = []
            for j in range(4):
                if j > 0:
                    before = x[i, j - 1]
                else:
                    before = pltpu.roll(pack[i // 2], 4, 0) if i % 2 else pack[i // 2]
                parts.append(jnp.where(sub8, before, x[i, j]))
            back = jnp.concatenate(parts, 0)
            row = 4 * quad + i
            dtok_o[0, row] = (cot[0, row].astype(F32) + back).astype(BF16)


    for c in range(CHUNKS):
        to_level(c)


    taken(smz_buf.at[pl.ds(0, 7)], zsem_s.at[3], zsem_r.at[3])
    total = smz_buf[0]
    for d in range(1, 8):
        total = total + smz_buf[d]
    smf_buf[core] = total
    remote(smf_buf.at[core], smf_buf.at[core], csem_s.at[4], csem_r.at[4], (other, wa, ba)).start()


    for c in range(CHUNKS):
        wait_level(c)


    taken(smf_buf.at[0], csem_s.at[4], csem_r.at[4])
    total_o[0:16, :] = smf_buf[0]
    total_o[16:32, :] = smf_buf[1]


def finish(pieces, total, moved, factor, dtok_o, dwqkv_o, dwproj_o, dtable_o, dscale_o, dgain_o):
    ba = lax.axis_index("ba")
    dtok_o[...] = moved[...]

    def rows(base, count):
        return pl.ds(pl.multiple_of(base, 64), count)

    def join(c, core, first, count):
        return pieces[c, 8 * core + first : 8 * core + first + count].reshape(16 * count, C).astype(F32)

    for c in range(CHUNKS):
        dwqkv_o[rows(128 * c + 192 * ba, 128), :] = join(c, 0, 0, 8)
    dwproj_o[0:128, :] = join(0, 1, 0, 8)
    dwqkv_o[rows(512 - 512 * ba, 64), :] = join(1, 1, 0, 4)
    dwproj_o[128:192, :] = join(1, 1, 4, 4)
    dwqkv_o[rows(384 - 320 * ba, 128), :] = join(2, 1, 0, 8)

    by_lane = jnp.concatenate([total[0:12], total[12:24]], axis=1)
    dtable_o[...] = fine(by_lane, offset_onehot(), NT) * factor[0:HEADS, 0:TABLE]
    dscale_o[...] = total[24:25, 0:HEADS] * factor[HEADS : HEADS + 1, 0:HEADS]
    for g in range(GROUPS):
        dgain_o[pl.ds(128 * g, 128)] = total[25 + g]


def step(tokens, cotangent, w_qkv, w_proj, table_logits, logit_scale, gain):
    vmem = pl.BlockSpec(memory_space=pltpu.VMEM)
    middle = [
        pltpu.VMEM((1, ROWS, COLS, C), BF16),
        pltpu.VMEM((CHUNKS, 16, 16, C), BF16),
        pltpu.VMEM((32, 128), F32),
        pltpu.VMEM((16, 256), F32),
    ]
    outs = [
        jax.ShapeDtypeStruct((1, ROWS, COLS, C), BF16),
        jax.ShapeDtypeStruct((576, C), F32),
        jax.ShapeDtypeStruct((192, C), F32),
        jax.ShapeDtypeStruct((HEADS, TABLE), F32),
        jax.ShapeDtypeStruct((1, HEADS), F32),
        jax.ShapeDtypeStruct((C,), F32),
    ]
    scratch = [
        pltpu.VMEM((1, ROWS, COLS, C), BF16),
        pltpu.VMEM((1, ROWS, COLS, C), BF16),
        pltpu.VMEM((C, 3 * C), BF16),
        pltpu.VMEM((C, C), BF16),
        pltpu.VMEM((HEADS, TABLE), F32),
        pltpu.VMEM((1, HEADS), F32),
        pltpu.VMEM((C,), F32),
        pltpu.VMEM((2, 64, C), BF16),
        pltpu.VMEM((2, 4, COLS, C), BF16),
        pltpu.VMEM((2, 64, C), BF16),
        pltpu.VMEM((2, 16, C), BF16),
        pltpu.VMEM((TOKENS, C), BF16),
        pltpu.VMEM((TOKENS, C), BF16),
        pltpu.VMEM((9, TOKENS, 128), BF16),
        pltpu.VMEM((GROUPS, TOKENS, 128), F32),
        pltpu.VMEM((GROUPS, TOKENS, 128), F32),
        pltpu.VMEM((GROUPS, PAIRS, 8, 128), F32),
        pltpu.VMEM((HEADS, 128, 128), F32),
        pltpu.VMEM((PAIRS, 128, 128), F32),
        pltpu.VMEM((GROUPS, PAIRS, TOKENS, 128), F32),
        pltpu.VMEM((GROUPS, PAIRS, TOKENS, 128), F32),
        pltpu.VMEM((GROUPS, TOKENS, 128), BF16),
        pltpu.VMEM((GROUPS, TOKENS, 128), BF16),
        pltpu.VMEM((TOKENS, C), BF16),
        pltpu.VMEM((GROUPS, TOKENS, C), BF16),
        pltpu.VMEM((HEADS, 128, 128), F32),
        pltpu.VMEM((TOKENS, C), BF16),
        pltpu.VMEM((4, COLS, C), BF16),
        pltpu.VMEM((64, C), BF16),
        pltpu.VMEM((4, COLS, C), BF16),
        pltpu.VMEM((64, C), BF16),
        pltpu.VMEM((16, C), BF16),
        pltpu.VMEM((8, 16, C), BF16),
        pltpu.VMEM((CHUNKS, 2, 2, 8, 16, C), BF16),
        pltpu.VMEM((CHUNKS, 2, 8, 16, C), BF16),
        pltpu.VMEM((CHUNKS, 2, 8, 16, C), BF16),
        pltpu.VMEM((CHUNKS, 15, 16, C), BF16),
        pltpu.VMEM((CHUNKS, 8, 16, C), BF16),
        pltpu.VMEM((32, 128), F32),
        pltpu.VMEM((16, 128), F32),
        pltpu.VMEM((16, 16, 128), F32),
        pltpu.VMEM((8, 16, 128), F32),
        pltpu.VMEM((2, 16, 128), F32),
        pltpu.SemaphoreType.REGULAR((3,)),
        pltpu.SemaphoreType.DMA((7,)),
        pltpu.SemaphoreType.DMA((9,)),
        pltpu.SemaphoreType.DMA((9,)),
        pltpu.SemaphoreType.DMA((5,)),
        pltpu.SemaphoreType.DMA((5,)),
        pltpu.SemaphoreType.DMA((4,)),
        pltpu.SemaphoreType.DMA((4,)),
        pltpu.SemaphoreType.DMA((4,)),
        pltpu.SemaphoreType.DMA((4,)),
        pltpu.SemaphoreType.DMA((3,)),
        pltpu.SemaphoreType.DMA((3,)),
    ]
    lscale = logit_scale.reshape(1, HEADS)
    moved, pieces, total, factor = pl.pallas_call(
        kernel,
        name="window_backward",
        out_shape=middle,
        in_specs=[pl.BlockSpec(memory_space=pltpu.HBM)] * 7,
        out_specs=[vmem] * 4,
        scratch_shapes=scratch,
        compiler_params=pltpu.CompilerParams(collective_id=0, has_side_effects=True, vmem_limit_bytes=65_980_000),
    )(tokens, cotangent, w_qkv, w_proj, table_logits, lscale, gain)
    d_tokens, d_wqkv, d_wproj, d_table, d_scale, d_gain = pl.pallas_call(
        finish, name="finish", out_shape=outs, in_specs=[vmem] * 4, out_specs=[vmem] * 6, compiler_params=pltpu.CompilerParams(vmem_limit_bytes=16 * 2**20)
    )(pieces, total, moved, factor)
    return d_tokens, d_wqkv.T, d_wproj.T, d_table, d_scale.reshape(HEADS), d_gain


def solution(mesh):
    image = P("ba", "ha", "wa", None)
    return jax.shard_map(
        step,
        mesh=mesh,
        in_specs=(image, image, P(), P(), P(), P(), P()),
        out_specs=(image, P(None, "ba"), P(None, "ba"), P(), P(), P()),
        check_vma=False,
    )
```

```python
import functools
import math

import jax
import jax.numpy as jnp
from jax import lax
from jax.experimental import pallas as pl
from jax.experimental.pallas import tpu as pltpu
from jax.sharding import PartitionSpec as P

MESH = pl.DeviceIdType.MESH
F32 = jnp.float32
BF16 = jnp.bfloat16
HIGHEST = lax.Precision.HIGHEST

EPS_NORM = 1e-05
MASK_FILL = -100.0
SCALE_CAP = math.log(100.0)
BIAS_RANGE = 16.0

ROWS, COLS, C = 16, 32, 384
TOKENS = ROWS * COLS
HEADS = 12
GROUPS = 3
PER = 4
PAIRS = 4
TABLE = 225
CHUNKS = 3
BARRIER = 7

NT = (((1,), (1,)), ((), ()))
TN = (((0,), (0,)), ((), ()))
NN = (((1,), (0,)), ((), ()))


def dot(a, b, dims=NN):
    return lax.dot_general(a, b, dims, preferred_element_type=F32)


def fine(a, b, dims=NN):
    return lax.dot_general(a, b, dims, precision=HIGHEST, preferred_element_type=F32)


def iota(shape, dim):
    return lax.broadcasted_iota(jnp.int32, shape, dim)


def split(x):
    high = x.astype(BF16)
    low = (x - high.astype(F32)).astype(BF16)
    return jnp.concatenate([high, low], axis=1)


def offset_onehot():
    entry = iota((TABLE, 256), 0)
    row = lax.shift_right_logical(entry * 4370, 16)
    col = entry - 15 * row - 7
    lane = ((row - 7) * 8 + col) & 127
    lane = jnp.where(col < 0, lane + 128, lane)
    return (lane == iota((TABLE, 256), 1)).astype(F32)


def remote(src, dst, send, recv, device):
    return pltpu.make_async_remote_copy(
        src_ref=src, dst_ref=dst, send_sem=send, recv_sem=recv, device_id=device, device_id_type=MESH
    )


def kernel(
    tok_h, cot_h, wqkv_h, wproj_h, table_h, lscale_h, gain_h,
    dtok_o, f_s, total_o, factor_o,
    tok, cot, wqkv, wproj, table, lscale, gain,
    pk_send, rows_recv, pk_recv, cr_recv,
    x_s, c_s, qkv_s, qinv_s, kinv_s, qrow_s, bias_s, mask_s, p_s, raw_s, both_s, att_s, datt_s, dproj_s, dqkv_s, dbias_s, dm_s,
    rows_send2, pk_send2, rows_recv2, pk_recv2, cr_recv2,
    keep_k, g_s, core_recv, s1_s, xy_recv, z_buf,
    sm_s, smc_recv, smx_buf, smz_buf, smf_buf,
    told, lsem, hsem_s, hsem_r, csem_s, csem_r, xsem_s, xsem_r, zsem_s, zsem_r, fsem_s, fsem_r,
):
    loads = [
        pltpu.make_async_copy(src, dst, lsem.at[n])
        for n, (src, dst) in enumerate(
            (
                (tok_h, tok), (cot_h, cot), (table_h, table), (wqkv_h, wqkv), (wproj_h, wproj),
                (lscale_h, lscale), (gain_h, gain),
            )
        )
    ]
    for load in loads[0:2]:
        load.start()

    ha, wa, ba = lax.axis_index("ha"), lax.axis_index("wa"), lax.axis_index("ba")
    core = ha % 2
    deep = ha // 2
    other = ha + 1 - 2 * core
    up, down = (ha + 15) % 16, (ha + 1) % 16
    left, right = (wa + 7) % 8, (wa + 1) % 8
    mine = ba * 8 + wa
    row_mine = core * 8 + wa

    plane = []
    for d in range(1, 16):
        at = (mine + d) % 16
        plane.append((at // 8, at % 8))
    depth = [(deep + d) % 8 * 2 + core for d in range(1, 8)]
    level = []
    for d in range(1, 16):
        at = (row_mine + d) % 16
        level.append((deep * 2 + at // 8, at % 8))

    barrier = pltpu.get_barrier_semaphore()
    greeted = [(ha, left, ba), (ha, right, ba), (ha, wa, 1 - ba)]
    greeted += [(up, wa, ba), (down, wa, ba), (up, left, ba), (down, right, ba)]
    for device in greeted:
        pl.semaphore_signal(barrier, inc=1, device_id=device, device_id_type=MESH)

    sub8 = iota((8, C), 0) < 4


    loads[0].wait()
    loads[1].wait()
    for load in loads[2:]:
        load.start()
    for n, ref in enumerate((tok, cot)):
        for quad in range(4):
            x = ref[0, 4 * quad : 4 * quad + 4, 0:16, :].astype(F32).reshape(4, 2, 8, C)[:, 0]
            tiles = [jnp.where(sub8, x[2 * i], pltpu.roll(x[2 * i + 1], 4, 0)) for i in range(2)]
            pk_send[n, 16 * quad : 16 * quad + 16, :] = jnp.concatenate(tiles, 0).astype(BF16)


    pl.semaphore_wait(barrier, BARRIER)
    for n, ref in enumerate((tok, cot)):
        for m, (src, dst, device) in enumerate(
            (
                (ref.at[0, pl.ds(0, 4)], rows_recv.at[n], (up, wa, ba)),
                (pk_send.at[n], pk_recv.at[n], (ha, left, ba)),
                (pk_send.at[n, pl.ds(0, 16)], cr_recv.at[n], (up, left, ba)),
            )
        ):
            remote(src, dst, hsem_s.at[3 * n + m], hsem_r.at[3 * n + m], device).start()

    def shifted(n, quad, pair):
        for ref, out in (((tok, x_s), (cot, c_s))[n],):
            if quad < 3:
                rows = ref[0, 4 * quad + 4 : 4 * quad + 8]
            else:
                rows = rows_recv[n]
            x = pltpu.roll(rows.astype(F32).reshape(16, 8, C), 4, 1).reshape(4, 4, 8, C)
            if pair == 1:
                pack = pk_recv[n, 16 * quad + 16 : 16 * quad + 32, :] if quad < 3 else cr_recv[n]
                pack = pack.astype(F32).reshape(2, 8, C)
            for window in range(2):
                j = 2 * pair + window
                parts = []
                for i in range(4):
                    if j < 3:
                        after = x[i, j + 1]
                    else:
                        after = pack[i // 2] if i % 2 else pltpu.roll(pack[i // 2], 4, 0)
                    parts.append(jnp.where(sub8, x[i, j], after))
                at = (quad // 2 * 2 + pair) * 128 + window * 64 + quad % 2 * 32
                out[at : at + 32, :] = jnp.concatenate(parts, 0).astype(BF16)

    def projected(first, count):
        at = slice(128 * first, 128 * (first + count))
        x = x_s[at, :]
        for part in range(3):
            y = dot(x, wqkv[:, C * part : C * part + C]).astype(BF16)
            for g in range(GROUPS):
                one = y[:, 128 * g : 128 * g + 128]
                qkv_s[3 * part + g, at, :] = one
                if part == 2:
                    continue
                wide = one.astype(F32)
                square = split(wide * wide)
                inverse = lax.rsqrt(dot(square, same) + 1.0)
                if part == 1:
                    kinv_s[g, at, :] = inverse
                    continue
                qinv_s[g, at, :] = inverse
                across_rows = lax.rsqrt(dot(pick, square, NT) + 1.0)
                for n in range(count):
                    qrow_s[g, first + n, 0:PER, :] = across_rows[0:PER, 128 * n : 128 * n + 128] * scale_rows[g]

    head_lanes = [(lax.shift_right_logical(iota((1, 128), 1), 5) == h) for h in range(PER)]
    head_mask = [m.astype(F32).astype(BF16) for m in head_lanes]
    head_mask2 = [jnp.concatenate([m, m], axis=1) for m in head_mask]
    left_lanes = (iota((1, 128), 1) < 64).astype(F32).astype(BF16)
    right_lanes = (iota((1, 128), 1) >= 64).astype(F32).astype(BF16)
    same = (lax.shift_right_logical(iota((256, 128), 0) & 127, 5) == lax.shift_right_logical(iota((256, 128), 1), 5))
    same = same.astype(F32).astype(BF16)
    pick = (lax.shift_right_logical(iota((8, 256), 1) & 127, 5) == iota((8, 256), 0)).astype(F32).astype(BF16)
    for n in (2, 5, 6):
        loads[n].wait()
    scales = jnp.exp(jnp.minimum(lscale[...], SCALE_CAP))
    scale_rows = [
        jnp.concatenate(
            [jnp.broadcast_to(scales[:, PER * g + h : PER * g + h + 1], (1, 128)) for h in range(PER)], axis=0
        )
        for g in range(GROUPS)
    ]

    def stacked(x):
        return jnp.concatenate([x * m for m in head_mask], axis=0)

    def paired(x):
        wide = jnp.concatenate([x[0:64], x[64:128]], axis=1)
        return jnp.concatenate([wide * m for m in head_mask2], axis=0)

    def apart(x):
        none = jnp.zeros((64, 128), BF16)
        return jnp.concatenate(
            [jnp.concatenate([x[0:64], none], axis=1), jnp.concatenate([none, x[64:128]], axis=1)], axis=0
        )

    def own(x):
        return jnp.concatenate([x[0:64, 0:128], x[64:128, 128:256]], axis=0)

    def spread(x):
        return jnp.concatenate([x * left_lanes, x * right_lanes], axis=0)

    def across(x, h):
        return jnp.where(
            query < 64,
            jnp.broadcast_to(x[0:64, 32 * h : 32 * h + 1], (64, 128)),
            jnp.broadcast_to(x[64:128, 32 * h : 32 * h + 1], (64, 128)),
        )

    def forward(items):
        raws = []
        for g, pair in items:
            at = slice(128 * pair, 128 * pair + 128)
            raws.append(dot(paired(qkv_s[3 + g, at, :]), apart(qkv_s[g, at, :]), NT))
        lows = []
        for (g, pair), raw in zip(items, raws):
            kinv = kinv_s[g, 128 * pair : 128 * pair + 128, :]
            low = []
            for h in range(PER):
                rows = slice(64 * h, 64 * h + 64)
                both = across(kinv, h) * qrow_s[g, pair, h : h + 1, :]
                both_s[g, pair, rows, :] = both
                z = raw[rows] * both
                raw_s[g, pair, rows, :] = z
                z = z + bias_s[PER * g + h] + mask_s[pair]
                e = jnp.exp(z - jnp.max(z, axis=0, keepdims=True))
                p = e * (1.0 / jnp.sum(e, axis=0, keepdims=True))
                p_s[g, pair, rows, :] = p
                low.append(p.astype(BF16))
            lows.append(low)
        for (g, pair), low in zip(items, lows):
            at = slice(128 * pair, 128 * pair + 128)
            v = paired(qkv_s[6 + g, at, :])
            att_s[g, at, :] = own(dot(jnp.concatenate(low, axis=0), v, TN)).astype(BF16)

    def tell(n, devices):
        for device in devices:
            pl.semaphore_signal(told.at[n], inc=1, device_id=device, device_id_type=MESH)

    tell(0, [(ha, left, ba), (ha, right, ba), (up, wa, ba), (down, wa, ba)])


    onehot = offset_onehot()
    sigma = jax.nn.sigmoid(table[...])
    lanes = fine(sigma * BIAS_RANGE, onehot)
    factor_o[0:HEADS, 0:TABLE] = BIAS_RANGE * sigma * (1.0 - sigma)
    factor_o[HEADS : HEADS + 1, 0:HEADS] = (lscale[...] < SCALE_CAP).astype(F32)
    key, query = iota((64, 128), 0), iota((64, 128), 1)
    first = query < 64
    ahead = (query & 7) >= (key & 7)

    def bit(x, n):
        return lax.shift_right_logical(x, n) & 1

    for h in range(HEADS):
        turned = [
            pltpu.roll(jnp.broadcast_to(lanes[h : h + 1, at : at + 128], (64, 128)), 0, 1, stride=1, stride_axis=0)
            for at in (0, 128)
        ]
        one = jnp.where(ahead, turned[0], turned[1])
        bias_s[h] = jnp.where(first, one, pltpu.roll(one, 64, 1))
    low_rows = bit(key, 5) != bit(query, 5)
    low_cols = bit(key, 2) != bit(query, 2)
    for pair in range(PAIRS):
        differ = jnp.zeros((64, 128), jnp.int32)
        if pair // 2 == 1:
            differ = jnp.where(low_rows, (ha == 15).astype(jnp.int32), differ)
        if pair % 2 == 1:
            differ = jnp.maximum(differ, jnp.where(low_cols & (query >= 64), (wa == 7).astype(jnp.int32), 0))
        mask_s[pair] = jnp.where(differ > 0, MASK_FILL, 0.0).astype(F32)


    for quad in range(2):
        shifted(0, quad, 0)
    loads[3].wait()
    projected(0, 1)
    forward([(g, 0) for g in range(GROUPS)])


    def taken(ref, send, recv):
        pltpu.make_async_copy(ref, ref, send).wait()
        pltpu.make_async_copy(ref, ref, recv).wait()

    taken(pk_recv.at[0], hsem_s.at[1], hsem_r.at[1])

    for quad in range(2):
        shifted(0, quad, 1)
    projected(1, 1)
    forward([(g, 1) for g in range(GROUPS)])

    taken(rows_recv.at[0], hsem_s.at[0], hsem_r.at[0])
    taken(cr_recv.at[0], hsem_s.at[2], hsem_r.at[2])
    pl.semaphore_wait(told.at[0], 4)
    tell(1, [(ha, (wa + 2) % 8, ba), (ha, (wa + 6) % 8, ba), ((ha + 2) % 16, wa, ba), ((ha + 14) % 16, wa, ba)])

    for quad in range(2, 4):
        for pair in range(2):
            shifted(0, quad, pair)
    projected(2, 2)

    forward([(g, pair) for g in range(GROUPS) for pair in range(2, PAIRS)])
    loads[4].wait()

    for m, ref in enumerate((rows_recv, pk_recv, cr_recv)):
        taken(ref.at[1], hsem_s.at[3 + m], hsem_r.at[3 + m])
    pl.semaphore_wait(told.at[1], 4)
    tell(2, [(ha, wa, 1 - ba), (other, wa, ba), ((ha + 4) % 16, wa, ba), ((ha + 12) % 16, wa, ba)])
    for quad in range(4):
        for pair in range(2):
            shifted(1, quad, pair)


    def mean(x):
        return jnp.mean(x, -1, keepdims=True)

    spans = [slice(128 * pair, 128 * pair + 128) for pair in range(PAIRS)]
    proj = [dot(jnp.concatenate([att_s[g, at, :] for g in range(GROUPS)], axis=1), wproj[...]) for at in spans]
    upstream = [c_s[at, :].astype(F32) for at in spans]
    scaled = [x * gain[...].reshape(1, C) for x in upstream]
    centre = [x - m for x, m in zip(proj, [mean(x) for x in proj])]
    scaled = [x - m for x, m in zip(scaled, [mean(x) for x in scaled])]
    inv_std = [lax.rsqrt(m + EPS_NORM) for m in [mean(x * x) for x in centre]]
    normed = [x * r for x, r in zip(centre, inv_std)]
    along = [mean(x * (u * gain[...].reshape(1, C))) for x, u in zip(normed, upstream)]
    dproj = [(r * (u - x * m)).astype(BF16) for r, u, x, m in zip(inv_std, scaled, normed, along)]
    dgain = jnp.zeros((1, C), F32)
    for u, x in zip(upstream, normed):
        dgain = dgain + jnp.sum(u * x, 0, keepdims=True)
    for at, d in zip(spans, dproj):
        dproj_s[at, :] = d
        datt = dot(d, wproj[...], NT).astype(BF16)
        for g in range(GROUPS):
            datt_s[g, at, :] = datt[:, 128 * g : 128 * g + 128]
    for g in range(GROUPS):
        sm_s[25 + g : 26 + g, :] = dgain[:, 128 * g : 128 * g + 128]
    sm_s[28:32, :] = jnp.zeros((4, 128), F32)


    att = [att_s[g] for g in range(GROUPS)]
    rows = [dot(dproj_s[...], a, TN).astype(BF16).reshape(2, 12, 16, 128) for a in att]
    for g in range(GROUPS):
        for half in range(2):
            g_s[0, 1, half, :, :, 128 * g : 128 * g + 128] = rows[g][half, 0:8]
            g_s[1, 1, half, 4:8, :, 128 * g : 128 * g + 128] = rows[g][half, 8:12]

    def core_copy(c):
        return remote(g_s.at[c, 1 - core], core_recv.at[c], csem_s.at[c], csem_r.at[c], (other, wa, ba))

    def to_plane(c):
        core_copy(c).wait()
        for b in range(2):
            s1_s[c, b] = (g_s[c, core, b].astype(F32) + core_recv[c, b].astype(F32)).astype(BF16)
        for d, (b, w) in enumerate(plane):
            remote(s1_s.at[c, b, w], xy_recv.at[c, d], xsem_s.at[c], xsem_r.at[c], (ha, w, b)).start()

    def to_depth(c):
        taken(xy_recv.at[c], xsem_s.at[c], xsem_r.at[c])
        total = s1_s[c, ba, wa].astype(F32)
        for d in range(15):
            total = total + xy_recv[c, d].astype(F32)
        z_buf[c, deep] = total.astype(BF16)
        for h in depth:
            remote(z_buf.at[c, deep], z_buf.at[c, deep], zsem_s.at[c], zsem_r.at[c], (h, wa, ba)).start()

    def to_level(c):
        taken(z_buf.at[c, pl.ds(0, 7)], zsem_s.at[c], zsem_r.at[c])
        total = z_buf[c, 0].astype(F32)
        for d in range(1, 8):
            total = total + z_buf[c, d].astype(F32)
        f_s[c, row_mine] = total.astype(BF16)
        for h, w in level:
            remote(f_s.at[c, row_mine], f_s.at[c, row_mine], fsem_s.at[c], fsem_r.at[c], (h, w, ba)).start()

    def wait_level(c):
        taken(f_s.at[c, pl.ds(0, 15)], fsem_s.at[c], fsem_r.at[c])


    for g in range(GROUPS):

        dscale = jnp.zeros((PER, 128), F32)
        spans = [slice(128 * pair, 128 * pair + 128) for pair in range(PAIRS)]
        raws = [dot(paired(qkv_s[6 + g, at, :]), apart(datt_s[g, at, :]), NT) for at in spans]
        lows, grads = [], []
        for pair, raw in enumerate(raws):
            low, grad, sums = [], [], []
            for h in range(PER):
                rows = slice(64 * h, 64 * h + 64)
                p = p_s[g, pair, rows, :]
                dp = raw[rows]
                ds = p * (dp - jnp.sum(dp * p, axis=0, keepdims=True))
                if pair == 0:
                    dbias_s[PER * g + h] = ds
                else:
                    dbias_s[PER * g + h] += ds
                sums.append(jnp.sum(ds * raw_s[g, pair, rows, :], axis=0, keepdims=True))
                grad.append((ds * both_s[g, pair, rows, :]).astype(BF16))
                low.append(p.astype(BF16))
            dscale = dscale + jnp.concatenate(sums, axis=0)
            lows.append(low)
            grads.append(grad)
        if g > 0:
            if g == 1:
                pl.semaphore_wait(told.at[2], 4)
            to_plane(g - 1)
        a = [
            own(dot(jnp.concatenate(grad, axis=0), paired(qkv_s[3 + g, at, :]), TN)) for grad, at in zip(grads, spans)
        ]
        b = [
            dot(jnp.concatenate([spread(x) for x in grad], axis=1), stacked(qkv_s[g, at, :]))
            for grad, at in zip(grads, spans)
        ]
        for low, at in zip(lows, spans):
            dv = dot(jnp.concatenate([spread(x) for x in low], axis=1), stacked(datt_s[g, at, :]))
            dqkv_s[g, at, 256:384] = dv.astype(BF16)
        for part, (grad, inverse) in enumerate(((a, qinv_s), (b, kinv_s))):
            unit = [qkv_s[3 * part + g, at, :].astype(F32) * inverse[g, at, :] for at in spans]
            along = [dot(split(u * x), same) for u, x in zip(unit, grad)]
            for u, x, y, at in zip(unit, grad, along, spans):
                dqkv_s[g, at, 128 * part : 128 * part + 128] = (x - u * y).astype(BF16)
        here = iota((PER, 128), 0) + PER * g == iota((PER, 128), 1)
        placed = jnp.where(here, jnp.sum(dscale, axis=1, keepdims=True), 0.0)
        placed = jnp.sum(placed, axis=0, keepdims=True)
        scale_row = placed if g == 0 else scale_row + placed
        for part in range(3):
            dw = dot(dqkv_s[g, :, 128 * part : 128 * part + 128], x_s[...], TN).astype(BF16).reshape(8, 16, C)
            if part == 0:
                g_s[g, 0, 0] = dw
            elif part == 2:
                g_s[g, 0, 1] = dw
            elif g == 0:
                keep_k[...] = dw
            elif g == 1:
                g_s[1, 1, 0, 0:4] = dw[0:4]
                g_s[1, 1, 1, 0:4] = dw[4:8]
            else:
                g_s[2, 1, 0] = keep_k[...]
                g_s[2, 1, 1] = dw
        core_copy(g).start()


    sm_s[24:25, :] = scale_row

    sub128 = iota((8, 128), 0)
    for h in range(HEADS):
        both = dbias_s[h]
        both = jnp.where(first, both + pltpu.roll(both, 64, 1), 0.0)
        for m, part in enumerate((jnp.where(ahead, both, 0.0), jnp.where(ahead, 0.0, both))):
            total = part[0:8]
            for n in range(1, 8):
                total = total + pltpu.roll(part[8 * n : 8 * n + 8], 128 - 8 * n, 1)
            for n in range(3):
                total = jnp.where(bit(sub128, n) == 1, pltpu.roll(total, 128 - 2**n, 1), total)
            sm_s[12 * m + h : 12 * m + h + 1, :] = jnp.sum(total, axis=0, keepdims=True)
    small_core = remote(
        sm_s.at[pl.ds(pl.multiple_of(16 * (1 - core), 16), 16)], smc_recv, csem_s.at[3], csem_r.at[3], (other, wa, ba)
    )
    small_core.start()


    to_plane(2)


    small_core.wait()
    smx_buf[mine] = sm_s[pl.ds(pl.multiple_of(16 * core, 16), 16), :] + smc_recv[...]
    for b, w in plane:
        remote(smx_buf.at[mine], smx_buf.at[mine], xsem_s.at[3], xsem_r.at[3], (ha, w, b)).start()


    to_depth(0)


    for pair in range(PAIRS):
        at = slice(128 * pair, 128 * pair + 128)
        total = jnp.zeros((128, C), F32)
        for g in range(GROUPS):
            w = jnp.concatenate([wqkv[:, C * n + 128 * g : C * n + 128 * g + 128] for n in range(3)], axis=1)
            total = total + dot(dqkv_s[g, at, :], w, NT)
        dm_s[at, :] = total.astype(BF16).astype(F32)

    def image_rows(quad):
        parts = []
        for i in range(4):
            for pair in range(2):
                for window in range(2):
                    at = (quad // 2 * 2 + pair) * 128 + window * 64 + quad % 2 * 32 + 8 * i
                    parts.append(dm_s[at : at + 8, :])
        return jnp.concatenate(parts, axis=0)

    for quad in range(4):
        x = image_rows(quad)
        if quad == 3:
            rows_send2[...] = x.astype(BF16).reshape(4, COLS, C)
        x = x.reshape(4, 4, 8, C)
        tiles = [jnp.where(sub8, pltpu.roll(x[2 * i, 3], 4, 0), x[2 * i + 1, 3]) for i in range(2)]
        pk_send2[16 * quad : 16 * quad + 16, :] = jnp.concatenate(tiles, 0).astype(BF16)
    halo = [
        remote(rows_send2, rows_recv2, hsem_s.at[6], hsem_r.at[6], (down, wa, ba)),
        remote(pk_send2, pk_recv2, hsem_s.at[7], hsem_r.at[7], (ha, right, ba)),
        remote(pk_send2.at[pl.ds(48, 16)], cr_recv2, hsem_s.at[8], hsem_r.at[8], (down, right, ba)),
    ]
    for copy in halo:
        copy.start()


    to_depth(1)
    to_depth(2)
    to_level(0)
    to_level(1)


    taken(smx_buf.at[pl.ds(0, 15)], xsem_s.at[3], xsem_r.at[3])
    total = smx_buf[0]
    for d in range(1, 16):
        total = total + smx_buf[d]
    smz_buf[deep] = total
    for h in depth:
        remote(smz_buf.at[deep], smz_buf.at[deep], zsem_s.at[3], zsem_r.at[3], (h, wa, ba)).start()


    to_level(2)


    taken(smz_buf.at[pl.ds(0, 7)], zsem_s.at[3], zsem_r.at[3])
    total = smz_buf[0]
    for d in range(1, 8):
        total = total + smz_buf[d]
    smf_buf[core] = total
    remote(smf_buf.at[core], smf_buf.at[core], csem_s.at[4], csem_r.at[4], (other, wa, ba)).start()


    for copy in halo:
        copy.wait()
    for quad in range(4):
        if quad == 0:
            rows, pack = rows_recv2[...].astype(F32), cr_recv2[...]
        else:
            rows, pack = image_rows(quad - 1), pk_recv2[16 * quad - 16 : 16 * quad, :]
        x = pltpu.roll(rows.reshape(16, 8, C), 4, 1).reshape(4, 4, 8, C)
        pack = pack.astype(F32).reshape(2, 8, C)
        for i in range(4):
            parts = []
            for j in range(4):
                if j > 0:
                    before = x[i, j - 1]
                else:
                    before = pltpu.roll(pack[i // 2], 4, 0) if i % 2 else pack[i // 2]
                parts.append(jnp.where(sub8, before, x[i, j]))
            back = jnp.concatenate(parts, 0)
            row = 4 * quad + i
            dtok_o[0, row] = (cot[0, row].astype(F32) + back).astype(BF16)


    for c in range(CHUNKS):
        wait_level(c)


    taken(smf_buf.at[0], csem_s.at[4], csem_r.at[4])
    total_o[0:16, :] = smf_buf[0]
    total_o[16:32, :] = smf_buf[1]


def finish(pieces, total, moved, factor, dtok_o, dwqkv_o, dwproj_o, dtable_o, dscale_o, dgain_o):
    ba = lax.axis_index("ba")
    dtok_o[...] = moved[...]

    def rows(base, count):
        return pl.ds(pl.multiple_of(base, 64), count)

    def join(c, core, first, count):
        return pieces[c, 8 * core + first : 8 * core + first + count].reshape(16 * count, C).astype(F32)

    for c in range(CHUNKS):
        dwqkv_o[rows(128 * c + 192 * ba, 128), :] = join(c, 0, 0, 8)
    dwproj_o[0:128, :] = join(0, 1, 0, 8)
    dwqkv_o[rows(512 - 512 * ba, 64), :] = join(1, 1, 0, 4)
    dwproj_o[128:192, :] = join(1, 1, 4, 4)
    dwqkv_o[rows(384 - 320 * ba, 128), :] = join(2, 1, 0, 8)

    by_lane = jnp.concatenate([total[0:12], total[12:24]], axis=1)
    dtable_o[...] = fine(by_lane, offset_onehot(), NT) * factor[0:HEADS, 0:TABLE]
    dscale_o[...] = total[24:25, 0:HEADS] * factor[HEADS : HEADS + 1, 0:HEADS]
    for g in range(GROUPS):
        dgain_o[pl.ds(128 * g, 128)] = total[25 + g]


def step(tokens, cotangent, w_qkv, w_proj, table_logits, logit_scale, gain):
    vmem = pl.BlockSpec(memory_space=pltpu.VMEM)
    middle = [
        pltpu.VMEM((1, ROWS, COLS, C), BF16),
        pltpu.VMEM((CHUNKS, 16, 16, C), BF16),
        pltpu.VMEM((32, 128), F32),
        pltpu.VMEM((16, 256), F32),
    ]
    outs = [
        jax.ShapeDtypeStruct((1, ROWS, COLS, C), BF16),
        jax.ShapeDtypeStruct((576, C), F32),
        jax.ShapeDtypeStruct((192, C), F32),
        jax.ShapeDtypeStruct((HEADS, TABLE), F32),
        jax.ShapeDtypeStruct((1, HEADS), F32),
        jax.ShapeDtypeStruct((C,), F32),
    ]
    scratch = [
        pltpu.VMEM((1, ROWS, COLS, C), BF16),
        pltpu.VMEM((1, ROWS, COLS, C), BF16),
        pltpu.VMEM((C, 3 * C), BF16),
        pltpu.VMEM((C, C), BF16),
        pltpu.VMEM((HEADS, TABLE), F32),
        pltpu.VMEM((1, HEADS), F32),
        pltpu.VMEM((C,), F32),
        pltpu.VMEM((2, 64, C), BF16),
        pltpu.VMEM((2, 4, COLS, C), BF16),
        pltpu.VMEM((2, 64, C), BF16),
        pltpu.VMEM((2, 16, C), BF16),
        pltpu.VMEM((TOKENS, C), BF16),
        pltpu.VMEM((TOKENS, C), BF16),
        pltpu.VMEM((9, TOKENS, 128), BF16),
        pltpu.VMEM((GROUPS, TOKENS, 128), F32),
        pltpu.VMEM((GROUPS, TOKENS, 128), F32),
        pltpu.VMEM((GROUPS, PAIRS, 8, 128), F32),
        pltpu.VMEM((HEADS, 64, 128), F32),
        pltpu.VMEM((PAIRS, 64, 128), F32),
        pltpu.VMEM((GROUPS, PAIRS, 256, 128), F32),
        pltpu.VMEM((GROUPS, PAIRS, 256, 128), F32),
        pltpu.VMEM((GROUPS, PAIRS, 256, 128), F32),
        pltpu.VMEM((GROUPS, TOKENS, 128), BF16),
        pltpu.VMEM((GROUPS, TOKENS, 128), BF16),
        pltpu.VMEM((TOKENS, C), BF16),
        pltpu.VMEM((GROUPS, TOKENS, C), BF16),
        pltpu.VMEM((HEADS, 64, 128), F32),
        pltpu.VMEM((TOKENS, C), F32),
        pltpu.VMEM((4, COLS, C), BF16),
        pltpu.VMEM((64, C), BF16),
        pltpu.VMEM((4, COLS, C), BF16),
        pltpu.VMEM((64, C), BF16),
        pltpu.VMEM((16, C), BF16),
        pltpu.VMEM((8, 16, C), BF16),
        pltpu.VMEM((CHUNKS, 2, 2, 8, 16, C), BF16),
        pltpu.VMEM((CHUNKS, 2, 8, 16, C), BF16),
        pltpu.VMEM((CHUNKS, 2, 8, 16, C), BF16),
        pltpu.VMEM((CHUNKS, 15, 16, C), BF16),
        pltpu.VMEM((CHUNKS, 8, 16, C), BF16),
        pltpu.VMEM((32, 128), F32),
        pltpu.VMEM((16, 128), F32),
        pltpu.VMEM((16, 16, 128), F32),
        pltpu.VMEM((8, 16, 128), F32),
        pltpu.VMEM((2, 16, 128), F32),
        pltpu.SemaphoreType.REGULAR((3,)),
        pltpu.SemaphoreType.DMA((7,)),
        pltpu.SemaphoreType.DMA((9,)),
        pltpu.SemaphoreType.DMA((9,)),
        pltpu.SemaphoreType.DMA((5,)),
        pltpu.SemaphoreType.DMA((5,)),
        pltpu.SemaphoreType.DMA((4,)),
        pltpu.SemaphoreType.DMA((4,)),
        pltpu.SemaphoreType.DMA((4,)),
        pltpu.SemaphoreType.DMA((4,)),
        pltpu.SemaphoreType.DMA((3,)),
        pltpu.SemaphoreType.DMA((3,)),
    ]
    lscale = logit_scale.reshape(1, HEADS)
    moved, pieces, total, factor = pl.pallas_call(
        kernel,
        name="window_backward",
        out_shape=middle,
        in_specs=[pl.BlockSpec(memory_space=pltpu.HBM)] * 7,
        out_specs=[vmem] * 4,
        scratch_shapes=scratch,
        compiler_params=pltpu.CompilerParams(collective_id=0, has_side_effects=True, vmem_limit_bytes=65_980_000),
    )(tokens, cotangent, w_qkv, w_proj, table_logits, lscale, gain)
    d_tokens, d_wqkv, d_wproj, d_table, d_scale, d_gain = pl.pallas_call(
        finish, name="finish", out_shape=outs, in_specs=[vmem] * 4, out_specs=[vmem] * 6, compiler_params=pltpu.CompilerParams(vmem_limit_bytes=16 * 2**20)
    )(pieces, total, moved, factor)
    return d_tokens, d_wqkv.T, d_wproj.T, d_table, d_scale.reshape(HEADS), d_gain


def solution(mesh):
    image = P("ba", "ha", "wa", None)
    return jax.shard_map(
        step,
        mesh=mesh,
        in_specs=(image, image, P(), P(), P(), P(), P()),
        out_specs=(image, P(None, "ba"), P(None, "ba"), P(), P(), P()),
        check_vma=False,
    )
```

```python
import functools
import math

import jax
import jax.numpy as jnp
from jax import lax
from jax.experimental import pallas as pl
from jax.experimental.pallas import tpu as pltpu
from jax.sharding import PartitionSpec as P

MESH = pl.DeviceIdType.MESH
F32 = jnp.float32
BF16 = jnp.bfloat16
HIGHEST = lax.Precision.HIGHEST

EPS_NORM = 1e-05
MASK_FILL = -100.0
SCALE_CAP = math.log(100.0)
BIAS_RANGE = 16.0

ROWS, COLS, C = 16, 32, 384
TOKENS = ROWS * COLS
HEADS = 12
GROUPS = 3
PER = 4
PAIRS = 4
TABLE = 225
CHUNKS = 3
BARRIER = 7

NT = (((1,), (1,)), ((), ()))
TN = (((0,), (0,)), ((), ()))
NN = (((1,), (0,)), ((), ()))


def dot(a, b, dims=NN):
    return lax.dot_general(a, b, dims, preferred_element_type=F32)


def fine(a, b, dims=NN):
    return lax.dot_general(a, b, dims, precision=HIGHEST, preferred_element_type=F32)


def iota(shape, dim):
    return lax.broadcasted_iota(jnp.int32, shape, dim)


def split(x):
    high = x.astype(BF16)
    low = (x - high.astype(F32)).astype(BF16)
    return jnp.concatenate([high, low], axis=1)


def offset_onehot():
    entry = iota((TABLE, 256), 0)
    row = lax.shift_right_logical(entry * 4370, 16)
    col = entry - 15 * row - 7
    lane = ((row - 7) * 8 + col) & 127
    lane = jnp.where(col < 0, lane + 128, lane)
    return (lane == iota((TABLE, 256), 1)).astype(F32)


def remote(src, dst, send, recv, device):
    return pltpu.make_async_remote_copy(
        src_ref=src, dst_ref=dst, send_sem=send, recv_sem=recv, device_id=device, device_id_type=MESH
    )


def kernel(
    tok_h, cot_h, wqkv_h, wproj_h, table_h, lscale_h, gain_h,
    dtok_o, f_s, total_o, factor_o,
    tok, cot, wqkv, wproj, table, lscale, gain,
    pk_send, rows_recv, pk_recv, cr_recv,
    x_s, c_s, qkv_s, qinv_s, kinv_s, qrow_s, bias_s, mask_s, p_s, raw_s, both_s, att_s, datt_s, dproj_s, dqkv_s, dbias_s, dm_s,
    rows_send2, pk_send2, rows_recv2, pk_recv2, cr_recv2,
    keep_k, g_s, core_recv, s1_s, xy_recv, z_buf,
    sm_s, smc_recv, smy_buf, smx_buf, smz_buf, smf_buf,
    told, lsem, hsem_s, hsem_r, csem_s, csem_r, xsem_s, xsem_r, zsem_s, zsem_r, fsem_s, fsem_r,
):
    loads = [
        pltpu.make_async_copy(src, dst, lsem.at[n])
        for n, (src, dst) in enumerate(
            (
                (tok_h, tok), (cot_h, cot), (table_h, table), (wqkv_h, wqkv), (wproj_h, wproj),
                (lscale_h, lscale), (gain_h, gain),
            )
        )
    ]
    for load in loads[0:2]:
        load.start()

    ha, wa, ba = lax.axis_index("ha"), lax.axis_index("wa"), lax.axis_index("ba")
    core = ha % 2
    deep = ha // 2
    other = ha + 1 - 2 * core
    up, down = (ha + 15) % 16, (ha + 1) % 16
    left, right = (wa + 7) % 8, (wa + 1) % 8
    mine = ba * 8 + wa
    row_mine = core * 8 + wa

    high, low_x = wa // 2, wa % 2

    def seat(a, b, c):
        return (ba + a) % 2, (high + b) % 4 * 2 + (low_x + c) % 2

    hops = {(a, b, c): (0, 1, 2, 1)[b] + (0, 1, 2, 1)[2 * a + c] for a in range(2) for b in range(4) for c in range(2)}
    away = sorted((o for o in hops if hops[o]), key=lambda o: (-hops[o], o))
    plane = [seat(*o) for o in away]
    depth = [(deep + d) % 8 * 2 + core for d in (4, 3, 5, 2, 6, 1, 7)]
    rows_away = [seat(*o)[1] for o in away if o[0] == 0]
    level = [[(ha, w) for w in rows_away], [(other, w) for w in rows_away] + [(ha, w) for w in rows_away] + [(other, wa)]]

    barrier = pltpu.get_barrier_semaphore()
    greeted = [(ha, left, ba), (ha, right, ba), (ha, wa, 1 - ba)]
    greeted += [(up, wa, ba), (down, wa, ba), (up, left, ba), (down, right, ba)]
    for device in greeted:
        pl.semaphore_signal(barrier, inc=1, device_id=device, device_id_type=MESH)

    sub8 = iota((8, C), 0) < 4


    loads[0].wait()
    loads[1].wait()
    for load in loads[2:]:
        load.start()
    for n, ref in enumerate((tok, cot)):
        for quad in range(4):
            x = ref[0, 4 * quad : 4 * quad + 4, 0:16, :].astype(F32).reshape(4, 2, 8, C)[:, 0]
            tiles = [jnp.where(sub8, x[2 * i], pltpu.roll(x[2 * i + 1], 4, 0)) for i in range(2)]
            pk_send[n, 16 * quad : 16 * quad + 16, :] = jnp.concatenate(tiles, 0).astype(BF16)


    pl.semaphore_wait(barrier, BARRIER)
    for n, ref in enumerate((tok, cot)):
        for m, (src, dst, device) in enumerate(
            (
                (ref.at[0, pl.ds(0, 4)], rows_recv.at[n], (up, wa, ba)),
                (pk_send.at[n], pk_recv.at[n], (ha, left, ba)),
                (pk_send.at[n, pl.ds(0, 16)], cr_recv.at[n], (up, left, ba)),
            )
        ):
            remote(src, dst, hsem_s.at[3 * n + m], hsem_r.at[3 * n + m], device).start()

    def shifted(n, quad, pair):
        for ref, out in (((tok, x_s), (cot, c_s))[n],):
            if quad < 3:
                rows = ref[0, 4 * quad + 4 : 4 * quad + 8]
            else:
                rows = rows_recv[n]
            x = pltpu.roll(rows.astype(F32).reshape(16, 8, C), 4, 1).reshape(4, 4, 8, C)
            if pair == 1:
                pack = pk_recv[n, 16 * quad + 16 : 16 * quad + 32, :] if quad < 3 else cr_recv[n]
                pack = pack.astype(F32).reshape(2, 8, C)
            for window in range(2):
                j = 2 * pair + window
                parts = []
                for i in range(4):
                    if j < 3:
                        after = x[i, j + 1]
                    else:
                        after = pack[i // 2] if i % 2 else pltpu.roll(pack[i // 2], 4, 0)
                    parts.append(jnp.where(sub8, x[i, j], after))
                at = (quad // 2 * 2 + pair) * 128 + window * 64 + quad % 2 * 32
                out[at : at + 32, :] = jnp.concatenate(parts, 0).astype(BF16)

    def projected(first, count):
        at = slice(128 * first, 128 * (first + count))
        x = x_s[at, :]
        for part in range(3):
            y = dot(x, wqkv[:, C * part : C * part + C]).astype(BF16)
            for g in range(GROUPS):
                one = y[:, 128 * g : 128 * g + 128]
                qkv_s[3 * part + g, at, :] = one
                if part == 2:
                    continue
                wide = one.astype(F32)
                square = split(wide * wide)
                inverse = lax.rsqrt(dot(square, same) + 1.0)
                if part == 1:
                    kinv_s[g, at, :] = inverse
                    continue
                qinv_s[g, at, :] = inverse
                across_rows = lax.rsqrt(dot(pick, square, NT) + 1.0)
                for n in range(count):
                    qrow_s[g, first + n, 0:PER, :] = across_rows[0:PER, 128 * n : 128 * n + 128] * scale_rows[g]

    head_lanes = [(lax.shift_right_logical(iota((1, 128), 1), 5) == h) for h in range(PER)]
    head_mask = [m.astype(F32).astype(BF16) for m in head_lanes]
    head_mask2 = [jnp.concatenate([m, m], axis=1) for m in head_mask]
    left_lanes = (iota((1, 128), 1) < 64).astype(F32).astype(BF16)
    right_lanes = (iota((1, 128), 1) >= 64).astype(F32).astype(BF16)
    same = (lax.shift_right_logical(iota((256, 128), 0) & 127, 5) == lax.shift_right_logical(iota((256, 128), 1), 5))
    same = same.astype(F32).astype(BF16)
    pick = (lax.shift_right_logical(iota((8, 256), 1) & 127, 5) == iota((8, 256), 0)).astype(F32).astype(BF16)
    for n in (2, 5, 6):
        loads[n].wait()
    scales = jnp.exp(jnp.minimum(lscale[...], SCALE_CAP))
    scale_rows = [
        jnp.concatenate(
            [jnp.broadcast_to(scales[:, PER * g + h : PER * g + h + 1], (1, 128)) for h in range(PER)], axis=0
        )
        for g in range(GROUPS)
    ]

    def stacked(x):
        return jnp.concatenate([x * m for m in head_mask], axis=0)

    def paired(x):
        wide = jnp.concatenate([x[0:64], x[64:128]], axis=1)
        return jnp.concatenate([wide * m for m in head_mask2], axis=0)

    def apart(x):
        none = jnp.zeros((64, 128), BF16)
        return jnp.concatenate(
            [jnp.concatenate([x[0:64], none], axis=1), jnp.concatenate([none, x[64:128]], axis=1)], axis=0
        )

    def own(x):
        return jnp.concatenate([x[0:64, 0:128], x[64:128, 128:256]], axis=0)

    def spread(x):
        return jnp.concatenate([x * left_lanes, x * right_lanes], axis=0)

    def across(x, h):
        return jnp.where(
            query < 64,
            jnp.broadcast_to(x[0:64, 32 * h : 32 * h + 1], (64, 128)),
            jnp.broadcast_to(x[64:128, 32 * h : 32 * h + 1], (64, 128)),
        )

    def forward(items):
        raws = []
        for g, pair in items:
            at = slice(128 * pair, 128 * pair + 128)
            raws.append(dot(paired(qkv_s[3 + g, at, :]), apart(qkv_s[g, at, :]), NT))
        lows = []
        for (g, pair), raw in zip(items, raws):
            kinv = kinv_s[g, 128 * pair : 128 * pair + 128, :]
            low = []
            for h in range(PER):
                rows = slice(64 * h, 64 * h + 64)
                both = across(kinv, h) * qrow_s[g, pair, h : h + 1, :]
                both_s[g, pair, rows, :] = both
                z = raw[rows] * both
                raw_s[g, pair, rows, :] = z
                z = z + bias_s[PER * g + h] + mask_s[pair]
                e = jnp.exp(z - jnp.max(z, axis=0, keepdims=True))
                p = e * (1.0 / jnp.sum(e, axis=0, keepdims=True))
                p_s[g, pair, rows, :] = p
                low.append(p.astype(BF16))
            lows.append(low)
        for (g, pair), low in zip(items, lows):
            at = slice(128 * pair, 128 * pair + 128)
            v = paired(qkv_s[6 + g, at, :])
            att_s[g, at, :] = own(dot(jnp.concatenate(low, axis=0), v, TN)).astype(BF16)

    def tell(n, devices):
        for device in devices:
            pl.semaphore_signal(told.at[n], inc=1, device_id=device, device_id_type=MESH)

    tell(0, [(ha, left, ba), (ha, right, ba), (up, wa, ba), (down, wa, ba)])


    onehot = offset_onehot()
    sigma = jax.nn.sigmoid(table[...])
    lanes = fine(sigma * BIAS_RANGE, onehot)
    factor_o[0:HEADS, 0:TABLE] = BIAS_RANGE * sigma * (1.0 - sigma)
    factor_o[HEADS : HEADS + 1, 0:HEADS] = (lscale[...] < SCALE_CAP).astype(F32)
    key, query = iota((64, 128), 0), iota((64, 128), 1)
    first = query < 64
    ahead = (query & 7) >= (key & 7)

    def bit(x, n):
        return lax.shift_right_logical(x, n) & 1

    for h in range(HEADS):
        turned = [
            pltpu.roll(jnp.broadcast_to(lanes[h : h + 1, at : at + 128], (64, 128)), 0, 1, stride=1, stride_axis=0)
            for at in (0, 128)
        ]
        one = jnp.where(ahead, turned[0], turned[1])
        bias_s[h] = jnp.where(first, one, pltpu.roll(one, 64, 1))
    low_rows = bit(key, 5) != bit(query, 5)
    low_cols = bit(key, 2) != bit(query, 2)
    for pair in range(PAIRS):
        differ = jnp.zeros((64, 128), jnp.int32)
        if pair // 2 == 1:
            differ = jnp.where(low_rows, (ha == 15).astype(jnp.int32), differ)
        if pair % 2 == 1:
            differ = jnp.maximum(differ, jnp.where(low_cols & (query >= 64), (wa == 7).astype(jnp.int32), 0))
        mask_s[pair] = jnp.where(differ > 0, MASK_FILL, 0.0).astype(F32)


    for quad in range(2):
        shifted(0, quad, 0)
    loads[3].wait()
    projected(0, 1)
    forward([(g, 0) for g in range(GROUPS)])


    def taken(ref, send, recv):
        pltpu.make_async_copy(ref, ref, send).wait()
        pltpu.make_async_copy(ref, ref, recv).wait()

    taken(pk_recv.at[0], hsem_s.at[1], hsem_r.at[1])

    for quad in range(2):
        shifted(0, quad, 1)
    projected(1, 1)
    forward([(g, 1) for g in range(GROUPS)])

    taken(rows_recv.at[0], hsem_s.at[0], hsem_r.at[0])
    taken(cr_recv.at[0], hsem_s.at[2], hsem_r.at[2])
    pl.semaphore_wait(told.at[0], 4)
    tell(1, [(ha, (wa + 2) % 8, ba), (ha, (wa + 6) % 8, ba), ((ha + 2) % 16, wa, ba), ((ha + 14) % 16, wa, ba)])

    for quad in range(2, 4):
        for pair in range(2):
            shifted(0, quad, pair)
    projected(2, 2)

    forward([(g, pair) for g in range(GROUPS) for pair in range(2, PAIRS)])
    loads[4].wait()

    for m, ref in enumerate((rows_recv, pk_recv, cr_recv)):
        taken(ref.at[1], hsem_s.at[3 + m], hsem_r.at[3 + m])
    pl.semaphore_wait(told.at[1], 4)
    tell(2, [(ha, wa, 1 - ba), (other, wa, ba), ((ha + 4) % 16, wa, ba), ((ha + 12) % 16, wa, ba)])
    for quad in range(4):
        for pair in range(2):
            shifted(1, quad, pair)


    def mean(x):
        return jnp.mean(x, -1, keepdims=True)

    spans = [slice(128 * pair, 128 * pair + 128) for pair in range(PAIRS)]
    proj = [dot(jnp.concatenate([att_s[g, at, :] for g in range(GROUPS)], axis=1), wproj[...]) for at in spans]
    upstream = [c_s[at, :].astype(F32) for at in spans]
    scaled = [x * gain[...].reshape(1, C) for x in upstream]
    centre = [x - m for x, m in zip(proj, [mean(x) for x in proj])]
    scaled = [x - m for x, m in zip(scaled, [mean(x) for x in scaled])]
    inv_std = [lax.rsqrt(m + EPS_NORM) for m in [mean(x * x) for x in centre]]
    normed = [x * r for x, r in zip(centre, inv_std)]
    along = [mean(x * (u * gain[...].reshape(1, C))) for x, u in zip(normed, upstream)]
    dproj = [(r * (u - x * m)).astype(BF16) for r, u, x, m in zip(inv_std, scaled, normed, along)]
    dgain = jnp.zeros((1, C), F32)
    for u, x in zip(upstream, normed):
        dgain = dgain + jnp.sum(u * x, 0, keepdims=True)
    for at, d in zip(spans, dproj):
        dproj_s[at, :] = d
        datt = dot(d, wproj[...], NT).astype(BF16)
        for g in range(GROUPS):
            datt_s[g, at, :] = datt[:, 128 * g : 128 * g + 128]
    for g in range(GROUPS):
        sm_s[25 + g : 26 + g, :] = dgain[:, 128 * g : 128 * g + 128]
    sm_s[28:32, :] = jnp.zeros((4, 128), F32)


    att = [att_s[g] for g in range(GROUPS)]
    rows = [dot(dproj_s[...], a, TN).astype(BF16).reshape(2, 12, 16, 128) for a in att]
    for g in range(GROUPS):
        for half in range(2):
            g_s[0, 1, half, :, :, 128 * g : 128 * g + 128] = rows[g][half, 0:8]
            g_s[1, 1, half, 4:8, :, 128 * g : 128 * g + 128] = rows[g][half, 8:12]

    def core_copy(c):
        return remote(g_s.at[c, 1 - core], core_recv.at[c], csem_s.at[c], csem_r.at[c], (other, wa, ba))

    def to_plane(c):
        core_copy(c).wait()
        for b in range(2):
            s1_s[c, b] = (g_s[c, core, b].astype(F32) + core_recv[c, b].astype(F32)).astype(BF16)
        for d, (b, w) in enumerate(plane):
            remote(s1_s.at[c, b, w], xy_recv.at[c, d], xsem_s.at[c], xsem_r.at[c], (ha, w, b)).start()

    def to_depth(c):
        taken(xy_recv.at[c], xsem_s.at[c], xsem_r.at[c])
        total = s1_s[c, ba, wa].astype(F32)
        for d in range(15):
            total = total + xy_recv[c, d].astype(F32)
        z_buf[c, deep] = total.astype(BF16)
        for h in depth:
            remote(z_buf.at[c, deep], z_buf.at[c, deep], zsem_s.at[c], zsem_r.at[c], (h, wa, ba)).start()

    def to_level(c):
        taken(z_buf.at[c, pl.ds(0, 7)], zsem_s.at[c], zsem_r.at[c])
        total = z_buf[c, 0].astype(F32)
        for d in range(1, 8):
            total = total + z_buf[c, d].astype(F32)
        f_s[c, row_mine] = total.astype(BF16)
        for h, w in level[c // 2]:
            remote(f_s.at[c, row_mine], f_s.at[c, row_mine], fsem_s.at[c], fsem_r.at[c], (h, w, ba)).start()

    def to_core(c):
        taken(f_s.at[c, pl.ds(0, 7)], fsem_s.at[c], fsem_r.at[c])
        half = f_s.at[c, pl.ds(pl.multiple_of(8 * core, 8), 8)]
        remote(half, half, csem_s.at[5 + c], csem_r.at[5 + c], (other, wa, ba)).start()

    def wait_level(c):
        if c < 2:
            taken(f_s.at[c, pl.ds(0, 8)], csem_s.at[5 + c], csem_r.at[5 + c])
        else:
            taken(f_s.at[c, pl.ds(0, 15)], fsem_s.at[c], fsem_r.at[c])


    for g in range(GROUPS):

        dscale = jnp.zeros((PER, 128), F32)
        spans = [slice(128 * pair, 128 * pair + 128) for pair in range(PAIRS)]
        raws = [dot(paired(qkv_s[6 + g, at, :]), apart(datt_s[g, at, :]), NT) for at in spans]
        lows, grads = [], []
        for pair, raw in enumerate(raws):
            low, grad, sums = [], [], []
            for h in range(PER):
                rows = slice(64 * h, 64 * h + 64)
                p = p_s[g, pair, rows, :]
                dp = raw[rows]
                ds = p * (dp - jnp.sum(dp * p, axis=0, keepdims=True))
                if pair == 0:
                    dbias_s[PER * g + h] = ds
                else:
                    dbias_s[PER * g + h] += ds
                sums.append(jnp.sum(ds * raw_s[g, pair, rows, :], axis=0, keepdims=True))
                grad.append((ds * both_s[g, pair, rows, :]).astype(BF16))
                low.append(p.astype(BF16))
            dscale = dscale + jnp.concatenate(sums, axis=0)
            lows.append(low)
            grads.append(grad)
        if g > 0:
            if g == 1:
                pl.semaphore_wait(told.at[2], 4)
            to_plane(g - 1)
        a = [
            own(dot(jnp.concatenate(grad, axis=0), paired(qkv_s[3 + g, at, :]), TN)) for grad, at in zip(grads, spans)
        ]
        b = [
            dot(jnp.concatenate([spread(x) for x in grad], axis=1), stacked(qkv_s[g, at, :]))
            for grad, at in zip(grads, spans)
        ]
        for low, at in zip(lows, spans):
            dv = dot(jnp.concatenate([spread(x) for x in low], axis=1), stacked(datt_s[g, at, :]))
            dqkv_s[g, at, 256:384] = dv.astype(BF16)
        for part, (grad, inverse) in enumerate(((a, qinv_s), (b, kinv_s))):
            unit = [qkv_s[3 * part + g, at, :].astype(F32) * inverse[g, at, :] for at in spans]
            along = [dot(split(u * x), same) for u, x in zip(unit, grad)]
            for u, x, y, at in zip(unit, grad, along, spans):
                dqkv_s[g, at, 128 * part : 128 * part + 128] = (x - u * y).astype(BF16)
        here = iota((PER, 128), 0) + PER * g == iota((PER, 128), 1)
        placed = jnp.where(here, jnp.sum(dscale, axis=1, keepdims=True), 0.0)
        placed = jnp.sum(placed, axis=0, keepdims=True)
        scale_row = placed if g == 0 else scale_row + placed
        for part in range(3):
            dw = dot(dqkv_s[g, :, 128 * part : 128 * part + 128], x_s[...], TN).astype(BF16).reshape(8, 16, C)
            if part == 0:
                g_s[g, 0, 0] = dw
            elif part == 2:
                g_s[g, 0, 1] = dw
            elif g == 0:
                keep_k[...] = dw
            elif g == 1:
                g_s[1, 1, 0, 0:4] = dw[0:4]
                g_s[1, 1, 1, 0:4] = dw[4:8]
            else:
                g_s[2, 1, 0] = keep_k[...]
                g_s[2, 1, 1] = dw
        core_copy(g).start()


    sm_s[24:25, :] = scale_row

    sub128 = iota((8, 128), 0)
    for h in range(HEADS):
        both = dbias_s[h]
        both = jnp.where(first, both + pltpu.roll(both, 64, 1), 0.0)
        for m, part in enumerate((jnp.where(ahead, both, 0.0), jnp.where(ahead, 0.0, both))):
            total = part[0:8]
            for n in range(1, 8):
                total = total + pltpu.roll(part[8 * n : 8 * n + 8], 128 - 8 * n, 1)
            for n in range(3):
                total = jnp.where(bit(sub128, n) == 1, pltpu.roll(total, 128 - 2**n, 1), total)
            sm_s[12 * m + h : 12 * m + h + 1, :] = jnp.sum(total, axis=0, keepdims=True)
    small_core = remote(
        sm_s.at[pl.ds(pl.multiple_of(16 * (1 - core), 16), 16)], smc_recv, csem_s.at[3], csem_r.at[3], (other, wa, ba)
    )
    small_core.start()


    to_plane(2)


    small_core.wait()
    smy_buf[high] = sm_s[pl.ds(pl.multiple_of(16 * core, 16), 16), :] + smc_recv[...]
    for b in (2, 1, 3):
        remote(smy_buf.at[high], smy_buf.at[high], xsem_s.at[3], xsem_r.at[3], (ha, seat(0, b, 0)[1], ba)).start()


    to_depth(0)


    for pair in range(PAIRS):
        at = slice(128 * pair, 128 * pair + 128)
        total = jnp.zeros((128, C), F32)
        for g in range(GROUPS):
            w = jnp.concatenate([wqkv[:, C * n + 128 * g : C * n + 128 * g + 128] for n in range(3)], axis=1)
            total = total + dot(dqkv_s[g, at, :], w, NT)
        dm_s[at, :] = total.astype(BF16).astype(F32)

    def image_rows(quad):
        parts = []
        for i in range(4):
            for pair in range(2):
                for window in range(2):
                    at = (quad // 2 * 2 + pair) * 128 + window * 64 + quad % 2 * 32 + 8 * i
                    parts.append(dm_s[at : at + 8, :])
        return jnp.concatenate(parts, axis=0)

    for quad in range(4):
        x = image_rows(quad)
        if quad == 3:
            rows_send2[...] = x.astype(BF16).reshape(4, COLS, C)
        x = x.reshape(4, 4, 8, C)
        tiles = [jnp.where(sub8, pltpu.roll(x[2 * i, 3], 4, 0), x[2 * i + 1, 3]) for i in range(2)]
        pk_send2[16 * quad : 16 * quad + 16, :] = jnp.concatenate(tiles, 0).astype(BF16)
    halo = [
        remote(rows_send2, rows_recv2, hsem_s.at[6], hsem_r.at[6], (down, wa, ba)),
        remote(pk_send2, pk_recv2, hsem_s.at[7], hsem_r.at[7], (ha, right, ba)),
        remote(pk_send2.at[pl.ds(48, 16)], cr_recv2, hsem_s.at[8], hsem_r.at[8], (down, right, ba)),
    ]
    for copy in halo:
        copy.start()


    to_depth(1)

    column = 2 * ba + low_x
    taken(smy_buf.at[pl.ds(0, 3)], xsem_s.at[3], xsem_r.at[3])
    smx_buf[column] = smy_buf[0] + smy_buf[1] + smy_buf[2] + smy_buf[3]
    for a, c in ((1, 0), (0, 1), (1, 1)):
        b, w = seat(a, 0, c)
        remote(smx_buf.at[column], smx_buf.at[column], xsem_s.at[4], xsem_r.at[4], (ha, w, b)).start()

    to_level(0)

    to_depth(2)

    to_level(1)


    taken(smx_buf.at[pl.ds(0, 3)], xsem_s.at[4], xsem_r.at[4])
    smz_buf[deep] = smx_buf[0] + smx_buf[1] + smx_buf[2] + smx_buf[3]
    for h in depth:
        remote(smz_buf.at[deep], smz_buf.at[deep], zsem_s.at[3], zsem_r.at[3], (h, wa, ba)).start()

    to_core(0)


    to_level(2)

    to_core(1)


    taken(smz_buf.at[pl.ds(0, 7)], zsem_s.at[3], zsem_r.at[3])
    total = smz_buf[0]
    for d in range(1, 8):
        total = total + smz_buf[d]
    smf_buf[core] = total
    remote(smf_buf.at[core], smf_buf.at[core], csem_s.at[4], csem_r.at[4], (other, wa, ba)).start()


    for copy in halo:
        copy.wait()
    for quad in range(4):
        if quad == 0:
            rows, pack = rows_recv2[...].astype(F32), cr_recv2[...]
        else:
            rows, pack = image_rows(quad - 1), pk_recv2[16 * quad - 16 : 16 * quad, :]
        x = pltpu.roll(rows.reshape(16, 8, C), 4, 1).reshape(4, 4, 8, C)
        pack = pack.astype(F32).reshape(2, 8, C)
        for i in range(4):
            parts = []
            for j in range(4):
                if j > 0:
                    before = x[i, j - 1]
                else:
                    before = pltpu.roll(pack[i // 2], 4, 0) if i % 2 else pack[i // 2]
                parts.append(jnp.where(sub8, before, x[i, j]))
            back = jnp.concatenate(parts, 0)
            row = 4 * quad + i
            dtok_o[0, row] = (cot[0, row].astype(F32) + back).astype(BF16)


    for c in range(CHUNKS):
        wait_level(c)


    taken(smf_buf.at[0], csem_s.at[4], csem_r.at[4])
    total_o[0:16, :] = smf_buf[0]
    total_o[16:32, :] = smf_buf[1]


def finish(pieces, total, moved, factor, dtok_o, dwqkv_o, dwproj_o, dtable_o, dscale_o, dgain_o):
    ba = lax.axis_index("ba")
    dtok_o[...] = moved[...]

    def rows(base, count):
        return pl.ds(pl.multiple_of(base, 64), count)

    def join(c, core, first, count):
        return pieces[c, 8 * core + first : 8 * core + first + count].reshape(16 * count, C).astype(F32)

    for c in range(CHUNKS):
        dwqkv_o[rows(128 * c + 192 * ba, 128), :] = join(c, 0, 0, 8)
    dwproj_o[0:128, :] = join(0, 1, 0, 8)
    dwqkv_o[rows(512 - 512 * ba, 64), :] = join(1, 1, 0, 4)
    dwproj_o[128:192, :] = join(1, 1, 4, 4)
    dwqkv_o[rows(384 - 320 * ba, 128), :] = join(2, 1, 0, 8)

    by_lane = jnp.concatenate([total[0:12], total[12:24]], axis=1)
    dtable_o[...] = fine(by_lane, offset_onehot(), NT) * factor[0:HEADS, 0:TABLE]
    dscale_o[...] = total[24:25, 0:HEADS] * factor[HEADS : HEADS + 1, 0:HEADS]
    for g in range(GROUPS):
        dgain_o[pl.ds(128 * g, 128)] = total[25 + g]


def step(tokens, cotangent, w_qkv, w_proj, table_logits, logit_scale, gain):
    vmem = pl.BlockSpec(memory_space=pltpu.VMEM)
    middle = [
        pltpu.VMEM((1, ROWS, COLS, C), BF16),
        pltpu.VMEM((CHUNKS, 16, 16, C), BF16),
        pltpu.VMEM((32, 128), F32),
        pltpu.VMEM((16, 256), F32),
    ]
    outs = [
        jax.ShapeDtypeStruct((1, ROWS, COLS, C), BF16),
        jax.ShapeDtypeStruct((576, C), F32),
        jax.ShapeDtypeStruct((192, C), F32),
        jax.ShapeDtypeStruct((HEADS, TABLE), F32),
        jax.ShapeDtypeStruct((1, HEADS), F32),
        jax.ShapeDtypeStruct((C,), F32),
    ]
    scratch = [
        pltpu.VMEM((1, ROWS, COLS, C), BF16),
        pltpu.VMEM((1, ROWS, COLS, C), BF16),
        pltpu.VMEM((C, 3 * C), BF16),
        pltpu.VMEM((C, C), BF16),
        pltpu.VMEM((HEADS, TABLE), F32),
        pltpu.VMEM((1, HEADS), F32),
        pltpu.VMEM((C,), F32),
        pltpu.VMEM((2, 64, C), BF16),
        pltpu.VMEM((2, 4, COLS, C), BF16),
        pltpu.VMEM((2, 64, C), BF16),
        pltpu.VMEM((2, 16, C), BF16),
        pltpu.VMEM((TOKENS, C), BF16),
        pltpu.VMEM((TOKENS, C), BF16),
        pltpu.VMEM((9, TOKENS, 128), BF16),
        pltpu.VMEM((GROUPS, TOKENS, 128), F32),
        pltpu.VMEM((GROUPS, TOKENS, 128), F32),
        pltpu.VMEM((GROUPS, PAIRS, 8, 128), F32),
        pltpu.VMEM((HEADS, 64, 128), F32),
        pltpu.VMEM((PAIRS, 64, 128), F32),
        pltpu.VMEM((GROUPS, PAIRS, 256, 128), F32),
        pltpu.VMEM((GROUPS, PAIRS, 256, 128), F32),
        pltpu.VMEM((GROUPS, PAIRS, 256, 128), F32),
        pltpu.VMEM((GROUPS, TOKENS, 128), BF16),
        pltpu.VMEM((GROUPS, TOKENS, 128), BF16),
        pltpu.VMEM((TOKENS, C), BF16),
        pltpu.VMEM((GROUPS, TOKENS, C), BF16),
        pltpu.VMEM((HEADS, 64, 128), F32),
        pltpu.VMEM((TOKENS, C), F32),
        pltpu.VMEM((4, COLS, C), BF16),
        pltpu.VMEM((64, C), BF16),
        pltpu.VMEM((4, COLS, C), BF16),
        pltpu.VMEM((64, C), BF16),
        pltpu.VMEM((16, C), BF16),
        pltpu.VMEM((8, 16, C), BF16),
        pltpu.VMEM((CHUNKS, 2, 2, 8, 16, C), BF16),
        pltpu.VMEM((CHUNKS, 2, 8, 16, C), BF16),
        pltpu.VMEM((CHUNKS, 2, 8, 16, C), BF16),
        pltpu.VMEM((CHUNKS, 15, 16, C), BF16),
        pltpu.VMEM((CHUNKS, 8, 16, C), BF16),
        pltpu.VMEM((32, 128), F32),
        pltpu.VMEM((16, 128), F32),
        pltpu.VMEM((4, 16, 128), F32),
        pltpu.VMEM((4, 16, 128), F32),
        pltpu.VMEM((8, 16, 128), F32),
        pltpu.VMEM((2, 16, 128), F32),
        pltpu.SemaphoreType.REGULAR((3,)),
        pltpu.SemaphoreType.DMA((7,)),
        pltpu.SemaphoreType.DMA((9,)),
        pltpu.SemaphoreType.DMA((9,)),
        pltpu.SemaphoreType.DMA((7,)),
        pltpu.SemaphoreType.DMA((7,)),
        pltpu.SemaphoreType.DMA((5,)),
        pltpu.SemaphoreType.DMA((5,)),
        pltpu.SemaphoreType.DMA((4,)),
        pltpu.SemaphoreType.DMA((4,)),
        pltpu.SemaphoreType.DMA((3,)),
        pltpu.SemaphoreType.DMA((3,)),
    ]
    lscale = logit_scale.reshape(1, HEADS)
    moved, pieces, total, factor = pl.pallas_call(
        kernel,
        name="window_backward",
        out_shape=middle,
        in_specs=[pl.BlockSpec(memory_space=pltpu.HBM)] * 7,
        out_specs=[vmem] * 4,
        scratch_shapes=scratch,
        compiler_params=pltpu.CompilerParams(collective_id=0, has_side_effects=True, vmem_limit_bytes=65_980_000),
    )(tokens, cotangent, w_qkv, w_proj, table_logits, lscale, gain)
    d_tokens, d_wqkv, d_wproj, d_table, d_scale, d_gain = pl.pallas_call(
        finish, name="finish", out_shape=outs, in_specs=[vmem] * 4, out_specs=[vmem] * 6, compiler_params=pltpu.CompilerParams(vmem_limit_bytes=16 * 2**20)
    )(pieces, total, moved, factor)
    return d_tokens, d_wqkv.T, d_wproj.T, d_table, d_scale.reshape(HEADS), d_gain


def solution(mesh):
    image = P("ba", "ha", "wa", None)
    return jax.shard_map(
        step,
        mesh=mesh,
        in_specs=(image, image, P(), P(), P(), P(), P()),
        out_specs=(image, P(None, "ba"), P(None, "ba"), P(), P(), P()),
        check_vma=False,
    )
```

```python
import functools
import math

import jax
import jax.numpy as jnp
from jax import lax
from jax.experimental import pallas as pl
from jax.experimental.pallas import tpu as pltpu
from jax.sharding import PartitionSpec as P

MESH = pl.DeviceIdType.MESH
F32 = jnp.float32
BF16 = jnp.bfloat16
HIGHEST = lax.Precision.HIGHEST

EPS_NORM = 1e-05
MASK_FILL = -100.0
SCALE_CAP = math.log(100.0)
BIAS_RANGE = 16.0

ROWS, COLS, C = 16, 32, 384
TOKENS = ROWS * COLS
HEADS = 12
GROUPS = 3
PER = 4
PAIRS = 4
TABLE = 225
CHUNKS = 3
BARRIER = 7

NT = (((1,), (1,)), ((), ()))
TN = (((0,), (0,)), ((), ()))
NN = (((1,), (0,)), ((), ()))


def dot(a, b, dims=NN):
    return lax.dot_general(a, b, dims, preferred_element_type=F32)


def fine(a, b, dims=NN):
    return lax.dot_general(a, b, dims, precision=HIGHEST, preferred_element_type=F32)


def iota(shape, dim):
    return lax.broadcasted_iota(jnp.int32, shape, dim)


def split(x):
    high = x.astype(BF16)
    low = (x - high.astype(F32)).astype(BF16)
    return jnp.concatenate([high, low], axis=1)


def offset_onehot():
    entry = iota((TABLE, 256), 0)
    row = lax.shift_right_logical(entry * 4370, 16)
    col = entry - 15 * row - 7
    lane = ((row - 7) * 8 + col) & 127
    lane = jnp.where(col < 0, lane + 128, lane)
    return (lane == iota((TABLE, 256), 1)).astype(F32)


def remote(src, dst, send, recv, device):
    return pltpu.make_async_remote_copy(
        src_ref=src, dst_ref=dst, send_sem=send, recv_sem=recv, device_id=device, device_id_type=MESH
    )


def kernel(
    tok_h, cot_h, wqkv_h, wproj_h, table_h, lscale_h, gain_h,
    dtok_o, f_s, total_o, factor_o,
    tok, cot, wqkv, wproj, table, lscale, gain,
    pk_send, rows_recv, pk_recv, cr_recv,
    x_s, c_s, qkv_s, qinv_s, kinv_s, qrow_s, bias_s, mask_s, p_s, raw_s, both_s, att_s, datt_s, dproj_s, dqkv_s, dbias_s, dm_s,
    rows_send2, pk_send2, rows_recv2, pk_recv2, cr_recv2,
    keep_k, g_s, core_recv, s1_s, xy_recv, z_buf,
    sm_s, smc_recv, smy_buf, smx_buf, smz_buf, smf_buf,
    told, lsem, hsem_s, hsem_r, csem_s, csem_r, xsem_s, xsem_r, zsem_s, zsem_r, fsem_s, fsem_r,
):
    loads = [
        pltpu.make_async_copy(src, dst, lsem.at[n])
        for n, (src, dst) in enumerate(
            (
                (tok_h, tok), (cot_h, cot), (table_h, table), (wqkv_h, wqkv), (wproj_h, wproj),
                (lscale_h, lscale), (gain_h, gain),
            )
        )
    ]
    for load in loads[0:2]:
        load.start()

    ha, wa, ba = lax.axis_index("ha"), lax.axis_index("wa"), lax.axis_index("ba")
    core = ha % 2
    deep = ha // 2
    other = ha + 1 - 2 * core
    up, down = (ha + 15) % 16, (ha + 1) % 16
    left, right = (wa + 7) % 8, (wa + 1) % 8
    mine = ba * 8 + wa
    row_mine = core * 8 + wa

    high, low_x = wa // 2, wa % 2

    def seat(a, b, c):
        return (ba + a) % 2, (high + b) % 4 * 2 + (low_x + c) % 2

    hops = {(a, b, c): (0, 1, 2, 1)[b] + (0, 1, 2, 1)[2 * a + c] for a in range(2) for b in range(4) for c in range(2)}
    away = sorted((o for o in hops if hops[o]), key=lambda o: (-hops[o], o))
    plane = [seat(*o) for o in away]
    depth = [(deep + d) % 8 * 2 + core for d in (4, 3, 5, 2, 6, 1, 7)]
    rows_away = [seat(*o)[1] for o in away if o[0] == 0]
    level = [[(ha, w) for w in rows_away], [(other, w) for w in rows_away] + [(ha, w) for w in rows_away] + [(other, wa)]]

    barrier = pltpu.get_barrier_semaphore()
    greeted = [(ha, left, ba), (ha, right, ba), (ha, wa, 1 - ba)]
    greeted += [(up, wa, ba), (down, wa, ba), (up, left, ba), (down, right, ba)]
    for device in greeted:
        pl.semaphore_signal(barrier, inc=1, device_id=device, device_id_type=MESH)

    sub8 = iota((8, C), 0) < 4


    loads[0].wait()
    loads[1].wait()
    for load in loads[2:]:
        load.start()
    for n, ref in enumerate((tok, cot)):
        for quad in range(4):
            x = ref[0, 4 * quad : 4 * quad + 4, 0:16, :].astype(F32).reshape(4, 2, 8, C)[:, 0]
            tiles = [jnp.where(sub8, x[2 * i], pltpu.roll(x[2 * i + 1], 4, 0)) for i in range(2)]
            pk_send[n, 16 * quad : 16 * quad + 16, :] = jnp.concatenate(tiles, 0).astype(BF16)


    pl.semaphore_wait(barrier, BARRIER)
    for n, ref in enumerate((tok, cot)):
        for m, (src, dst, device) in enumerate(
            (
                (ref.at[0, pl.ds(0, 4)], rows_recv.at[n], (up, wa, ba)),
                (pk_send.at[n], pk_recv.at[n], (ha, left, ba)),
                (pk_send.at[n, pl.ds(0, 16)], cr_recv.at[n], (up, left, ba)),
            )
        ):
            remote(src, dst, hsem_s.at[3 * n + m], hsem_r.at[3 * n + m], device).start()

    def shifted(n, quad, pair):
        for ref, out in (((tok, x_s), (cot, c_s))[n],):
            if quad < 3:
                rows = ref[0, 4 * quad + 4 : 4 * quad + 8]
            else:
                rows = rows_recv[n]
            x = pltpu.roll(rows.astype(F32).reshape(16, 8, C), 4, 1).reshape(4, 4, 8, C)
            if pair == 1:
                pack = pk_recv[n, 16 * quad + 16 : 16 * quad + 32, :] if quad < 3 else cr_recv[n]
                pack = pack.astype(F32).reshape(2, 8, C)
            for window in range(2):
                j = 2 * pair + window
                parts = []
                for i in range(4):
                    if j < 3:
                        after = x[i, j + 1]
                    else:
                        after = pack[i // 2] if i % 2 else pltpu.roll(pack[i // 2], 4, 0)
                    parts.append(jnp.where(sub8, x[i, j], after))
                at = (quad // 2 * 2 + pair) * 128 + window * 64 + quad % 2 * 32
                out[at : at + 32, :] = jnp.concatenate(parts, 0).astype(BF16)

    def projected(first, count):
        at = slice(128 * first, 128 * (first + count))
        x = x_s[at, :]
        for part in range(3):
            y = dot(x, wqkv[:, C * part : C * part + C]).astype(BF16)
            for g in range(GROUPS):
                one = y[:, 128 * g : 128 * g + 128]
                qkv_s[3 * part + g, at, :] = one
                if part == 2:
                    continue
                wide = one.astype(F32)
                square = split(wide * wide)
                inverse = lax.rsqrt(dot(square, same) + 1.0)
                if part == 1:
                    kinv_s[g, at, :] = inverse
                    continue
                qinv_s[g, at, :] = inverse
                across_rows = lax.rsqrt(dot(pick, square, NT) + 1.0)
                for n in range(count):
                    qrow_s[g, first + n, 0:PER, :] = across_rows[0:PER, 128 * n : 128 * n + 128] * scale_rows[g]

    head_lanes = [(lax.shift_right_logical(iota((1, 128), 1), 5) == h) for h in range(PER)]
    head_mask = [m.astype(F32).astype(BF16) for m in head_lanes]
    head_mask2 = [jnp.concatenate([m, m], axis=1) for m in head_mask]
    left_lanes = (iota((1, 128), 1) < 64).astype(F32).astype(BF16)
    right_lanes = (iota((1, 128), 1) >= 64).astype(F32).astype(BF16)
    same = (lax.shift_right_logical(iota((256, 128), 0) & 127, 5) == lax.shift_right_logical(iota((256, 128), 1), 5))
    same = same.astype(F32).astype(BF16)
    pick = (lax.shift_right_logical(iota((8, 256), 1) & 127, 5) == iota((8, 256), 0)).astype(F32).astype(BF16)
    for n in (2, 5, 6):
        loads[n].wait()
    scales = jnp.exp(jnp.minimum(lscale[...], SCALE_CAP))
    scale_rows = [
        jnp.concatenate(
            [jnp.broadcast_to(scales[:, PER * g + h : PER * g + h + 1], (1, 128)) for h in range(PER)], axis=0
        )
        for g in range(GROUPS)
    ]

    def stacked(x):
        return jnp.concatenate([x * m for m in head_mask], axis=0)

    def paired(x):
        wide = jnp.concatenate([x[0:64], x[64:128]], axis=1)
        return jnp.concatenate([wide * m for m in head_mask2], axis=0)

    def apart(x):
        none = jnp.zeros((64, 128), BF16)
        return jnp.concatenate(
            [jnp.concatenate([x[0:64], none], axis=1), jnp.concatenate([none, x[64:128]], axis=1)], axis=0
        )

    def own(x):
        return jnp.concatenate([x[0:64, 0:128], x[64:128, 128:256]], axis=0)

    def spread(x):
        return jnp.concatenate([x * left_lanes, x * right_lanes], axis=0)

    def across(x, h):
        return jnp.where(
            query < 64,
            jnp.broadcast_to(x[0:64, 32 * h : 32 * h + 1], (64, 128)),
            jnp.broadcast_to(x[64:128, 32 * h : 32 * h + 1], (64, 128)),
        )

    def forward(items):
        raws = []
        for g, pair in items:
            at = slice(128 * pair, 128 * pair + 128)
            raws.append(dot(paired(qkv_s[3 + g, at, :]), apart(qkv_s[g, at, :]), NT))
        lows = []
        for (g, pair), raw in zip(items, raws):
            kinv = kinv_s[g, 128 * pair : 128 * pair + 128, :]
            low = []
            for h in range(PER):
                rows = slice(64 * h, 64 * h + 64)
                both = across(kinv, h) * qrow_s[g, pair, h : h + 1, :]
                both_s[g, pair, rows, :] = both
                z = raw[rows] * both
                raw_s[g, pair, rows, :] = z
                z = z + bias_s[PER * g + h] + mask_s[pair]
                e = jnp.exp(z - jnp.max(z, axis=0, keepdims=True))
                p = e * (1.0 / jnp.sum(e, axis=0, keepdims=True))
                p_s[g, pair, rows, :] = p
                low.append(p.astype(BF16))
            lows.append(low)
        for (g, pair), low in zip(items, lows):
            at = slice(128 * pair, 128 * pair + 128)
            v = paired(qkv_s[6 + g, at, :])
            att_s[g, at, :] = own(dot(jnp.concatenate(low, axis=0), v, TN)).astype(BF16)

    def tell(n, devices):
        for device in devices:
            pl.semaphore_signal(told.at[n], inc=1, device_id=device, device_id_type=MESH)

    tell(0, [(ha, left, ba), (ha, right, ba), (up, wa, ba), (down, wa, ba)])


    onehot = offset_onehot()
    sigma = jax.nn.sigmoid(table[...])
    lanes = fine(sigma * BIAS_RANGE, onehot)
    factor_o[0:HEADS, 0:TABLE] = BIAS_RANGE * sigma * (1.0 - sigma)
    factor_o[HEADS : HEADS + 1, 0:HEADS] = (lscale[...] < SCALE_CAP).astype(F32)
    key, query = iota((64, 128), 0), iota((64, 128), 1)
    first = query < 64
    ahead = (query & 7) >= (key & 7)

    def bit(x, n):
        return lax.shift_right_logical(x, n) & 1

    for h in range(HEADS):
        turned = [
            pltpu.roll(jnp.broadcast_to(lanes[h : h + 1, at : at + 128], (64, 128)), 0, 1, stride=1, stride_axis=0)
            for at in (0, 128)
        ]
        one = jnp.where(ahead, turned[0], turned[1])
        bias_s[h] = jnp.where(first, one, pltpu.roll(one, 64, 1))
    low_rows = bit(key, 5) != bit(query, 5)
    low_cols = bit(key, 2) != bit(query, 2)
    for pair in range(PAIRS):
        differ = jnp.zeros((64, 128), jnp.int32)
        if pair // 2 == 1:
            differ = jnp.where(low_rows, (ha == 15).astype(jnp.int32), differ)
        if pair % 2 == 1:
            differ = jnp.maximum(differ, jnp.where(low_cols & (query >= 64), (wa == 7).astype(jnp.int32), 0))
        mask_s[pair] = jnp.where(differ > 0, MASK_FILL, 0.0).astype(F32)


    for quad in range(2):
        shifted(0, quad, 0)
    loads[3].wait()
    projected(0, 1)
    forward([(g, 0) for g in range(GROUPS)])


    def taken(ref, send, recv):
        pltpu.make_async_copy(ref, ref, send).wait()
        pltpu.make_async_copy(ref, ref, recv).wait()

    taken(pk_recv.at[0], hsem_s.at[1], hsem_r.at[1])

    for quad in range(2):
        shifted(0, quad, 1)
    projected(1, 1)
    forward([(g, 1) for g in range(GROUPS)])

    taken(rows_recv.at[0], hsem_s.at[0], hsem_r.at[0])
    taken(cr_recv.at[0], hsem_s.at[2], hsem_r.at[2])
    pl.semaphore_wait(told.at[0], 4)
    tell(1, [(ha, (wa + 2) % 8, ba), (ha, (wa + 6) % 8, ba), ((ha + 2) % 16, wa, ba), ((ha + 14) % 16, wa, ba)])

    for quad in range(2, 4):
        for pair in range(2):
            shifted(0, quad, pair)
    projected(2, 2)

    forward([(g, pair) for g in range(GROUPS) for pair in range(2, PAIRS)])
    loads[4].wait()

    for m, ref in enumerate((rows_recv, pk_recv, cr_recv)):
        taken(ref.at[1], hsem_s.at[3 + m], hsem_r.at[3 + m])
    pl.semaphore_wait(told.at[1], 4)
    tell(2, [(ha, wa, 1 - ba), (other, wa, ba), ((ha + 4) % 16, wa, ba), ((ha + 12) % 16, wa, ba)])
    for quad in range(4):
        for pair in range(2):
            shifted(1, quad, pair)


    def mean(x):
        return jnp.mean(x, -1, keepdims=True)

    spans = [slice(128 * pair, 128 * pair + 128) for pair in range(PAIRS)]
    proj = [dot(jnp.concatenate([att_s[g, at, :] for g in range(GROUPS)], axis=1), wproj[...]) for at in spans]
    upstream = [c_s[at, :].astype(F32) for at in spans]
    scaled = [x * gain[...].reshape(1, C) for x in upstream]
    centre = [x - m for x, m in zip(proj, [mean(x) for x in proj])]
    scaled = [x - m for x, m in zip(scaled, [mean(x) for x in scaled])]
    inv_std = [lax.rsqrt(m + EPS_NORM) for m in [mean(x * x) for x in centre]]
    normed = [x * r for x, r in zip(centre, inv_std)]
    along = [mean(x * (u * gain[...].reshape(1, C))) for x, u in zip(normed, upstream)]
    dproj = [(r * (u - x * m)).astype(BF16) for r, u, x, m in zip(inv_std, scaled, normed, along)]
    dgain = jnp.zeros((1, C), F32)
    for u, x in zip(upstream, normed):
        dgain = dgain + jnp.sum(u * x, 0, keepdims=True)
    for at, d in zip(spans, dproj):
        dproj_s[at, :] = d
        datt = dot(d, wproj[...], NT).astype(BF16)
        for g in range(GROUPS):
            datt_s[g, at, :] = datt[:, 128 * g : 128 * g + 128]
    for g in range(GROUPS):
        sm_s[25 + g : 26 + g, :] = dgain[:, 128 * g : 128 * g + 128]
    sm_s[28:32, :] = jnp.zeros((4, 128), F32)


    att = [att_s[g] for g in range(GROUPS)]
    rows = [dot(dproj_s[...], a, TN).astype(BF16).reshape(2, 12, 16, 128) for a in att]
    for g in range(GROUPS):
        for half in range(2):
            g_s[0, 1, half, :, :, 128 * g : 128 * g + 128] = rows[g][half, 0:8]
            g_s[1, 1, half, 4:8, :, 128 * g : 128 * g + 128] = rows[g][half, 8:12]

    def core_copy(c):
        return remote(g_s.at[c, 1 - core], core_recv.at[c], csem_s.at[c], csem_r.at[c], (other, wa, ba))

    def to_plane(c):
        core_copy(c).wait()
        for b in range(2):
            s1_s[c, b] = (g_s[c, core, b].astype(F32) + core_recv[c, b].astype(F32)).astype(BF16)
        for d, (b, w) in enumerate(plane):
            remote(s1_s.at[c, b, w], xy_recv.at[c, d], xsem_s.at[c], xsem_r.at[c], (ha, w, b)).start()

    def to_depth(c):
        taken(xy_recv.at[c], xsem_s.at[c], xsem_r.at[c])
        total = s1_s[c, ba, wa].astype(F32)
        for d in range(15):
            total = total + xy_recv[c, d].astype(F32)
        z_buf[c, deep] = total.astype(BF16)
        for h in depth:
            remote(z_buf.at[c, deep], z_buf.at[c, deep], zsem_s.at[c], zsem_r.at[c], (h, wa, ba)).start()

    def to_level(c):
        taken(z_buf.at[c, pl.ds(0, 7)], zsem_s.at[c], zsem_r.at[c])
        total = z_buf[c, 0].astype(F32)
        for d in range(1, 8):
            total = total + z_buf[c, d].astype(F32)
        f_s[c, row_mine] = total.astype(BF16)
        for h, w in level[c // 2]:
            remote(f_s.at[c, row_mine], f_s.at[c, row_mine], fsem_s.at[c], fsem_r.at[c], (h, w, ba)).start()

    def to_core(c):
        taken(f_s.at[c, pl.ds(0, 7)], fsem_s.at[c], fsem_r.at[c])
        half = f_s.at[c, pl.ds(pl.multiple_of(8 * core, 8), 8)]
        remote(half, half, csem_s.at[5 + c], csem_r.at[5 + c], (other, wa, ba)).start()

    def wait_level(c):
        if c < 2:
            taken(f_s.at[c, pl.ds(0, 8)], csem_s.at[5 + c], csem_r.at[5 + c])
        else:
            taken(f_s.at[c, pl.ds(0, 15)], fsem_s.at[c], fsem_r.at[c])


    for g in range(GROUPS):

        dscale = jnp.zeros((PER, 128), F32)
        spans = [slice(128 * pair, 128 * pair + 128) for pair in range(PAIRS)]
        raws = [dot(paired(qkv_s[6 + g, at, :]), apart(datt_s[g, at, :]), NT) for at in spans]
        lows, grads = [], []
        for pair, raw in enumerate(raws):
            low, grad, sums = [], [], []
            for h in range(PER):
                rows = slice(64 * h, 64 * h + 64)
                p = p_s[g, pair, rows, :]
                dp = raw[rows]
                ds = p * (dp - jnp.sum(dp * p, axis=0, keepdims=True))
                if pair == 0:
                    dbias_s[PER * g + h] = ds
                else:
                    dbias_s[PER * g + h] += ds
                sums.append(jnp.sum(ds * raw_s[g, pair, rows, :], axis=0, keepdims=True))
                grad.append((ds * both_s[g, pair, rows, :]).astype(BF16))
                low.append(p.astype(BF16))
            dscale = dscale + jnp.concatenate(sums, axis=0)
            lows.append(low)
            grads.append(grad)
        if g > 0:
            if g == 1:
                pl.semaphore_wait(told.at[2], 4)
            to_plane(g - 1)
        a = [
            own(dot(jnp.concatenate(grad, axis=0), paired(qkv_s[3 + g, at, :]), TN)) for grad, at in zip(grads, spans)
        ]
        b = [
            dot(jnp.concatenate([spread(x) for x in grad], axis=1), stacked(qkv_s[g, at, :]))
            for grad, at in zip(grads, spans)
        ]
        for low, at in zip(lows, spans):
            dv = dot(jnp.concatenate([spread(x) for x in low], axis=1), stacked(datt_s[g, at, :]))
            dqkv_s[g, at, 256:384] = dv.astype(BF16)
        for part, (grad, inverse) in enumerate(((a, qinv_s), (b, kinv_s))):
            unit = [qkv_s[3 * part + g, at, :].astype(F32) * inverse[g, at, :] for at in spans]
            along = [dot(split(u * x), same) for u, x in zip(unit, grad)]
            for u, x, y, at in zip(unit, grad, along, spans):
                dqkv_s[g, at, 128 * part : 128 * part + 128] = (x - u * y).astype(BF16)
        here = iota((PER, 128), 0) + PER * g == iota((PER, 128), 1)
        placed = jnp.where(here, jnp.sum(dscale, axis=1, keepdims=True), 0.0)
        placed = jnp.sum(placed, axis=0, keepdims=True)
        scale_row = placed if g == 0 else scale_row + placed
        for part in range(3):
            dw = dot(dqkv_s[g, :, 128 * part : 128 * part + 128], x_s[...], TN).astype(BF16).reshape(8, 16, C)
            if part == 0:
                g_s[g, 0, 0] = dw
            elif part == 2:
                g_s[g, 0, 1] = dw
            elif g == 0:
                keep_k[...] = dw
            elif g == 1:
                g_s[1, 1, 0, 0:4] = dw[0:4]
                g_s[1, 1, 1, 0:4] = dw[4:8]
            else:
                g_s[2, 1, 0] = keep_k[...]
                g_s[2, 1, 1] = dw
        core_copy(g).start()


    sm_s[24:25, :] = scale_row

    sub128 = iota((8, 128), 0)
    for h in range(HEADS):
        both = dbias_s[h]
        both = jnp.where(first, both + pltpu.roll(both, 64, 1), 0.0)
        for m, part in enumerate((jnp.where(ahead, both, 0.0), jnp.where(ahead, 0.0, both))):
            total = part[0:8]
            for n in range(1, 8):
                total = total + pltpu.roll(part[8 * n : 8 * n + 8], 128 - 8 * n, 1)
            for n in range(3):
                total = jnp.where(bit(sub128, n) == 1, pltpu.roll(total, 128 - 2**n, 1), total)
            sm_s[12 * m + h : 12 * m + h + 1, :] = jnp.sum(total, axis=0, keepdims=True)
    small_core = remote(
        sm_s.at[pl.ds(pl.multiple_of(16 * (1 - core), 16), 16)], smc_recv, csem_s.at[3], csem_r.at[3], (other, wa, ba)
    )
    small_core.start()


    to_plane(2)


    small_core.wait()
    smy_buf[high] = sm_s[pl.ds(pl.multiple_of(16 * core, 16), 16), :] + smc_recv[...]
    for b in (2, 1, 3):
        remote(smy_buf.at[high], smy_buf.at[high], xsem_s.at[3], xsem_r.at[3], (ha, seat(0, b, 0)[1], ba)).start()


    to_depth(0)


    for pair in range(PAIRS):
        at = slice(128 * pair, 128 * pair + 128)
        total = jnp.zeros((128, C), F32)
        for g in range(GROUPS):
            w = jnp.concatenate([wqkv[:, C * n + 128 * g : C * n + 128 * g + 128] for n in range(3)], axis=1)
            total = total + dot(dqkv_s[g, at, :], w, NT)
        dm_s[at, :] = total.astype(BF16).astype(F32)

    def image_rows(quad):
        parts = []
        for i in range(4):
            for pair in range(2):
                for window in range(2):
                    at = (quad // 2 * 2 + pair) * 128 + window * 64 + quad % 2 * 32 + 8 * i
                    parts.append(dm_s[at : at + 8, :])
        return jnp.concatenate(parts, axis=0)

    for quad in range(4):
        x = image_rows(quad)
        if quad == 3:
            rows_send2[...] = x.astype(BF16).reshape(4, COLS, C)
        x = x.reshape(4, 4, 8, C)
        tiles = [jnp.where(sub8, pltpu.roll(x[2 * i, 3], 4, 0), x[2 * i + 1, 3]) for i in range(2)]
        pk_send2[16 * quad : 16 * quad + 16, :] = jnp.concatenate(tiles, 0).astype(BF16)
    halo = [
        remote(rows_send2, rows_recv2, hsem_s.at[6], hsem_r.at[6], (down, wa, ba)),
        remote(pk_send2, pk_recv2, hsem_s.at[7], hsem_r.at[7], (ha, right, ba)),
        remote(pk_send2.at[pl.ds(48, 16)], cr_recv2, hsem_s.at[8], hsem_r.at[8], (down, right, ba)),
    ]
    for copy in halo:
        copy.start()


    to_depth(1)

    column = 2 * ba + low_x
    taken(smy_buf.at[pl.ds(0, 3)], xsem_s.at[3], xsem_r.at[3])
    smx_buf[column] = smy_buf[0] + smy_buf[1] + smy_buf[2] + smy_buf[3]
    for a, c in ((1, 0), (0, 1), (1, 1)):
        b, w = seat(a, 0, c)
        remote(smx_buf.at[column], smx_buf.at[column], xsem_s.at[4], xsem_r.at[4], (ha, w, b)).start()

    to_depth(2)

    to_level(0)

    taken(smx_buf.at[pl.ds(0, 3)], xsem_s.at[4], xsem_r.at[4])
    smz_buf[deep] = smx_buf[0] + smx_buf[1] + smx_buf[2] + smx_buf[3]
    for h in depth:
        remote(smz_buf.at[deep], smz_buf.at[deep], zsem_s.at[3], zsem_r.at[3], (h, wa, ba)).start()

    to_level(1)

    to_core(0)


    to_level(2)

    to_core(1)


    taken(smz_buf.at[pl.ds(0, 7)], zsem_s.at[3], zsem_r.at[3])
    total = smz_buf[0]
    for d in range(1, 8):
        total = total + smz_buf[d]
    smf_buf[core] = total
    remote(smf_buf.at[core], smf_buf.at[core], csem_s.at[4], csem_r.at[4], (other, wa, ba)).start()


    for copy in halo:
        copy.wait()
    for quad in range(4):
        if quad == 0:
            rows, pack = rows_recv2[...].astype(F32), cr_recv2[...]
        else:
            rows, pack = image_rows(quad - 1), pk_recv2[16 * quad - 16 : 16 * quad, :]
        x = pltpu.roll(rows.reshape(16, 8, C), 4, 1).reshape(4, 4, 8, C)
        pack = pack.astype(F32).reshape(2, 8, C)
        for i in range(4):
            parts = []
            for j in range(4):
                if j > 0:
                    before = x[i, j - 1]
                else:
                    before = pltpu.roll(pack[i // 2], 4, 0) if i % 2 else pack[i // 2]
                parts.append(jnp.where(sub8, before, x[i, j]))
            back = jnp.concatenate(parts, 0)
            row = 4 * quad + i
            dtok_o[0, row] = (cot[0, row].astype(F32) + back).astype(BF16)


    for c in range(CHUNKS):
        wait_level(c)


    taken(smf_buf.at[0], csem_s.at[4], csem_r.at[4])
    total_o[0:16, :] = smf_buf[0]
    total_o[16:32, :] = smf_buf[1]


def finish(pieces, total, moved, factor, dtok_o, dwqkv_o, dwproj_o, dtable_o, dscale_o, dgain_o):
    ba = lax.axis_index("ba")
    dtok_o[...] = moved[...]

    def rows(base, count):
        return pl.ds(pl.multiple_of(base, 64), count)

    def join(c, core, first, count):
        return pieces[c, 8 * core + first : 8 * core + first + count].reshape(16 * count, C).astype(F32)

    for c in range(CHUNKS):
        dwqkv_o[rows(128 * c + 192 * ba, 128), :] = join(c, 0, 0, 8)
    dwproj_o[0:128, :] = join(0, 1, 0, 8)
    dwqkv_o[rows(512 - 512 * ba, 64), :] = join(1, 1, 0, 4)
    dwproj_o[128:192, :] = join(1, 1, 4, 4)
    dwqkv_o[rows(384 - 320 * ba, 128), :] = join(2, 1, 0, 8)

    by_lane = jnp.concatenate([total[0:12], total[12:24]], axis=1)
    dtable_o[...] = fine(by_lane, offset_onehot(), NT) * factor[0:HEADS, 0:TABLE]
    dscale_o[...] = total[24:25, 0:HEADS] * factor[HEADS : HEADS + 1, 0:HEADS]
    for g in range(GROUPS):
        dgain_o[pl.ds(128 * g, 128)] = total[25 + g]


def step(tokens, cotangent, w_qkv, w_proj, table_logits, logit_scale, gain):
    vmem = pl.BlockSpec(memory_space=pltpu.VMEM)
    middle = [
        pltpu.VMEM((1, ROWS, COLS, C), BF16),
        pltpu.VMEM((CHUNKS, 16, 16, C), BF16),
        pltpu.VMEM((32, 128), F32),
        pltpu.VMEM((16, 256), F32),
    ]
    outs = [
        jax.ShapeDtypeStruct((1, ROWS, COLS, C), BF16),
        jax.ShapeDtypeStruct((576, C), F32),
        jax.ShapeDtypeStruct((192, C), F32),
        jax.ShapeDtypeStruct((HEADS, TABLE), F32),
        jax.ShapeDtypeStruct((1, HEADS), F32),
        jax.ShapeDtypeStruct((C,), F32),
    ]
    scratch = [
        pltpu.VMEM((1, ROWS, COLS, C), BF16),
        pltpu.VMEM((1, ROWS, COLS, C), BF16),
        pltpu.VMEM((C, 3 * C), BF16),
        pltpu.VMEM((C, C), BF16),
        pltpu.VMEM((HEADS, TABLE), F32),
        pltpu.VMEM((1, HEADS), F32),
        pltpu.VMEM((C,), F32),
        pltpu.VMEM((2, 64, C), BF16),
        pltpu.VMEM((2, 4, COLS, C), BF16),
        pltpu.VMEM((2, 64, C), BF16),
        pltpu.VMEM((2, 16, C), BF16),
        pltpu.VMEM((TOKENS, C), BF16),
        pltpu.VMEM((TOKENS, C), BF16),
        pltpu.VMEM((9, TOKENS, 128), BF16),
        pltpu.VMEM((GROUPS, TOKENS, 128), F32),
        pltpu.VMEM((GROUPS, TOKENS, 128), F32),
        pltpu.VMEM((GROUPS, PAIRS, 8, 128), F32),
        pltpu.VMEM((HEADS, 64, 128), F32),
        pltpu.VMEM((PAIRS, 64, 128), F32),
        pltpu.VMEM((GROUPS, PAIRS, 256, 128), F32),
        pltpu.VMEM((GROUPS, PAIRS, 256, 128), F32),
        pltpu.VMEM((GROUPS, PAIRS, 256, 128), F32),
        pltpu.VMEM((GROUPS, TOKENS, 128), BF16),
        pltpu.VMEM((GROUPS, TOKENS, 128), BF16),
        pltpu.VMEM((TOKENS, C), BF16),
        pltpu.VMEM((GROUPS, TOKENS, C), BF16),
        pltpu.VMEM((HEADS, 64, 128), F32),
        pltpu.VMEM((TOKENS, C), F32),
        pltpu.VMEM((4, COLS, C), BF16),
        pltpu.VMEM((64, C), BF16),
        pltpu.VMEM((4, COLS, C), BF16),
        pltpu.VMEM((64, C), BF16),
        pltpu.VMEM((16, C), BF16),
        pltpu.VMEM((8, 16, C), BF16),
        pltpu.VMEM((CHUNKS, 2, 2, 8, 16, C), BF16),
        pltpu.VMEM((CHUNKS, 2, 8, 16, C), BF16),
        pltpu.VMEM((CHUNKS, 2, 8, 16, C), BF16),
        pltpu.VMEM((CHUNKS, 15, 16, C), BF16),
        pltpu.VMEM((CHUNKS, 8, 16, C), BF16),
        pltpu.VMEM((32, 128), F32),
        pltpu.VMEM((16, 128), F32),
        pltpu.VMEM((4, 16, 128), F32),
        pltpu.VMEM((4, 16, 128), F32),
        pltpu.VMEM((8, 16, 128), F32),
        pltpu.VMEM((2, 16, 128), F32),
        pltpu.SemaphoreType.REGULAR((3,)),
        pltpu.SemaphoreType.DMA((7,)),
        pltpu.SemaphoreType.DMA((9,)),
        pltpu.SemaphoreType.DMA((9,)),
        pltpu.SemaphoreType.DMA((7,)),
        pltpu.SemaphoreType.DMA((7,)),
        pltpu.SemaphoreType.DMA((5,)),
        pltpu.SemaphoreType.DMA((5,)),
        pltpu.SemaphoreType.DMA((4,)),
        pltpu.SemaphoreType.DMA((4,)),
        pltpu.SemaphoreType.DMA((3,)),
        pltpu.SemaphoreType.DMA((3,)),
    ]
    lscale = logit_scale.reshape(1, HEADS)
    moved, pieces, total, factor = pl.pallas_call(
        kernel,
        name="window_backward",
        out_shape=middle,
        in_specs=[pl.BlockSpec(memory_space=pltpu.HBM)] * 7,
        out_specs=[vmem] * 4,
        scratch_shapes=scratch,
        compiler_params=pltpu.CompilerParams(collective_id=0, has_side_effects=True, vmem_limit_bytes=65_980_000),
    )(tokens, cotangent, w_qkv, w_proj, table_logits, lscale, gain)
    d_tokens, d_wqkv, d_wproj, d_table, d_scale, d_gain = pl.pallas_call(
        finish, name="finish", out_shape=outs, in_specs=[vmem] * 4, out_specs=[vmem] * 6, compiler_params=pltpu.CompilerParams(vmem_limit_bytes=16 * 2**20)
    )(pieces, total, moved, factor)
    return d_tokens, d_wqkv.T, d_wproj.T, d_table, d_scale.reshape(HEADS), d_gain


def solution(mesh):
    image = P("ba", "ha", "wa", None)
    return jax.shard_map(
        step,
        mesh=mesh,
        in_specs=(image, image, P(), P(), P(), P(), P()),
        out_specs=(image, P(None, "ba"), P(None, "ba"), P(), P(), P()),
        check_vma=False,
    )
```
